128 devices in a mesh: model: 64 (over z, y, x), data: 2 (over core).
Axes of the slice: x: 4, y: 4, z: 4, core: 2. Of those that a mesh axis runs over, the one named last changes fastest.
Arguments:
- tokens: bfloat16 [16384, 1664], P('data')
- w_up: bfloat16 [1664, 8192], P(None, 'model')
- w_down: bfloat16 [8192, 1664], P('model')
- task_heads: bfloat16 [8, 1664, 2], replicated
- labels: int32 [8, 16384], P(None, 'data')
Outputs:
- output 1: float32 [8], replicated
- output 2: float32 [1664, 8192], P('data', 'model')
- output 3: float32 [8192, 1664], P(('model', 'data'))
All inputs are finite; a program needn't handle non-finite values.
Results may differ from the reference program's by a relative error of at most 0.001.
Values are sent between devices in bfloat16 or wider.
A program may use at most 1 GiB of HBM per device.

```python
import jax
import jax.numpy as jnp
from jax import lax

HIDDEN = 1664
FFN = 8192
CLASSES = 2
TASKS = 8
TOKENS = 16384
SEGMENT = 8192
BLOCK = 256
STEPS = 20


def setup_inputs(seed: int = 0) -> dict:
    key_list = jax.random.split(jax.random.key(seed), 12)
    n_seg = TOKENS // SEGMENT
    seg_shift = jax.random.normal(key_list[0], (n_seg, 1, HIDDEN), jnp.float32)
    x_body = jax.random.normal(key_list[1], (n_seg, SEGMENT, HIDDEN), jnp.float32)
    tokens = (x_body + 0.5 * seg_shift).reshape(TOKENS, HIDDEN).astype(jnp.bfloat16)
    w_up = (jax.random.normal(key_list[2], (HIDDEN, FFN), jnp.float32) * HIDDEN ** -0.5).astype(jnp.bfloat16)
    w_down = (jax.random.normal(key_list[3], (FFN, HIDDEN), jnp.float32) * FFN ** -0.5).astype(jnp.bfloat16)
    task_sign = jnp.where(jnp.arange(TASKS) % 2 == 0, 1.0, -1.0).astype(jnp.float32)
    head_base = jax.random.normal(key_list[4], (HIDDEN, CLASSES), jnp.float32)
    head_own = jax.random.normal(key_list[5], (TASKS, HIDDEN, CLASSES), jnp.float32)
    task_heads = ((0.8 * task_sign[:, None, None] * head_base[None] + 0.6 * head_own) * (1.5 * HIDDEN ** -0.5)).astype(jnp.bfloat16)
    seg_pref = jax.random.randint(key_list[6], (n_seg, 1), 0, CLASSES)
    keep_pref = jax.random.randint(key_list[7], (n_seg, SEGMENT), 0, 4)
    any_label = jax.random.randint(key_list[8], (n_seg, SEGMENT), 0, CLASSES)
    shared = jnp.where(keep_pref < 3, seg_pref, any_label).reshape(TOKENS)
    own_label = jax.random.randint(key_list[9], (TASKS, TOKENS), 0, CLASSES)
    keep_shared = jax.random.randint(key_list[10], (TASKS, TOKENS), 0, 4)
    labels = jnp.where(keep_shared < 3, shared[None, :], own_label).astype(jnp.int32)
    return {'tokens': tokens, 'w_up': w_up, 'w_down': w_down, 'task_heads': task_heads, 'labels': labels}


def simplex_weights(gram_mat):
    trace_scale = jnp.trace(gram_mat) / TASKS

    def eg_step(weights, unused):
        updated = weights * jnp.exp(-jnp.sum(gram_mat * weights[None, :], axis=1) / trace_scale)
        return updated / jnp.sum(updated), None

    start_w = jnp.full((TASKS,), 1.0 / TASKS, jnp.float32)
    weights, unused = lax.scan(eg_step, start_w, None, length=STEPS)
    return weights


def reference(tokens, w_up, w_down, task_heads, labels):
    n_blocks = TOKENS // BLOCK
    tok_blocks = tokens.reshape(n_blocks, BLOCK, HIDDEN)
    lab_blocks = labels.reshape(TASKS, n_blocks, BLOCK).transpose(1, 0, 2)
    heads_f = task_heads.astype(jnp.float32)
    down_f = w_down.astype(jnp.float32)

    def block_grads(grad_acc, block_in):
        tok_blk, lab_blk = block_in
        pre_act = jnp.dot(tok_blk, w_up, preferred_element_type=jnp.float32)
        act_val, gelu_slope = jax.jvp(jax.nn.gelu, (pre_act,), (jnp.ones_like(pre_act),))
        act_bf = act_val.astype(jnp.bfloat16)
        mlp_out = jnp.dot(act_bf, w_down, preferred_element_type=jnp.float32)
        trunk_out = (tok_blk.astype(jnp.float32) + mlp_out).astype(jnp.bfloat16)
        logits = jnp.einsum('bd,tdc->tbc', trunk_out.astype(jnp.float32), heads_f)
        class_prob = jax.nn.softmax(logits, axis=-1)
        onehot = jax.nn.one_hot(lab_blk, CLASSES, dtype=jnp.float32)
        dlogit = (class_prob - onehot) / TOKENS
        d_trunk = jnp.einsum('tbc,tdc->tbd', dlogit, heads_f).astype(jnp.bfloat16).astype(jnp.float32)
        g_down = jnp.einsum('bf,tbd->tfd', act_bf.astype(jnp.float32), d_trunk)
        d_act = jnp.einsum('tbd,fd->tbf', d_trunk, down_f)
        d_pre = (d_act * gelu_slope[None]).astype(jnp.bfloat16).astype(jnp.float32)
        g_up = jnp.einsum('bd,tbf->tdf', tok_blk.astype(jnp.float32), d_pre)
        return (grad_acc[0] + g_up, grad_acc[1] + g_down), None

    zero_acc = (jnp.zeros((TASKS, HIDDEN, FFN), jnp.float32), jnp.zeros((TASKS, FFN, HIDDEN), jnp.float32))
    (g_up, g_down), unused = lax.scan(block_grads, zero_acc, (tok_blocks, lab_blocks))
    gram_mat = jnp.einsum('tij,sij->ts', g_up, g_up) + jnp.einsum('tij,sij->ts', g_down, g_down)
    task_weights = simplex_weights(gram_mat)
    grad_up = jnp.einsum('t,tij->ij', task_weights, g_up)
    grad_down = jnp.einsum('t,tij->ij', task_weights, g_down)
    return task_weights, grad_up, grad_down
```

```python
import functools

import jax
import jax.numpy as jnp
from jax import lax
from jax.experimental import pallas as pl
from jax.experimental.pallas import tpu as pltpu
from jax.sharding import PartitionSpec as P

STEPS = 20
LANES = 128
MESH = pl.DeviceIdType.MESH
F32 = jnp.float32
BF16 = jnp.bfloat16
C_GELU = 0.7978845608028654
K_GELU = 0.044715
NT = (((1,), (1,)), ((), ()))


def peer(model, data):
    return {"model": model, "data": data}


def ring_barrier(n_model, me_d, pair):
    sem = pltpu.get_barrier_semaphore()
    me = lax.axis_index("model")

    def tell(k, carry):
        pl.semaphore_signal(sem, inc=1, device_id=peer(lax.rem(me + k, n_model), me_d), device_id_type=MESH)
        return carry

    lax.fori_loop(1, n_model, tell, 0)
    if pair:
        pl.semaphore_signal(sem, inc=1, device_id=peer(me, 1 - me_d), device_id_type=MESH)
    return sem, n_model - 1 + (1 if pair else 0)


def forward_kernel(n_model, tile, win, x_ref, w1t_ref, ut_ref, gpt_ref, u2_ref, xz_ref,
                   xbuf, usend, xsem, send_sem, recv_sem, pair_sem):
    me = lax.axis_index("model")
    core = lax.axis_index("data")
    n_tok = x_ref.shape[0]
    blk = n_tok // n_model
    n_tile = n_tok // tile
    per = tile // blk
    off = x_ref.shape[1] - win
    sem, count = ring_barrier(n_model, core, True)
    start = lax.div(me, per)

    def tile_at(i):
        return lax.rem(i + start, n_tile)

    def fetch(i, slot):
        rows = pl.ds(pl.multiple_of(tile_at(i) * tile, tile), tile)
        return pltpu.make_async_copy(x_ref.at[rows, :], xbuf.at[slot], xsem.at[slot])

    fetch(0, 0).start()
    pl.semaphore_wait(sem, count)
    mine = pl.ds(pl.multiple_of(me * blk, blk), blk)
    own_x = pltpu.make_async_copy(x_ref.at[mine, pl.ds(pl.multiple_of(core * off, LANES), win)],
                                  xz_ref.at[pl.ds(0, blk), :], pair_sem.at[0])
    own_x.start()
    far_x = pltpu.make_async_remote_copy(
        src_ref=x_ref.at[mine, pl.ds(pl.multiple_of((1 - core) * off, LANES), win)],
        dst_ref=xz_ref.at[pl.ds(blk, blk), :], send_sem=pair_sem.at[1], recv_sem=pair_sem.at[2],
        device_id=peer(me, 1 - core), device_id_type=MESH)
    far_x.start()

    def step(i, carry):
        slot = lax.rem(i, 2)

        @pl.when(i + 1 < n_tile)
        def _():
            fetch(i + 1, 1 - slot).start()

        fetch(i, slot).wait()
        base = pl.multiple_of(tile_at(i) * tile, tile)
        a = lax.dot_general(w1t_ref[...], xbuf[slot], NT, preferred_element_type=F32)
        a2 = a * a
        th = jnp.tanh(C_GELU * (a + K_GELU * (a * a2)))
        cdf = 0.5 * (1.0 + th)
        slope = cdf + a * (0.5 * (1.0 - th * th) * (C_GELU * (1.0 + (3.0 * K_GELU) * a2)))
        u_f = a * cdf
        ut_ref[:, pl.ds(base, tile)] = u_f.astype(BF16)
        gpt_ref[:, pl.ds(base, tile)] = slope
        usend[pl.ds(base, tile), :] = u_f.T.astype(BF16)
        dst = u2_ref.at[pl.ds(0, blk), pl.ds(pl.multiple_of(me * LANES, LANES), LANES)]
        for k in range(per):
            src = usend.at[pl.ds(pl.multiple_of(base + k * blk, blk), blk), :]
            owner = tile_at(i) * per + k

            @pl.when(owner != me)
            def _():
                pltpu.make_async_remote_copy(
                    src_ref=src, dst_ref=dst, send_sem=send_sem, recv_sem=recv_sem,
                    device_id=peer(owner, core), device_id_type=MESH).start()

            @pl.when(owner == me)
            def _():
                pltpu.make_async_copy(src, dst, recv_sem).start()
        return carry

    lax.fori_loop(0, n_tile, step, 0)
    own_u = u2_ref.at[pl.ds(0, blk), :]
    pltpu.make_async_copy(own_u, own_u, recv_sem).wait()
    far_u = pltpu.make_async_remote_copy(
        src_ref=own_u, dst_ref=u2_ref.at[pl.ds(blk, blk), :], send_sem=pair_sem.at[3], recv_sem=pair_sem.at[4],
        device_id=peer(me, 1 - core), device_id_type=MESH)
    far_u.start()
    sent = usend.at[pl.ds(0, n_tok - blk), :]
    pltpu.make_async_copy(sent, sent, send_sem).wait()
    own_x.wait()
    far_x.wait()
    far_u.wait()


def token_kernel(n_model, chunk, n_total, u2_ref, w2g_ref, xz_ref, ht_ref, lab_ref, et_ref,
                 wbuf, acc, lsend, lrecv, esend, wsem, pair_sem, send_sem, recv_sem):
    me = lax.axis_index("model")
    core = lax.axis_index("data")
    blk = u2_ref.shape[0] // 2
    n_chunk = w2g_ref.shape[0] // chunk
    n_task = lab_ref.shape[0]
    sem, count = ring_barrier(n_model, core, True)

    def fetch(i, slot):
        rows = pl.ds(pl.multiple_of(i * chunk, chunk), chunk)
        return pltpu.make_async_copy(w2g_ref.at[rows, :], wbuf.at[slot], wsem.at[slot])

    fetch(0, 0).start()
    fetch(1, 1).start()
    acc[...] = xz_ref[...].astype(F32) * 0.0

    def step(i, carry):
        slot = lax.rem(i, 3)

        @pl.when(i + 2 < n_chunk)
        def _():
            fetch(i + 2, lax.rem(i + 2, 3)).start()

        fetch(i, slot).wait()
        cols = pl.ds(pl.multiple_of(i * chunk, chunk), chunk)
        acc[...] += jnp.dot(u2_ref[:, cols], wbuf[slot], preferred_element_type=F32)
        return carry

    lax.fori_loop(0, n_chunk, step, 0)
    z = (xz_ref[...].astype(F32) + acc[...]).astype(BF16)
    part = lax.dot_general(ht_ref[...], z, NT, preferred_element_type=F32)
    lsend[...] = part[:, blk:]
    pl.semaphore_wait(sem, count)
    swap = pltpu.make_async_remote_copy(
        src_ref=lsend, dst_ref=lrecv, send_sem=pair_sem.at[0], recv_sem=pair_sem.at[1],
        device_id=peer(me, 1 - core), device_id_type=MESH)
    swap.start()
    swap.wait()
    logit = part[:, :blk] + lrecv[...]
    gap = logit[:n_task, :] - logit[n_task:, :]
    first = lab_ref[...] == 0
    wrong = 1.0 / (1.0 + jnp.exp(jnp.where(first, gap, -gap)))
    esend[...] = jnp.where(first, -wrong, wrong) * (1.0 / n_total)

    dst = et_ref.at[:, pl.ds(pl.multiple_of(me * blk, LANES), blk)]

    def send(k, carry):
        pltpu.make_async_remote_copy(
            src_ref=esend, dst_ref=dst, send_sem=send_sem, recv_sem=recv_sem,
            device_id=peer(lax.rem(me + k, n_model), core), device_id_type=MESH).start()
        return carry

    lax.fori_loop(1, n_model, send, 0)
    pltpu.make_async_copy(esend, dst, recv_sem).start()
    pltpu.make_async_copy(et_ref, et_ref, recv_sem).wait()
    sent = et_ref.at[:, pl.ds(0, (n_model - 1) * blk)]
    pltpu.make_async_copy(sent, sent, send_sem).wait()


def grad_kernel(et_ref, ut_ref, gpt_ref, x_ref, w2_ref, drow_ref, dcol_ref, gdn_ref, gup_ref,
                dn_acc, up_acc, ebr, dat, out_sem):
    step = pl.program_id(0)
    n_task, tile = et_ref.shape
    width, hidden = w2_ref.shape
    wide = 256
    cuts = [(c, min(wide, hidden - c)) for c in range(0, hidden, wide)]

    @pl.when(step == 0)
    def _():
        dn_acc[...] = jnp.zeros_like(dn_acc)
        up_acc[...] = jnp.zeros_like(up_acc)

    for t in range(n_task):
        ebr[t] = et_ref[t:t + 1, :]

    def one_task(t, carry):
        e_row = ebr[t]
        for n in range(0, tile, wide):
            e_n = e_row[:, n:n + wide]
            da = jnp.zeros((width, wide), F32)
            for c, size in cuts:
                d_c = dcol_ref[t, c:c + size, :]
                d_c = jnp.concatenate([d_c] * (wide // LANES), axis=1)
                dz_t = (d_c * e_n).astype(BF16)
                da = da + jnp.dot(w2_ref[:, c:c + size], dz_t, preferred_element_type=F32)
            dat[pl.ds(pl.multiple_of(t * width, width), width), n:n + wide] = (da * gpt_ref[:, n:n + wide]).astype(BF16)
        e_col = jnp.broadcast_to(e_row, (LANES, tile)).T
        for c, size in cuts:
            e_b = e_col
            e_b = jnp.concatenate([e_b] * (size // LANES), axis=1)
            dz = (e_b * drow_ref[t, :, c:c + size]).astype(BF16)
            dn_acc[t, :, c:c + size] += jnp.dot(ut_ref[...], dz, preferred_element_type=F32)
        return carry

    lax.fori_loop(0, n_task, one_task, 0)
    rows = 2 * width

    def up_part(m, carry):
        at = pl.ds(pl.multiple_of(m * rows, rows), rows)
        left = dat[at, :]
        for c, size in cuts:
            up_acc[at, c:c + size] += jnp.dot(left, x_ref[:, c:c + size], preferred_element_type=F32)
        return carry

    lax.fori_loop(0, n_task * width // rows, up_part, 0)

    @pl.when(step == pl.num_programs(0) - 1)
    def _():
        one = pltpu.make_async_copy(dn_acc, gdn_ref, out_sem.at[0])
        two = pltpu.make_async_copy(up_acc, gup_ref, out_sem.at[1])
        one.start()
        two.start()
        one.wait()
        two.wait()


def mix_kernel(n_model, win, gdn_ref, gup_ref, a_ref, g1_ref, g2_ref,
               dn_own, dn_far, up_own, up_far, msend, mrecv, g1t, dsem, usem, send_sem, recv_sem):
    me = lax.axis_index("model")
    core = lax.axis_index("data")
    n_task, half, hidden = dn_own.shape
    width = 2 * half
    off = hidden - win
    sem = pltpu.get_barrier_semaphore()

    n_all = 2 * n_model
    slot = me * 2 + core

    def other(k):
        at = lax.rem(slot + k, n_all)
        return peer(lax.div(at, 2), lax.rem(at, 2))

    def tell(k, carry):
        pl.semaphore_signal(sem, inc=1, device_id=other(k), device_id_type=MESH)
        return carry

    lax.fori_loop(1, n_all, tell, 0)
    my_cols = pl.ds(pl.multiple_of(core * off, LANES), win)
    far_cols = pl.ds(pl.multiple_of((1 - core) * off, LANES), win)
    local = []
    for t in range(n_task):
        local.append(pltpu.make_async_copy(
            gdn_ref.at[t, pl.ds(pl.multiple_of(core * half, half), half), :], dn_own.at[t], dsem.at[0, t]))
        local.append(pltpu.make_async_copy(
            gup_ref.at[pl.ds(t * width, width), my_cols], up_own.at[t], usem.at[0, t]))
    for c in local:
        c.start()
    pl.semaphore_wait(sem, n_all - 1)
    far = []
    for t in range(n_task):
        far.append(pltpu.make_async_remote_copy(
            src_ref=gdn_ref.at[t, pl.ds(pl.multiple_of((1 - core) * half, half), half), :], dst_ref=dn_far.at[t],
            send_sem=dsem.at[1, t], recv_sem=dsem.at[2, t], device_id=peer(me, 1 - core), device_id_type=MESH))
        far.append(pltpu.make_async_remote_copy(
            src_ref=gup_ref.at[pl.ds(t * width, width), far_cols], dst_ref=up_far.at[t],
            send_sem=usem.at[1, t], recv_sem=usem.at[2, t], device_id=peer(me, 1 - core), device_id_type=MESH))
    for c in far:
        c.start()
    for c in local:
        c.wait()
    for c in far:
        c.wait()

    pairs = [(t, s) for t in range(n_task) for s in range(t, n_task)]
    lane = lax.broadcasted_iota(jnp.int32, (8, LANES), 1)

    def fold(own, other, r, c, keep, sums):
        rows = pl.ds(pl.multiple_of(r * 8, 8), 8)
        vals = []
        for t in range(n_task):
            v = own[t, rows, c:c + LANES] + other[t, rows, c:c + LANES]
            own[t, rows, c:c + LANES] = v
            vals.append(v if keep is None else jnp.where(keep, v, 0.0))
        return tuple(acc + vals[t] * vals[s] for acc, (t, s) in zip(sums, pairs))

    sums = tuple(jnp.zeros((8, LANES), F32) for _ in pairs)
    for c in range(0, hidden, LANES):
        sums = lax.fori_loop(0, half // 8, functools.partial(
            lambda c, r, s: fold(dn_own, dn_far, r, c, None, s), c), sums)
    first = core * (win - hidden // 2)
    for c in range(0, win, LANES):
        edge = c < win - hidden // 2 or c + LANES > hidden // 2
        keep = (lane + c >= first) & (lane + c < first + hidden // 2) if edge else None
        sums = lax.fori_loop(0, width // 8, functools.partial(
            lambda c, keep, r, s: fold(up_own, up_far, r, c, keep, s), c, keep), sums)

    row = lax.broadcasted_iota(jnp.int32, (8, LANES), 0)
    part = jnp.zeros((8, LANES), F32)
    for acc, (t, s) in zip(sums, pairs):
        total = jnp.sum(jnp.sum(acc, axis=1, keepdims=True), axis=0, keepdims=True)
        here = ((row == t) & (lane == s)) | ((row == s) & (lane == t))
        part = part + jnp.where(here, total, 0.0)
    msend[...] = part

    def send(k, carry):
        pltpu.make_async_remote_copy(
            src_ref=msend, dst_ref=mrecv.at[slot], send_sem=send_sem, recv_sem=recv_sem,
            device_id=other(k), device_id_type=MESH).start()
        return carry

    lax.fori_loop(1, n_all, send, 0)
    pltpu.make_async_copy(msend, mrecv.at[slot], recv_sem).start()
    pltpu.make_async_copy(mrecv, mrecv, recv_sem).wait()
    gram = jnp.sum(mrecv[...], axis=0)

    scale = jnp.sum(jnp.sum(jnp.where(row == lane, gram, 0.0), axis=1, keepdims=True), axis=0, keepdims=True) / n_task
    gram = gram / scale
    w = jnp.where(lane < n_task, 1.0 / n_task, 0.0).astype(F32)

    def eg_pair(i, w):
        v = w[:, 0:1] * 0.0 + jnp.sum(gram * w, axis=1, keepdims=True)
        w_col = jnp.sum(jnp.where(row == lane, w, 0.0), axis=1, keepdims=True)
        w_col = w_col * jnp.exp(-v)
        w_col = w_col / jnp.sum(w_col, axis=0, keepdims=True)
        v = jnp.sum(gram * w_col, axis=0, keepdims=True)
        w_row = jnp.sum(jnp.where(row == lane, w_col, 0.0), axis=0, keepdims=True)
        w_row = w_row * jnp.exp(-v)
        w_row = w_row / jnp.sum(w_row, axis=1, keepdims=True)
        return jnp.broadcast_to(w_row, (8, LANES))

    w = lax.fori_loop(0, STEPS // 2, eg_pair, w)
    a_ref[...] = w
    a = [jnp.sum(jnp.where(lane == t, w, 0.0), axis=1, keepdims=True) for t in range(n_task)]

    for c in range(0, hidden, LANES):
        def body2(r, carry, c=c):
            rows = pl.ds(pl.multiple_of(r * 8, 8), 8)
            total = a[0] * dn_own[0, rows, c:c + LANES]
            for t in range(1, n_task):
                total = total + a[t] * dn_own[t, rows, c:c + LANES]
            g2_ref[rows, c:c + LANES] = total
            return carry
        lax.fori_loop(0, half // 8, body2, 0)
    for c in range(0, win, LANES):
        def body1(r, carry, c=c):
            rows = pl.ds(pl.multiple_of(r * 8, 8), 8)
            total = a[0] * up_own[0, rows, c:c + LANES]
            for t in range(1, n_task):
                total = total + a[t] * up_own[t, rows, c:c + LANES]
            up_far[0, rows, c:c + LANES] = total
            return carry
        lax.fori_loop(0, width // 8, body1, 0)
    for c in range(0, win, LANES):
        g1t[c:c + LANES, :] = up_far[0, :, c:c + LANES].T
    g1_ref[...] = g1t[pl.ds(pl.multiple_of(first, 8), hidden // 2), :]
    sent = mrecv.at[pl.ds(0, n_all - 1)]
    pltpu.make_async_copy(sent, sent, send_sem).wait()


def solution(mesh):
    n_model, n_data = mesh.shape['model'], mesh.shape['data']

    def local_step(tokens, w_up, w_down, task_heads, labels):
        n_tok, hidden = tokens.shape
        n_total = n_tok * n_data
        width = w_up.shape[1]
        n_task = task_heads.shape[0]
        blk = n_tok // n_model
        win = -(-(hidden // 2) // LANES) * LANES
        off = hidden - win
        me = lax.axis_index('model')
        core = lax.axis_index('data')
        any_spec = pl.BlockSpec(memory_space=pl.ANY)
        vmem_spec = pl.BlockSpec(memory_space=pltpu.VMEM)
        big = 60 * 1024 * 1024

        w2_win = lax.dynamic_slice(w_down, (0, core * off), (width, win))
        w2_all = lax.all_gather(w2_win, 'model', axis=0, tiled=True)

        tile = min(512, n_tok)
        ut, gpt, u2, xz = pl.pallas_call(
            functools.partial(forward_kernel, n_model, tile, win),
            out_shape=(jax.ShapeDtypeStruct((width, n_tok), BF16), jax.ShapeDtypeStruct((width, n_tok), F32),
                       jax.ShapeDtypeStruct((2 * blk, n_model * width), BF16),
                       jax.ShapeDtypeStruct((2 * blk, win), BF16)),
            in_specs=[any_spec, vmem_spec],
            out_specs=(vmem_spec, vmem_spec, any_spec, any_spec),
            scratch_shapes=[pltpu.VMEM((2, tile, hidden), BF16), pltpu.VMEM((n_tok, width), BF16),
                            pltpu.SemaphoreType.DMA((2,)), pltpu.SemaphoreType.DMA, pltpu.SemaphoreType.DMA,
                            pltpu.SemaphoreType.DMA((5,))],
            compiler_params=pltpu.CompilerParams(collective_id=0, has_side_effects=True, vmem_limit_bytes=big),
            cost_estimate=pl.CostEstimate(flops=4 * n_tok * hidden * width, bytes_accessed=n_tok * hidden * 2,
                                          transcendentals=n_tok * width),
            name='forward_send')(tokens, w_up.T)

        heads = task_heads.astype(F32)
        h_t = jnp.concatenate([task_heads[:, :, 0], task_heads[:, :, 1]], axis=0)
        h_win = lax.dynamic_slice(h_t, (0, core * off), (2 * n_task, win))
        col = lax.broadcasted_iota(jnp.int32, (2 * n_task, win), 1)
        edge = core * (win - hidden // 2)
        h_win = jnp.where((col >= edge) & (col < edge + hidden // 2), h_win, jnp.zeros_like(h_win))
        my_lab = lax.dynamic_slice(labels, (0, me * blk), (n_task, blk))
        chunk = min(512, n_model * width)
        e_t = pl.pallas_call(
            functools.partial(token_kernel, n_model, chunk, n_total),
            out_shape=jax.ShapeDtypeStruct((n_task, n_tok), F32),
            in_specs=[vmem_spec, any_spec, vmem_spec, vmem_spec, vmem_spec],
            out_specs=vmem_spec,
            scratch_shapes=[pltpu.VMEM((3, chunk, win), BF16), pltpu.VMEM((2 * blk, win), F32),
                            pltpu.VMEM((2 * n_task, blk), F32), pltpu.VMEM((2 * n_task, blk), F32),
                            pltpu.VMEM((n_task, blk), F32), pltpu.SemaphoreType.DMA((3,)),
                            pltpu.SemaphoreType.DMA((2,)), pltpu.SemaphoreType.DMA, pltpu.SemaphoreType.DMA],
            compiler_params=pltpu.CompilerParams(collective_id=1, has_side_effects=True, vmem_limit_bytes=big),
            cost_estimate=pl.CostEstimate(flops=2 * n_tok * hidden * width, bytes_accessed=n_model * width * win * 2,
                                          transcendentals=0),
            name='token_side')(u2, w2_all, xz, h_win, my_lab)

        d_row = heads[:, :, 0] - heads[:, :, 1]
        d_col = jnp.broadcast_to(d_row[:, :, None], (n_task, hidden, LANES))
        t_b = min(512, n_tok)
        const2 = lambda i: (0, 0)
        g_dn, g_up = pl.pallas_call(
            grad_kernel,
            out_shape=(jax.ShapeDtypeStruct((n_task, width, hidden), F32),
                       jax.ShapeDtypeStruct((n_task * width, hidden), F32)),
            grid=(n_tok // t_b,),
            in_specs=[pl.BlockSpec((n_task, t_b), lambda i: (0, i)), pl.BlockSpec((width, t_b), lambda i: (0, i)),
                      pl.BlockSpec((width, t_b), lambda i: (0, i)), pl.BlockSpec((t_b, hidden), lambda i: (i, 0)),
                      pl.BlockSpec((width, hidden), const2, pipeline_mode=pl.Buffered(1)),
                      pl.BlockSpec((n_task, 1, hidden), lambda i: (0, 0, 0), pipeline_mode=pl.Buffered(1)),
                      pl.BlockSpec((n_task, hidden, LANES), lambda i: (0, 0, 0), pipeline_mode=pl.Buffered(1))],
            out_specs=(any_spec, any_spec),
            scratch_shapes=[pltpu.VMEM((n_task, width, hidden), F32), pltpu.VMEM((n_task * width, hidden), F32),
                            pltpu.VMEM((n_task, 1, t_b), F32),
                            pltpu.VMEM((n_task * width, t_b), BF16),
                            pltpu.SemaphoreType.DMA((2,))],
            compiler_params=pltpu.CompilerParams(dimension_semantics=('arbitrary',), vmem_limit_bytes=big),
            cost_estimate=pl.CostEstimate(flops=48 * n_tok * hidden * width, bytes_accessed=n_tok * hidden * 2,
                                          transcendentals=0),
            name='task_grads')(e_t, ut, gpt, tokens, w_down, d_row[:, None, :], d_col)

        half = width // 2
        weights, grad_up, grad_down = pl.pallas_call(
            functools.partial(mix_kernel, n_model, win),
            out_shape=(jax.ShapeDtypeStruct((8, LANES), F32), jax.ShapeDtypeStruct((hidden // 2, width), F32),
                       jax.ShapeDtypeStruct((half, hidden), F32)),
            in_specs=[any_spec, any_spec],
            out_specs=(vmem_spec, vmem_spec, vmem_spec),
            scratch_shapes=[pltpu.VMEM((n_task, half, hidden), F32), pltpu.VMEM((n_task, half, hidden), F32),
                            pltpu.VMEM((n_task, width, win), F32), pltpu.VMEM((n_task, width, win), F32),
                            pltpu.VMEM((8, LANES), F32), pltpu.VMEM((2 * n_model, 8, LANES), F32),
                            pltpu.VMEM((win, width), F32),
                            pltpu.SemaphoreType.DMA((3, n_task)), pltpu.SemaphoreType.DMA((3, n_task)),
                            pltpu.SemaphoreType.DMA, pltpu.SemaphoreType.DMA],
            compiler_params=pltpu.CompilerParams(collective_id=2, has_side_effects=True, vmem_limit_bytes=big),
            name='mix')(g_dn, g_up)
        return weights[0, :n_task], grad_up, grad_down

    return jax.shard_map(
        local_step, mesh=mesh,
        in_specs=(P('data', None), P(None, 'model'), P('model', None), P(None, None, None), P(None, 'data')),
        out_specs=(P(None), P('data', 'model'), P(('model', 'data'), None)),
        check_vma=False)
```

```python
import functools

import jax
import jax.numpy as jnp
from jax import lax
from jax.experimental import pallas as pl
from jax.experimental.pallas import tpu as pltpu
from jax.sharding import PartitionSpec as P

STEPS = 20
LANES = 128
MESH = pl.DeviceIdType.MESH
F32 = jnp.float32
BF16 = jnp.bfloat16
C_GELU = 0.7978845608028654
K_GELU = 0.044715
NT = (((1,), (1,)), ((), ()))


def peer(model, data):
    return {"model": model, "data": data}


def ring_barrier(n_model, me_d, pair):
    sem = pltpu.get_barrier_semaphore()
    me = lax.axis_index("model")

    def tell(k, carry):
        pl.semaphore_signal(sem, inc=1, device_id=peer(lax.rem(me + k, n_model), me_d), device_id_type=MESH)
        return carry

    lax.fori_loop(1, n_model, tell, 0)
    if pair:
        pl.semaphore_signal(sem, inc=1, device_id=peer(me, 1 - me_d), device_id_type=MESH)
    return sem, n_model - 1 + (1 if pair else 0)


def forward_kernel(n_model, win, n_total, x_ref, w1t_ref, w2_ref, ht_ref, lab_ref, ut_ref, gpt_ref, et_ref,
                   xbuf, usend, ut_s, gp_s, uslab, wslab, xz, zout, zrelay, zin, lsend, lrecv, esend,
                   xsem, osem, usend_sem, urecv_sem, wsend_sem, wrecv_sem, psend_sem, precv_sem,
                   zsend_sem, zrecv_sem, esend_sem, erecv_sem, lsem):
    me = lax.axis_index("model")
    core = lax.axis_index("data")
    ring = 4
    plane = ring * ring
    n_tok, hidden = x_ref.shape
    blk = n_tok // n_model
    width = w1t_ref.shape[0]
    n_task = lab_ref.shape[0]
    off = hidden - win
    part = width // 2
    px, py, pz = lax.rem(me, ring), lax.rem(lax.div(me, ring), ring), lax.div(me, plane)
    group = lax.div(me, ring)
    n_step = plane
    per = plane // ring

    def at(x, y, z):
        model = lax.rem(z + ring, ring) * plane + lax.rem(y + ring, ring) * ring + lax.rem(x + ring, ring)
        return peer(model, core)

    def remote(src, dst, ssem, rsem, dev):
        return pltpu.make_async_remote_copy(src_ref=src, dst_ref=dst, send_sem=ssem, recv_sem=rsem,
                                            device_id=dev, device_id_type=MESH)

    partner = peer(me, 1 - core)
    sem, count = ring_barrier(n_model, core, True)
    shifts = (2, 1, 3, 0)

    def block_of(i, k):
        sub = lax.div(i, per)
        shift = jnp.where(sub == 0, 2, jnp.where(sub == 1, 1, jnp.where(sub == 2, 3, 0)))
        g = lax.rem(group + lax.rem(i, per) * per + k, plane)
        return sub, g, g * ring + lax.rem(px + shift, ring)

    def fetch(i, slot):
        out = []
        for k in range(per):
            b = block_of(i, k)[2]
            out.append(pltpu.make_async_copy(
                x_ref.at[pl.ds(pl.multiple_of(b * blk, blk), blk), :], xbuf.at[slot, pl.ds(k * blk, blk), :],
                xsem.at[slot, k]))
        return out

    for c in fetch(0, 0):
        c.start()
    w_cols = pl.ds(pl.multiple_of(core * off, LANES), win)
    mine = pl.ds(pl.multiple_of(me * blk, blk), blk)
    own = [pltpu.make_async_copy(x_ref.at[mine, w_cols], xz.at[0], lsem.at[0])]
    coords = ((py, pz), (pz, py))
    for h in range(2):
        c1, c2 = coords[h]
        own.append(pltpu.make_async_copy(w2_ref.at[pl.ds(h * part, part), w_cols],
                                         wslab.at[h, c2 * ring + c1], lsem.at[1 + h]))
    for c in own:
        c.start()

    def near(h, axis, d):
        y_axis = (h == 0) == (axis == 0)
        return at(px, py + d, pz) if y_axis else at(px, py, pz + d)

    def gather_copy(h, stage, way):
        c1, c2 = coords[h]
        d = 1 if way == 0 else -1
        sems = (wsend_sem.at[h, stage, way], wrecv_sem.at[h, stage, way])
        if stage == 0:
            src = w2_ref.at[pl.ds(h * part, part), w_cols]
            return remote(src, wslab.at[h, c2 * ring + c1], *sems, near(h, 0, d))
        if stage == 1:
            piece = c2 * ring + lax.rem(c1 - d + ring, ring)
            ref = wslab.at[h, piece, pl.ds(way * (part // 2), part // 2), :]
            return remote(ref, ref, *sems, near(h, 0, d))
        if stage == 2:
            ref = wslab.at[h, pl.ds(c2 * ring, ring)]
            return remote(ref, ref, *sems, near(h, 1, d))
        ref = wslab.at[h, pl.ds(lax.rem(c2 - d + ring, ring) * ring + way * (ring // 2), ring // 2)]
        return remote(ref, ref, *sems, near(h, 1, d))

    hw = [(h, way) for h in range(2) for way in range(2)]
    pl.semaphore_wait(sem, count)
    far_x = remote(x_ref.at[mine, pl.ds(pl.multiple_of((1 - core) * off, LANES), win)], xz.at[1],
                   psend_sem.at[4], precv_sem.at[4], partner)
    for h, way in hw:
        gather_copy(h, 0, way).start()
    far_x.start()

    def step(i, carry):
        slot = lax.rem(i, 2)

        @pl.when(i + 1 < n_step)
        def _():
            for c in fetch(i + 1, 1 - slot):
                c.start()

        for c in fetch(i, slot):
            c.wait()
        a = lax.dot_general(w1t_ref[...], xbuf[slot], NT, preferred_element_type=F32)
        a2 = a * a
        th = jnp.tanh(C_GELU * (a + K_GELU * (a * a2)))
        cdf = 0.5 * (1.0 + th)
        slope = cdf + a * (0.5 * (1.0 - th * th) * (C_GELU * (1.0 + (3.0 * K_GELU) * a2)))
        u_f = a * cdf
        u_b = u_f.astype(BF16)
        usend[pl.ds(pl.multiple_of(i * per * blk, blk), per * blk), :] = u_f.T.astype(BF16)
        for k in range(per):
            sub, g, b = block_of(i, k)
            cols = pl.ds(pl.multiple_of(b * blk, blk), blk)
            ut_s[:, cols] = u_b[:, k * blk:(k + 1) * blk]
            gp_s[:, cols] = slope[:, k * blk:(k + 1) * blk]
            src = usend.at[pl.ds(pl.multiple_of((i * per + k) * blk, blk), blk), :]
            dst = uslab.at[0, sub, :, pl.ds(pl.multiple_of(group * width, width), width)]

            @pl.when(g != group)
            def _():
                remote(src, dst, usend_sem, urecv_sem.at[sub], peer(g * ring + px, core)).start()

            @pl.when(g == group)
            def _():
                pltpu.make_async_copy(src, dst, urecv_sem.at[sub]).start()
        return carry

    lax.fori_loop(0, n_step // 4, step, 0)
    for h, way in hw:
        gather_copy(h, 0, way).wait_recv()
        gather_copy(h, 1, way).start()
    lax.fori_loop(n_step // 4, n_step // 2, step, 0)
    for c in own:
        c.wait()
    for h, way in hw:
        gather_copy(h, 1, way).wait_recv()
    for h, way in hw:
        gather_copy(h, 2, way).start()
    lax.fori_loop(n_step // 2, n_step, step, 0)
    out_ut = pltpu.make_async_copy(ut_s, ut_ref, osem.at[0])
    out_gp = pltpu.make_async_copy(gp_s, gpt_ref, osem.at[1])
    out_ut.start()
    out_gp.start()
    for h, way in hw:
        gather_copy(h, 2, way).wait_recv()
        gather_copy(h, 3, way).start()

    def u_pair(s):
        return remote(uslab.at[0, s], uslab.at[1, s], psend_sem.at[s], precv_sem.at[s], partner)

    def u_arrive(s):
        pltpu.make_async_copy(uslab.at[0, s], uslab.at[0, s], urecv_sem.at[s]).wait()
        u_pair(s).start()

    def z_copy(n):
        left, right = at(px - 1, py, pz), at(px + 1, py, pz)
        src, dst, dev = ((zout.at[0, 0], zrelay.at[0], right), (zout.at[0, 1], zrelay.at[1], left),
                         (zout.at[1], zin.at[0], right), (zout.at[2], zin.at[1], left))[n]
        return remote(src, dst, zsend_sem.at[n], zrecv_sem.at[n], dev)

    def rows_of(g):
        y, z = g % ring, g // ring
        return [(0, z * ring + y), (1, y * ring + z)]

    def partial_z(s, put):
        for c in range(0, win, 256):
            size = min(256, win - c)
            total = jnp.zeros((2 * blk, size), F32)
            for g in range(0, plane, 2):
                left = jnp.concatenate([uslab[q, s, :, g * width:(g + 2) * width] for q in range(2)], axis=0)
                right = jnp.concatenate([wslab[h, j, :, c:c + size] for h, j in rows_of(g) + rows_of(g + 1)], axis=0)
                total = total + jnp.dot(left, right, preferred_element_type=F32)
            put(c, size, total)

    u_arrive(0)
    for h, way in hw:
        gather_copy(h, 3, way).wait_recv()
    u_pair(0).wait_recv()

    def put_far(c, size, total):
        zout[0, 0, :, c:c + size] = total[:blk]
        zout[0, 1, :, c:c + size] = total[blk:]

    partial_z(0, put_far)
    z_copy(0).start()
    z_copy(1).start()
    for s in (1, 2):
        u_arrive(s)
        u_pair(s).wait_recv()
        z_copy(s - 1).wait_recv()

        def put_near(c, size, total, s=s):
            for q in range(2):
                v = total[q * blk:(q + 1) * blk]
                zout[s, q, :, c:c + size] = v + zrelay[q, :, c:c + size] if q == s - 1 else v

        partial_z(s, put_near)
        z_copy(s + 1).start()
    u_arrive(3)
    u_pair(3).wait_recv()
    far_x.wait_recv()
    z_copy(0).wait_send()
    z_copy(1).wait_send()

    def put_own(c, size, total):
        for q in range(2):
            zout[0, q, :, c:c + size] = total[q * blk:(q + 1) * blk]

    partial_z(3, put_own)
    z_copy(2).wait_recv()
    z_copy(3).wait_recv()
    gaps = []
    for q in range(2):
        z = (xz[q].astype(F32) + ((zout[0, q] + zin[0, q]) + zin[1, q])).astype(BF16)
        gaps.append(lax.dot_general(ht_ref[...], z, NT, preferred_element_type=F32))
    lsend[...] = gaps[1]
    swap = remote(lsend, lrecv, psend_sem.at[5], precv_sem.at[5], partner)
    swap.start()
    swap.wait()
    logit = gaps[0] + lrecv[...]
    gap = logit[:n_task, :] - logit[n_task:, :]
    first = lab_ref[:, mine] == 0
    wrong = 1.0 / (1.0 + jnp.exp(jnp.where(first, gap, -gap)))
    esend[...] = jnp.where(first, -wrong, wrong) * (1.0 / n_total)
    dst = et_ref.at[:, pl.ds(pl.multiple_of(me * blk, LANES), blk)]

    def send(k, carry):
        remote(esend, dst, esend_sem, erecv_sem, peer(lax.rem(me + k, n_model), core)).start()
        return carry

    lax.fori_loop(1, n_model, send, 0)
    pltpu.make_async_copy(esend, dst, erecv_sem).start()
    for h, way in hw:
        for stage in range(4):
            gather_copy(h, stage, way).wait_send()
    for s in range(4):
        u_pair(s).wait_send()
    far_x.wait_send()
    z_copy(2).wait_send()
    z_copy(3).wait_send()
    sent = usend.at[pl.ds(0, n_tok - ring * blk), :]
    pltpu.make_async_copy(sent, sent, usend_sem).wait()
    out_ut.wait()
    out_gp.wait()
    pltpu.make_async_copy(et_ref, et_ref, erecv_sem).wait()
    sent = et_ref.at[:, pl.ds(0, (n_model - 1) * blk)]
    pltpu.make_async_copy(sent, sent, esend_sem).wait()


def grad_kernel(et_ref, ut_ref, gpt_ref, x_ref, w2_ref, drow_ref, dcol_ref, gdn_ref, gup_ref,
                dn_acc, up_acc, ebr, dat, out_sem):
    step = pl.program_id(0)
    n_task, tile = et_ref.shape
    width, hidden = w2_ref.shape
    wide = 256
    cuts = [(c, min(wide, hidden - c)) for c in range(0, hidden, wide)]

    @pl.when(step == 0)
    def _():
        dn_acc[...] = jnp.zeros_like(dn_acc)
        up_acc[...] = jnp.zeros_like(up_acc)

    for t in range(n_task):
        ebr[t] = et_ref[t:t + 1, :]

    def one_task(t, carry):
        e_row = ebr[t]
        for n in range(0, tile, wide):
            e_n = e_row[:, n:n + wide]
            da = jnp.zeros((width, wide), F32)
            for c, size in cuts:
                d_c = dcol_ref[t, c:c + size, :]
                d_c = jnp.concatenate([d_c] * (wide // LANES), axis=1)
                dz_t = (d_c * e_n).astype(BF16)
                da = da + jnp.dot(w2_ref[:, c:c + size], dz_t, preferred_element_type=F32)
            dat[pl.ds(pl.multiple_of(t * width, width), width), n:n + wide] = (da * gpt_ref[:, n:n + wide]).astype(BF16)
        e_col = jnp.broadcast_to(e_row, (LANES, tile)).T
        for c, size in cuts:
            e_b = e_col
            e_b = jnp.concatenate([e_b] * (size // LANES), axis=1)
            dz = (e_b * drow_ref[t, :, c:c + size]).astype(BF16)
            dn_acc[t, :, c:c + size] += jnp.dot(ut_ref[...], dz, preferred_element_type=F32)
        return carry

    lax.fori_loop(0, n_task, one_task, 0)
    rows = 2 * width

    def up_part(m, carry):
        at = pl.ds(pl.multiple_of(m * rows, rows), rows)
        left = dat[at, :]
        for c, size in cuts:
            up_acc[at, c:c + size] += jnp.dot(left, x_ref[:, c:c + size], preferred_element_type=F32)
        return carry

    lax.fori_loop(0, n_task * width // rows, up_part, 0)

    @pl.when(step == pl.num_programs(0) - 1)
    def _():
        one = pltpu.make_async_copy(dn_acc, gdn_ref, out_sem.at[0])
        two = pltpu.make_async_copy(up_acc, gup_ref, out_sem.at[1])
        one.start()
        two.start()
        one.wait()
        two.wait()


def mix_kernel(n_model, win, gdn_ref, gup_ref, a_ref, g1_ref, g2_ref,
               dn_own, dn_far, up_own, up_far, msend, mrecv, g1t, dsem, usem, send_sem, recv_sem):
    me = lax.axis_index("model")
    core = lax.axis_index("data")
    n_task, half, hidden = dn_own.shape
    width = 2 * half
    off = hidden - win
    sem = pltpu.get_barrier_semaphore()

    n_all = 2 * n_model
    slot = me * 2 + core

    def other(k):
        at = lax.rem(slot + k, n_all)
        return peer(lax.div(at, 2), lax.rem(at, 2))

    def tell(k, carry):
        pl.semaphore_signal(sem, inc=1, device_id=other(k), device_id_type=MESH)
        return carry

    lax.fori_loop(1, n_all, tell, 0)
    my_cols = pl.ds(pl.multiple_of(core * off, LANES), win)
    far_cols = pl.ds(pl.multiple_of((1 - core) * off, LANES), win)
    local = []
    for t in range(n_task):
        local.append(pltpu.make_async_copy(
            gdn_ref.at[t, pl.ds(pl.multiple_of(core * half, half), half), :], dn_own.at[t], dsem.at[0, t]))
        local.append(pltpu.make_async_copy(
            gup_ref.at[pl.ds(t * width, width), my_cols], up_own.at[t], usem.at[0, t]))
    for c in local:
        c.start()
    pl.semaphore_wait(sem, n_all - 1)
    far = []
    for t in range(n_task):
        far.append(pltpu.make_async_remote_copy(
            src_ref=gdn_ref.at[t, pl.ds(pl.multiple_of((1 - core) * half, half), half), :], dst_ref=dn_far.at[t],
            send_sem=dsem.at[1, t], recv_sem=dsem.at[2, t], device_id=peer(me, 1 - core), device_id_type=MESH))
        far.append(pltpu.make_async_remote_copy(
            src_ref=gup_ref.at[pl.ds(t * width, width), far_cols], dst_ref=up_far.at[t],
            send_sem=usem.at[1, t], recv_sem=usem.at[2, t], device_id=peer(me, 1 - core), device_id_type=MESH))
    for c in far:
        c.start()
    for c in local:
        c.wait()
    for c in far:
        c.wait()

    pairs = [(t, s) for t in range(n_task) for s in range(t, n_task)]
    lane = lax.broadcasted_iota(jnp.int32, (8, LANES), 1)

    def fold(own, other, r, c, keep, sums):
        rows = pl.ds(pl.multiple_of(r * 8, 8), 8)
        vals = []
        for t in range(n_task):
            v = own[t, rows, c:c + LANES] + other[t, rows, c:c + LANES]
            own[t, rows, c:c + LANES] = v
            vals.append(v if keep is None else jnp.where(keep, v, 0.0))
        return tuple(acc + vals[t] * vals[s] for acc, (t, s) in zip(sums, pairs))

    sums = tuple(jnp.zeros((8, LANES), F32) for _ in pairs)
    for c in range(0, hidden, LANES):
        sums = lax.fori_loop(0, half // 8, functools.partial(
            lambda c, r, s: fold(dn_own, dn_far, r, c, None, s), c), sums)
    first = core * (win - hidden // 2)
    for c in range(0, win, LANES):
        edge = c < win - hidden // 2 or c + LANES > hidden // 2
        keep = (lane + c >= first) & (lane + c < first + hidden // 2) if edge else None
        sums = lax.fori_loop(0, width // 8, functools.partial(
            lambda c, keep, r, s: fold(up_own, up_far, r, c, keep, s), c, keep), sums)

    row = lax.broadcasted_iota(jnp.int32, (8, LANES), 0)
    part = jnp.zeros((8, LANES), F32)
    for acc, (t, s) in zip(sums, pairs):
        total = jnp.sum(jnp.sum(acc, axis=1, keepdims=True), axis=0, keepdims=True)
        here = ((row == t) & (lane == s)) | ((row == s) & (lane == t))
        part = part + jnp.where(here, total, 0.0)
    msend[...] = part

    def send(k, carry):
        pltpu.make_async_remote_copy(
            src_ref=msend, dst_ref=mrecv.at[slot], send_sem=send_sem, recv_sem=recv_sem,
            device_id=other(k), device_id_type=MESH).start()
        return carry

    lax.fori_loop(1, n_all, send, 0)
    pltpu.make_async_copy(msend, mrecv.at[slot], recv_sem).start()
    pltpu.make_async_copy(mrecv, mrecv, recv_sem).wait()
    gram = jnp.sum(mrecv[...], axis=0)

    scale = jnp.sum(jnp.sum(jnp.where(row == lane, gram, 0.0), axis=1, keepdims=True), axis=0, keepdims=True) / n_task
    gram = gram / scale
    w = jnp.where(lane < n_task, 1.0 / n_task, 0.0).astype(F32)

    def eg_pair(i, w):
        v = w[:, 0:1] * 0.0 + jnp.sum(gram * w, axis=1, keepdims=True)
        w_col = jnp.sum(jnp.where(row == lane, w, 0.0), axis=1, keepdims=True)
        w_col = w_col * jnp.exp(-v)
        w_col = w_col / jnp.sum(w_col, axis=0, keepdims=True)
        v = jnp.sum(gram * w_col, axis=0, keepdims=True)
        w_row = jnp.sum(jnp.where(row == lane, w_col, 0.0), axis=0, keepdims=True)
        w_row = w_row * jnp.exp(-v)
        w_row = w_row / jnp.sum(w_row, axis=1, keepdims=True)
        return jnp.broadcast_to(w_row, (8, LANES))

    w = lax.fori_loop(0, STEPS // 2, eg_pair, w)
    a_ref[...] = w
    a = [jnp.sum(jnp.where(lane == t, w, 0.0), axis=1, keepdims=True) for t in range(n_task)]

    for c in range(0, hidden, LANES):
        def body2(r, carry, c=c):
            rows = pl.ds(pl.multiple_of(r * 8, 8), 8)
            total = a[0] * dn_own[0, rows, c:c + LANES]
            for t in range(1, n_task):
                total = total + a[t] * dn_own[t, rows, c:c + LANES]
            g2_ref[rows, c:c + LANES] = total
            return carry
        lax.fori_loop(0, half // 8, body2, 0)
    for c in range(0, win, LANES):
        def body1(r, carry, c=c):
            rows = pl.ds(pl.multiple_of(r * 8, 8), 8)
            total = a[0] * up_own[0, rows, c:c + LANES]
            for t in range(1, n_task):
                total = total + a[t] * up_own[t, rows, c:c + LANES]
            up_far[0, rows, c:c + LANES] = total
            return carry
        lax.fori_loop(0, width // 8, body1, 0)
    for c in range(0, win, LANES):
        g1t[c:c + LANES, :] = up_far[0, :, c:c + LANES].T
    g1_ref[...] = g1t[pl.ds(pl.multiple_of(first, 8), hidden // 2), :]
    sent = mrecv.at[pl.ds(0, n_all - 1)]
    pltpu.make_async_copy(sent, sent, send_sem).wait()


def solution(mesh):
    n_model, n_data = mesh.shape['model'], mesh.shape['data']

    def local_step(tokens, w_up, w_down, task_heads, labels):
        n_tok, hidden = tokens.shape
        n_total = n_tok * n_data
        width = w_up.shape[1]
        n_task = task_heads.shape[0]
        blk = n_tok // n_model
        win = -(-(hidden // 2) // LANES) * LANES
        off = hidden - win
        me = lax.axis_index('model')
        core = lax.axis_index('data')
        any_spec = pl.BlockSpec(memory_space=pl.ANY)
        vmem_spec = pl.BlockSpec(memory_space=pltpu.VMEM)
        big = 60 * 1024 * 1024

        heads = task_heads.astype(F32)
        h_t = jnp.concatenate([task_heads[:, :, 0], task_heads[:, :, 1]], axis=0)
        h_win = lax.dynamic_slice(h_t, (0, core * off), (2 * n_task, win))
        col = lax.broadcasted_iota(jnp.int32, (2 * n_task, win), 1)
        edge = core * (win - hidden // 2)
        h_win = jnp.where((col >= edge) & (col < edge + hidden // 2), h_win, jnp.zeros_like(h_win))
        dma = pltpu.SemaphoreType.DMA
        e_t_shape = jax.ShapeDtypeStruct((n_task, n_tok), F32)
        ut, gpt, e_t = pl.pallas_call(
            functools.partial(forward_kernel, n_model, win, n_total),
            out_shape=(jax.ShapeDtypeStruct((width, n_tok), BF16), jax.ShapeDtypeStruct((width, n_tok), F32), e_t_shape),
            in_specs=[any_spec, vmem_spec, vmem_spec, vmem_spec, vmem_spec],
            out_specs=(any_spec, any_spec, vmem_spec),
            scratch_shapes=[pltpu.VMEM((2, 4 * blk, hidden), BF16), pltpu.VMEM((n_tok, width), BF16),
                            pltpu.VMEM((width, n_tok), BF16), pltpu.VMEM((width, n_tok), F32),
                            pltpu.VMEM((2, 4, blk, 16 * width), BF16), pltpu.VMEM((2, 16, width // 2, win), BF16),
                            pltpu.VMEM((2, blk, win), BF16), pltpu.VMEM((3, 2, blk, win), F32),
                            pltpu.VMEM((2, blk, win), F32), pltpu.VMEM((2, 2, blk, win), F32),
                            pltpu.VMEM((2 * n_task, blk), F32), pltpu.VMEM((2 * n_task, blk), F32),
                            pltpu.VMEM((n_task, blk), F32),
                            dma((2, 4)), dma((2,)), dma, dma((4,)), dma((2, 4, 2)), dma((2, 4, 2)),
                            dma((6,)), dma((6,)), dma((4,)), dma((4,)), dma, dma, dma((3,))],
            compiler_params=pltpu.CompilerParams(collective_id=0, has_side_effects=True, vmem_limit_bytes=big),
            cost_estimate=pl.CostEstimate(flops=4 * n_tok * hidden * width, bytes_accessed=n_tok * hidden * 2,
                                          transcendentals=n_tok * width),
            name='forward')(tokens, w_up.T, w_down, h_win, labels)

        d_row = heads[:, :, 0] - heads[:, :, 1]
        d_col = jnp.broadcast_to(d_row[:, :, None], (n_task, hidden, LANES))
        t_b = min(512, n_tok)
        const2 = lambda i: (0, 0)
        g_dn, g_up = pl.pallas_call(
            grad_kernel,
            out_shape=(jax.ShapeDtypeStruct((n_task, width, hidden), F32),
                       jax.ShapeDtypeStruct((n_task * width, hidden), F32)),
            grid=(n_tok // t_b,),
            in_specs=[pl.BlockSpec((n_task, t_b), lambda i: (0, i)), pl.BlockSpec((width, t_b), lambda i: (0, i)),
                      pl.BlockSpec((width, t_b), lambda i: (0, i)), pl.BlockSpec((t_b, hidden), lambda i: (i, 0)),
                      pl.BlockSpec((width, hidden), const2, pipeline_mode=pl.Buffered(1)),
                      pl.BlockSpec((n_task, 1, hidden), lambda i: (0, 0, 0), pipeline_mode=pl.Buffered(1)),
                      pl.BlockSpec((n_task, hidden, LANES), lambda i: (0, 0, 0), pipeline_mode=pl.Buffered(1))],
            out_specs=(any_spec, any_spec),
            scratch_shapes=[pltpu.VMEM((n_task, width, hidden), F32), pltpu.VMEM((n_task * width, hidden), F32),
                            pltpu.VMEM((n_task, 1, t_b), F32),
                            pltpu.VMEM((n_task * width, t_b), BF16),
                            pltpu.SemaphoreType.DMA((2,))],
            compiler_params=pltpu.CompilerParams(dimension_semantics=('arbitrary',), vmem_limit_bytes=big),
            cost_estimate=pl.CostEstimate(flops=48 * n_tok * hidden * width, bytes_accessed=n_tok * hidden * 2,
                                          transcendentals=0),
            name='task_grads')(e_t, ut, gpt, tokens, w_down, d_row[:, None, :], d_col)

        half = width // 2
        weights, grad_up, grad_down = pl.pallas_call(
            functools.partial(mix_kernel, n_model, win),
            out_shape=(jax.ShapeDtypeStruct((8, LANES), F32), jax.ShapeDtypeStruct((hidden // 2, width), F32),
                       jax.ShapeDtypeStruct((half, hidden), F32)),
            in_specs=[any_spec, any_spec],
            out_specs=(vmem_spec, vmem_spec, vmem_spec),
            scratch_shapes=[pltpu.VMEM((n_task, half, hidden), F32), pltpu.VMEM((n_task, half, hidden), F32),
                            pltpu.VMEM((n_task, width, win), F32), pltpu.VMEM((n_task, width, win), F32),
                            pltpu.VMEM((8, LANES), F32), pltpu.VMEM((2 * n_model, 8, LANES), F32),
                            pltpu.VMEM((win, width), F32),
                            pltpu.SemaphoreType.DMA((3, n_task)), pltpu.SemaphoreType.DMA((3, n_task)),
                            pltpu.SemaphoreType.DMA, pltpu.SemaphoreType.DMA],
            compiler_params=pltpu.CompilerParams(collective_id=2, has_side_effects=True, vmem_limit_bytes=big),
            name='mix')(g_dn, g_up)
        return weights[0, :n_task], grad_up, grad_down

    return jax.shard_map(
        local_step, mesh=mesh,
        in_specs=(P('data', None), P(None, 'model'), P('model', None), P(None, None, None), P(None, 'data')),
        out_specs=(P(None), P('data', 'model'), P(('model', 'data'), None)),
        check_vma=False)
```

```python
import functools

import jax
import jax.numpy as jnp
from jax import lax
from jax.experimental import pallas as pl
from jax.experimental.pallas import tpu as pltpu
from jax.sharding import PartitionSpec as P

STEPS = 20
LANES = 128
MESH = pl.DeviceIdType.MESH
F32 = jnp.float32
BF16 = jnp.bfloat16
C_GELU = 0.7978845608028654
K_GELU = 0.044715
NT = (((1,), (1,)), ((), ()))


def peer(model, data):
    return {"model": model, "data": data}


def ring_barrier(n_model, me_d, pair):
    sem = pltpu.get_barrier_semaphore()
    me = lax.axis_index("model")

    def tell(k, carry):
        pl.semaphore_signal(sem, inc=1, device_id=peer(lax.rem(me + k, n_model), me_d), device_id_type=MESH)
        return carry

    lax.fori_loop(1, n_model, tell, 0)
    if pair:
        pl.semaphore_signal(sem, inc=1, device_id=peer(me, 1 - me_d), device_id_type=MESH)
    return sem, n_model - 1 + (1 if pair else 0)


def forward_kernel(n_model, win, n_total, x_ref, w1t_ref, w2_ref, ht_ref, lab_ref, ut_ref, gpt_ref, et_ref,
                   xbuf, usend, ut_s, gp_s, uslab, wslab, xz, zout, zrelay, zin, lsend, lrecv, esend,
                   xsem, osem, usend_sem, urecv_sem, wsend_sem, wrecv_sem, psend_sem, precv_sem,
                   zsend_sem, zrecv_sem, esend_sem, erecv_sem, lsem):
    me = lax.axis_index("model")
    core = lax.axis_index("data")
    ring = 4
    plane = ring * ring
    n_tok, hidden = x_ref.shape
    blk = n_tok // n_model
    width = w1t_ref.shape[0]
    n_task = lab_ref.shape[0]
    off = hidden - win
    part = width // 2
    px, py, pz = lax.rem(me, ring), lax.rem(lax.div(me, ring), ring), lax.div(me, plane)
    group = lax.div(me, ring)
    n_step = plane
    per = plane // ring

    def at(x, y, z):
        model = lax.rem(z + ring, ring) * plane + lax.rem(y + ring, ring) * ring + lax.rem(x + ring, ring)
        return peer(model, core)

    def remote(src, dst, ssem, rsem, dev):
        return pltpu.make_async_remote_copy(src_ref=src, dst_ref=dst, send_sem=ssem, recv_sem=rsem,
                                            device_id=dev, device_id_type=MESH)

    partner = peer(me, 1 - core)
    sem, count = ring_barrier(n_model, core, True)
    shifts = (2, 1, 3, 0)

    def block_of(i, k):
        sub = lax.div(i, per)
        shift = jnp.where(sub == 0, 2, jnp.where(sub == 1, 1, jnp.where(sub == 2, 3, 0)))
        g = lax.rem(group + lax.rem(i, per) * per + k, plane)
        return sub, g, g * ring + lax.rem(px + shift, ring)

    def fetch(i, slot):
        out = []
        for k in range(per):
            b = block_of(i, k)[2]
            out.append(pltpu.make_async_copy(
                x_ref.at[pl.ds(pl.multiple_of(b * blk, blk), blk), :], xbuf.at[slot, pl.ds(k * blk, blk), :],
                xsem.at[slot, k]))
        return out

    for c in fetch(0, 0):
        c.start()
    w_cols = pl.ds(pl.multiple_of(core * off, LANES), win)
    mine = pl.ds(pl.multiple_of(me * blk, blk), blk)
    own = [pltpu.make_async_copy(x_ref.at[mine, w_cols], xz.at[0], lsem.at[0])]
    coords = ((py, pz), (pz, py))
    for h in range(2):
        c1, c2 = coords[h]
        own.append(pltpu.make_async_copy(w2_ref.at[pl.ds(h * part, part), w_cols],
                                         wslab.at[h, c2 * ring + c1], lsem.at[1 + h]))
    for c in own:
        c.start()

    def near(h, axis, d):
        y_axis = (h == 0) == (axis == 0)
        return at(px, py + d, pz) if y_axis else at(px, py, pz + d)

    def gather_copy(h, stage, way):
        c1, c2 = coords[h]
        d = 1 if way == 0 else -1
        sems = (wsend_sem.at[h, stage, way], wrecv_sem.at[h, stage, way])
        if stage == 0:
            src = w2_ref.at[pl.ds(h * part, part), w_cols]
            return remote(src, wslab.at[h, c2 * ring + c1], *sems, near(h, 0, d))
        if stage == 1:
            piece = c2 * ring + lax.rem(c1 - d + ring, ring)
            ref = wslab.at[h, piece, pl.ds(way * (part // 2), part // 2), :]
            return remote(ref, ref, *sems, near(h, 0, d))
        if stage == 2:
            ref = wslab.at[h, pl.ds(c2 * ring, ring)]
            return remote(ref, ref, *sems, near(h, 1, d))
        ref = wslab.at[h, pl.ds(lax.rem(c2 - d + ring, ring) * ring + way * (ring // 2), ring // 2)]
        return remote(ref, ref, *sems, near(h, 1, d))

    hw = [(h, way) for h in range(2) for way in range(2)]
    pl.semaphore_wait(sem, count)
    far_x = remote(x_ref.at[mine, pl.ds(pl.multiple_of((1 - core) * off, LANES), win)], xz.at[1],
                   psend_sem.at[4], precv_sem.at[4], partner)
    for h, way in hw:
        gather_copy(h, 0, way).start()
    far_x.start()

    def step(i, carry):
        slot = lax.rem(i, 2)

        @pl.when(i + 1 < n_step)
        def _():
            for c in fetch(i + 1, 1 - slot):
                c.start()

        for c in fetch(i, slot):
            c.wait()
        a = lax.dot_general(w1t_ref[...], xbuf[slot], NT, preferred_element_type=F32)
        a2 = a * a
        th = jnp.tanh(C_GELU * (a + K_GELU * (a * a2)))
        cdf = 0.5 * (1.0 + th)
        slope = cdf + a * (0.5 * (1.0 - th * th) * (C_GELU * (1.0 + (3.0 * K_GELU) * a2)))
        u_f = a * cdf
        u_b = u_f.astype(BF16)
        usend[pl.ds(pl.multiple_of(i * per * blk, blk), per * blk), :] = u_f.T.astype(BF16)
        for k in range(per):
            sub, g, b = block_of(i, k)
            cols = pl.ds(pl.multiple_of(b * blk, blk), blk)
            ut_s[:, cols] = u_b[:, k * blk:(k + 1) * blk]
            gp_s[:, cols] = slope[:, k * blk:(k + 1) * blk]
        return carry

    def give(n, carry):
        sub, g, b = block_of(lax.div(n, per), lax.rem(n, per))
        src = usend.at[pl.ds(pl.multiple_of(n * blk, blk), blk), :]
        dst = uslab.at[0, sub, :, pl.ds(pl.multiple_of(group * width, width), width)]

        @pl.when(g != group)
        def _():
            remote(src, dst, usend_sem, urecv_sem.at[sub], peer(g * ring + px, core)).start()

        @pl.when(g == group)
        def _():
            pltpu.make_async_copy(src, dst, urecv_sem.at[sub]).start()
        return carry

    lax.fori_loop(0, n_step // 4, step, 0)
    lax.fori_loop(0, plane, give, 0)
    for h, way in hw:
        gather_copy(h, 0, way).wait_recv()
        gather_copy(h, 1, way).start()
    lax.fori_loop(n_step // 4, n_step // 2, step, 0)
    for c in own:
        c.wait()
    for h, way in hw:
        gather_copy(h, 1, way).wait_recv()
    for h, way in hw:
        gather_copy(h, 2, way).start()
    lax.fori_loop(n_step // 2, n_step, step, 0)
    out_ut = pltpu.make_async_copy(ut_s, ut_ref, osem.at[0])
    out_gp = pltpu.make_async_copy(gp_s, gpt_ref, osem.at[1])
    out_ut.start()
    out_gp.start()
    for h, way in hw:
        gather_copy(h, 2, way).wait_recv()
        gather_copy(h, 3, way).start()
    lax.fori_loop(plane, 4 * plane, give, 0)

    def u_pair(s):
        return remote(uslab.at[0, s], uslab.at[1, s], psend_sem.at[s], precv_sem.at[s], partner)

    def u_arrive(s):
        pltpu.make_async_copy(uslab.at[0, s], uslab.at[0, s], urecv_sem.at[s]).wait()
        u_pair(s).start()

    def z_copy(n):
        left, right = at(px - 1, py, pz), at(px + 1, py, pz)
        src, dst, dev = ((zout.at[0, 0], zrelay.at[0], right), (zout.at[0, 1], zrelay.at[1], left),
                         (zout.at[1], zin.at[0], right), (zout.at[2], zin.at[1], left))[n]
        return remote(src, dst, zsend_sem.at[n], zrecv_sem.at[n], dev)

    def rows_of(g):
        y, z = g % ring, g // ring
        return [(0, z * ring + y), (1, y * ring + z)]

    def partial_z(s, put):
        for c in range(0, win, 256):
            size = min(256, win - c)
            total = jnp.zeros((2 * blk, size), F32)
            for g in range(0, plane, 2):
                left = jnp.concatenate([uslab[q, s, :, g * width:(g + 2) * width] for q in range(2)], axis=0)
                right = jnp.concatenate([wslab[h, j, :, c:c + size] for h, j in rows_of(g) + rows_of(g + 1)], axis=0)
                total = total + jnp.dot(left, right, preferred_element_type=F32)
            put(c, size, total)

    u_arrive(0)
    for h, way in hw:
        gather_copy(h, 3, way).wait_recv()
    u_pair(0).wait_recv()

    def put_far(c, size, total):
        zout[0, 0, :, c:c + size] = total[:blk]
        zout[0, 1, :, c:c + size] = total[blk:]

    partial_z(0, put_far)
    z_copy(0).start()
    z_copy(1).start()
    for s in (1, 2):
        u_arrive(s)
        u_pair(s).wait_recv()
        z_copy(s - 1).wait_recv()

        def put_near(c, size, total, s=s):
            for q in range(2):
                v = total[q * blk:(q + 1) * blk]
                zout[s, q, :, c:c + size] = v + zrelay[q, :, c:c + size] if q == s - 1 else v

        partial_z(s, put_near)
        z_copy(s + 1).start()
    u_arrive(3)
    u_pair(3).wait_recv()
    far_x.wait_recv()
    z_copy(0).wait_send()
    z_copy(1).wait_send()

    def put_own(c, size, total):
        for q in range(2):
            zout[0, q, :, c:c + size] = total[q * blk:(q + 1) * blk]

    partial_z(3, put_own)
    z_copy(2).wait_recv()
    z_copy(3).wait_recv()
    gaps = []
    for q in range(2):
        z = (xz[q].astype(F32) + ((zout[0, q] + zin[0, q]) + zin[1, q])).astype(BF16)
        gaps.append(lax.dot_general(ht_ref[...], z, NT, preferred_element_type=F32))
    lsend[...] = gaps[1]
    swap = remote(lsend, lrecv, psend_sem.at[5], precv_sem.at[5], partner)
    swap.start()
    swap.wait()
    logit = gaps[0] + lrecv[...]
    gap = logit[:n_task, :] - logit[n_task:, :]
    first = lab_ref[:, mine] == 0
    wrong = 1.0 / (1.0 + jnp.exp(jnp.where(first, gap, -gap)))
    esend[...] = jnp.where(first, -wrong, wrong) * (1.0 / n_total)
    dst = et_ref.at[:, pl.ds(pl.multiple_of(me * blk, LANES), blk)]

    def send(k, carry):
        remote(esend, dst, esend_sem, erecv_sem, peer(lax.rem(me + k, n_model), core)).start()
        return carry

    lax.fori_loop(1, n_model, send, 0)
    pltpu.make_async_copy(esend, dst, erecv_sem).start()
    for h, way in hw:
        for stage in range(4):
            gather_copy(h, stage, way).wait_send()
    for s in range(4):
        u_pair(s).wait_send()
    far_x.wait_send()
    z_copy(2).wait_send()
    z_copy(3).wait_send()
    sent = usend.at[pl.ds(0, n_tok - ring * blk), :]
    pltpu.make_async_copy(sent, sent, usend_sem).wait()
    out_ut.wait()
    out_gp.wait()
    pltpu.make_async_copy(et_ref, et_ref, erecv_sem).wait()
    sent = et_ref.at[:, pl.ds(0, (n_model - 1) * blk)]
    pltpu.make_async_copy(sent, sent, esend_sem).wait()


def grad_kernel(et_ref, ut_ref, gpt_ref, x_ref, w2_ref, drow_ref, gdn_ref, gup_ref,
                dn_acc, up_acc, dcol, ebr, dat, out_sem):
    step = pl.program_id(0)
    n_task, tile = et_ref.shape
    width, hidden = w2_ref.shape
    wide = 256
    cuts = [(c, min(wide, hidden - c)) for c in range(0, hidden, wide)]

    @pl.when(step == 0)
    def _():
        dn_acc[...] = jnp.zeros_like(dn_acc)
        up_acc[...] = jnp.zeros_like(up_acc)

        def spread(t, carry):
            dcol[t] = jnp.broadcast_to(drow_ref[t], (LANES, hidden)).T
            return carry

        lax.fori_loop(0, n_task, spread, 0)

    for t in range(n_task):
        ebr[t] = et_ref[t:t + 1, :]

    def pair_of_tasks(m, carry):
        rows = pl.ds(pl.multiple_of(2 * m * width, 2 * width), 2 * width)
        e_cols = []
        for q in range(2):
            t = 2 * m + q
            e_row = ebr[t]
            for n in range(0, tile, wide):
                e_n = e_row[:, n:n + wide]
                da = jnp.zeros((width, wide), F32)
                for c, size in cuts:
                    d_c = dcol[t, c:c + size, :]
                    d_c = jnp.concatenate([d_c] * (wide // LANES), axis=1)
                    dz_t = (d_c * e_n).astype(BF16)
                    da = da + jnp.dot(w2_ref[:, c:c + size], dz_t, preferred_element_type=F32)
                dat[pl.ds(pl.multiple_of(t * width, width), width), n:n + wide] = (
                    da * gpt_ref[:, n:n + wide]).astype(BF16)
        for q in range(2):
            t = 2 * m + q
            e_col = jnp.broadcast_to(ebr[t], (LANES, tile)).T
            for c, size in cuts:
                e_b = jnp.concatenate([e_col] * (size // LANES), axis=1)
                dz = (e_b * drow_ref[t, :, c:c + size]).astype(BF16)
                dn_acc[t, :, c:c + size] += jnp.dot(ut_ref[...], dz, preferred_element_type=F32)
        left = dat[rows, :]
        for c, size in cuts:
            up_acc[rows, c:c + size] += jnp.dot(left, x_ref[:, c:c + size], preferred_element_type=F32)
        return carry

    lax.fori_loop(0, n_task // 2, pair_of_tasks, 0)

    @pl.when(step == pl.num_programs(0) - 1)
    def _():
        one = pltpu.make_async_copy(dn_acc, gdn_ref, out_sem.at[0])
        two = pltpu.make_async_copy(up_acc, gup_ref, out_sem.at[1])
        one.start()
        two.start()
        one.wait()
        two.wait()


def mix_kernel(n_model, win, gdn_ref, gup_ref, a_ref, g1_ref, g2_ref,
               dn_own, dn_far, up_own, up_far, msend, mrecv, g1t, dsem, usem, send_sem, recv_sem):
    me = lax.axis_index("model")
    core = lax.axis_index("data")
    n_task, half, hidden = dn_own.shape
    width = 2 * half
    off = hidden - win
    sem = pltpu.get_barrier_semaphore()

    n_all = 2 * n_model
    slot = me * 2 + core

    def other(k):
        at = lax.rem(slot + k, n_all)
        return peer(lax.div(at, 2), lax.rem(at, 2))

    def tell(k, carry):
        pl.semaphore_signal(sem, inc=1, device_id=other(k), device_id_type=MESH)
        return carry

    lax.fori_loop(1, n_all, tell, 0)
    my_cols = pl.ds(pl.multiple_of(core * off, LANES), win)
    far_cols = pl.ds(pl.multiple_of((1 - core) * off, LANES), win)
    local = []
    for t in range(n_task):
        local.append(pltpu.make_async_copy(
            gdn_ref.at[t, pl.ds(pl.multiple_of(core * half, half), half), :], dn_own.at[t], dsem.at[0, t]))
        local.append(pltpu.make_async_copy(
            gup_ref.at[pl.ds(t * width, width), my_cols], up_own.at[t], usem.at[0, t]))
    for c in local:
        c.start()
    pl.semaphore_wait(sem, n_all - 1)
    far = []
    for t in range(n_task):
        far.append(pltpu.make_async_remote_copy(
            src_ref=gdn_ref.at[t, pl.ds(pl.multiple_of((1 - core) * half, half), half), :], dst_ref=dn_far.at[t],
            send_sem=dsem.at[1, t], recv_sem=dsem.at[2, t], device_id=peer(me, 1 - core), device_id_type=MESH))
        far.append(pltpu.make_async_remote_copy(
            src_ref=gup_ref.at[pl.ds(t * width, width), far_cols], dst_ref=up_far.at[t],
            send_sem=usem.at[1, t], recv_sem=usem.at[2, t], device_id=peer(me, 1 - core), device_id_type=MESH))
    for c in far:
        c.start()
    for c in local:
        c.wait()
    for c in far:
        c.wait()

    pairs = [(t, s) for t in range(n_task) for s in range(t, n_task)]
    lane = lax.broadcasted_iota(jnp.int32, (8, LANES), 1)

    def fold(own, other, r, c, keep, sums):
        rows = pl.ds(pl.multiple_of(r * 8, 8), 8)
        vals = []
        for t in range(n_task):
            v = own[t, rows, c:c + LANES] + other[t, rows, c:c + LANES]
            own[t, rows, c:c + LANES] = v
            vals.append(v if keep is None else jnp.where(keep, v, 0.0))
        return tuple(acc + vals[t] * vals[s] for acc, (t, s) in zip(sums, pairs))

    sums = tuple(jnp.zeros((8, LANES), F32) for _ in pairs)
    for c in range(0, hidden, LANES):
        sums = lax.fori_loop(0, half // 8, functools.partial(
            lambda c, r, s: fold(dn_own, dn_far, r, c, None, s), c), sums)
    first = core * (win - hidden // 2)
    for c in range(0, win, LANES):
        edge = c < win - hidden // 2 or c + LANES > hidden // 2
        keep = (lane + c >= first) & (lane + c < first + hidden // 2) if edge else None
        sums = lax.fori_loop(0, width // 8, functools.partial(
            lambda c, keep, r, s: fold(up_own, up_far, r, c, keep, s), c, keep), sums)

    row = lax.broadcasted_iota(jnp.int32, (8, LANES), 0)
    part = jnp.zeros((8, LANES), F32)
    for acc, (t, s) in zip(sums, pairs):
        total = jnp.sum(jnp.sum(acc, axis=1, keepdims=True), axis=0, keepdims=True)
        here = ((row == t) & (lane == s)) | ((row == s) & (lane == t))
        part = part + jnp.where(here, total, 0.0)
    msend[...] = part

    def send(k, carry):
        pltpu.make_async_remote_copy(
            src_ref=msend, dst_ref=mrecv.at[slot], send_sem=send_sem, recv_sem=recv_sem,
            device_id=other(k), device_id_type=MESH).start()
        return carry

    lax.fori_loop(1, n_all, send, 0)
    pltpu.make_async_copy(msend, mrecv.at[slot], recv_sem).start()
    pltpu.make_async_copy(mrecv, mrecv, recv_sem).wait()
    gram = jnp.sum(mrecv[...], axis=0)

    scale = jnp.sum(jnp.sum(jnp.where(row == lane, gram, 0.0), axis=1, keepdims=True), axis=0, keepdims=True) / n_task
    gram = gram / scale
    w = jnp.where(lane < n_task, 1.0 / n_task, 0.0).astype(F32)

    def eg_pair(i, w):
        v = w[:, 0:1] * 0.0 + jnp.sum(gram * w, axis=1, keepdims=True)
        w_col = jnp.sum(jnp.where(row == lane, w, 0.0), axis=1, keepdims=True)
        w_col = w_col * jnp.exp(-v)
        w_col = w_col / jnp.sum(w_col, axis=0, keepdims=True)
        v = jnp.sum(gram * w_col, axis=0, keepdims=True)
        w_row = jnp.sum(jnp.where(row == lane, w_col, 0.0), axis=0, keepdims=True)
        w_row = w_row * jnp.exp(-v)
        w_row = w_row / jnp.sum(w_row, axis=1, keepdims=True)
        return jnp.broadcast_to(w_row, (8, LANES))

    w = lax.fori_loop(0, STEPS // 2, eg_pair, w)
    a_ref[...] = w
    a = [jnp.sum(jnp.where(lane == t, w, 0.0), axis=1, keepdims=True) for t in range(n_task)]

    for c in range(0, hidden, LANES):
        def body2(r, carry, c=c):
            rows = pl.ds(pl.multiple_of(r * 8, 8), 8)
            total = a[0] * dn_own[0, rows, c:c + LANES]
            for t in range(1, n_task):
                total = total + a[t] * dn_own[t, rows, c:c + LANES]
            g2_ref[rows, c:c + LANES] = total
            return carry
        lax.fori_loop(0, half // 8, body2, 0)
    for c in range(0, win, LANES):
        def body1(r, carry, c=c):
            rows = pl.ds(pl.multiple_of(r * 8, 8), 8)
            total = a[0] * up_own[0, rows, c:c + LANES]
            for t in range(1, n_task):
                total = total + a[t] * up_own[t, rows, c:c + LANES]
            up_far[0, rows, c:c + LANES] = total
            return carry
        lax.fori_loop(0, width // 8, body1, 0)
    for c in range(0, win, LANES):
        g1t[c:c + LANES, :] = up_far[0, :, c:c + LANES].T
    g1_ref[...] = g1t[pl.ds(pl.multiple_of(first, 8), hidden // 2), :]
    sent = mrecv.at[pl.ds(0, n_all - 1)]
    pltpu.make_async_copy(sent, sent, send_sem).wait()


def solution(mesh):
    n_model, n_data = mesh.shape['model'], mesh.shape['data']

    def local_step(tokens, w_up, w_down, task_heads, labels):
        n_tok, hidden = tokens.shape
        n_total = n_tok * n_data
        width = w_up.shape[1]
        n_task = task_heads.shape[0]
        blk = n_tok // n_model
        win = -(-(hidden // 2) // LANES) * LANES
        off = hidden - win
        me = lax.axis_index('model')
        core = lax.axis_index('data')
        any_spec = pl.BlockSpec(memory_space=pl.ANY)
        vmem_spec = pl.BlockSpec(memory_space=pltpu.VMEM)
        big = 60 * 1024 * 1024

        heads = task_heads.astype(F32)
        h_t = jnp.concatenate([task_heads[:, :, 0], task_heads[:, :, 1]], axis=0)
        h_win = lax.dynamic_slice(h_t, (0, core * off), (2 * n_task, win))
        col = lax.broadcasted_iota(jnp.int32, (2 * n_task, win), 1)
        edge = core * (win - hidden // 2)
        h_win = jnp.where((col >= edge) & (col < edge + hidden // 2), h_win, jnp.zeros_like(h_win))
        dma = pltpu.SemaphoreType.DMA
        e_t_shape = jax.ShapeDtypeStruct((n_task, n_tok), F32)
        ut, gpt, e_t = pl.pallas_call(
            functools.partial(forward_kernel, n_model, win, n_total),
            out_shape=(jax.ShapeDtypeStruct((width, n_tok), BF16), jax.ShapeDtypeStruct((width, n_tok), F32), e_t_shape),
            in_specs=[any_spec, vmem_spec, vmem_spec, vmem_spec, vmem_spec],
            out_specs=(any_spec, any_spec, vmem_spec),
            scratch_shapes=[pltpu.VMEM((2, 4 * blk, hidden), BF16), pltpu.VMEM((n_tok, width), BF16),
                            pltpu.VMEM((width, n_tok), BF16), pltpu.VMEM((width, n_tok), F32),
                            pltpu.VMEM((2, 4, blk, 16 * width), BF16), pltpu.VMEM((2, 16, width // 2, win), BF16),
                            pltpu.VMEM((2, blk, win), BF16), pltpu.VMEM((3, 2, blk, win), F32),
                            pltpu.VMEM((2, blk, win), F32), pltpu.VMEM((2, 2, blk, win), F32),
                            pltpu.VMEM((2 * n_task, blk), F32), pltpu.VMEM((2 * n_task, blk), F32),
                            pltpu.VMEM((n_task, blk), F32),
                            dma((2, 4)), dma((2,)), dma, dma((4,)), dma((2, 4, 2)), dma((2, 4, 2)),
                            dma((6,)), dma((6,)), dma((4,)), dma((4,)), dma, dma, dma((3,))],
            compiler_params=pltpu.CompilerParams(collective_id=0, has_side_effects=True, vmem_limit_bytes=big),
            cost_estimate=pl.CostEstimate(flops=4 * n_tok * hidden * width, bytes_accessed=n_tok * hidden * 2,
                                          transcendentals=n_tok * width),
            name='forward')(tokens, w_up.T, w_down, h_win, labels)

        d_row = heads[:, :, 0] - heads[:, :, 1]
        t_b = min(1024, n_tok)
        const2 = lambda i: (0, 0)
        g_dn, g_up = pl.pallas_call(
            grad_kernel,
            out_shape=(jax.ShapeDtypeStruct((n_task, width, hidden), F32),
                       jax.ShapeDtypeStruct((n_task * width, hidden), F32)),
            grid=(n_tok // t_b,),
            in_specs=[pl.BlockSpec((n_task, t_b), lambda i: (0, i)), pl.BlockSpec((width, t_b), lambda i: (0, i)),
                      pl.BlockSpec((width, t_b), lambda i: (0, i)), pl.BlockSpec((t_b, hidden), lambda i: (i, 0)),
                      pl.BlockSpec((width, hidden), const2, pipeline_mode=pl.Buffered(1)),
                      pl.BlockSpec((n_task, 1, hidden), lambda i: (0, 0, 0), pipeline_mode=pl.Buffered(1))],
            out_specs=(any_spec, any_spec),
            scratch_shapes=[pltpu.VMEM((n_task, width, hidden), F32), pltpu.VMEM((n_task * width, hidden), F32),
                            pltpu.VMEM((n_task, hidden, LANES), F32), pltpu.VMEM((n_task, 1, t_b), F32),
                            pltpu.VMEM((n_task * width, t_b), BF16),
                            pltpu.SemaphoreType.DMA((2,))],
            compiler_params=pltpu.CompilerParams(dimension_semantics=('arbitrary',), vmem_limit_bytes=big),
            cost_estimate=pl.CostEstimate(flops=48 * n_tok * hidden * width, bytes_accessed=n_tok * hidden * 2,
                                          transcendentals=0),
            name='task_grads')(e_t, ut, gpt, tokens, w_down, d_row[:, None, :])

        half = width // 2
        weights, grad_up, grad_down = pl.pallas_call(
            functools.partial(mix_kernel, n_model, win),
            out_shape=(jax.ShapeDtypeStruct((8, LANES), F32), jax.ShapeDtypeStruct((hidden // 2, width), F32),
                       jax.ShapeDtypeStruct((half, hidden), F32)),
            in_specs=[any_spec, any_spec],
            out_specs=(vmem_spec, vmem_spec, vmem_spec),
            scratch_shapes=[pltpu.VMEM((n_task, half, hidden), F32), pltpu.VMEM((n_task, half, hidden), F32),
                            pltpu.VMEM((n_task, width, win), F32), pltpu.VMEM((n_task, width, win), F32),
                            pltpu.VMEM((8, LANES), F32), pltpu.VMEM((2 * n_model, 8, LANES), F32),
                            pltpu.VMEM((win, width), F32),
                            pltpu.SemaphoreType.DMA((3, n_task)), pltpu.SemaphoreType.DMA((3, n_task)),
                            pltpu.SemaphoreType.DMA, pltpu.SemaphoreType.DMA],
            compiler_params=pltpu.CompilerParams(collective_id=2, has_side_effects=True, vmem_limit_bytes=big),
            name='mix')(g_dn, g_up)
        return weights[0, :n_task], grad_up, grad_down

    return jax.shard_map(
        local_step, mesh=mesh,
        in_specs=(P('data', None), P(None, 'model'), P('model', None), P(None, None, None), P(None, 'data')),
        out_specs=(P(None), P('data', 'model'), P(('model', 'data'), None)),
        check_vma=False)
```

```python
import functools

import jax
import jax.numpy as jnp
from jax import lax
from jax.experimental import pallas as pl
from jax.experimental.pallas import tpu as pltpu
from jax.sharding import PartitionSpec as P

STEPS = 20
LANES = 128
MESH = pl.DeviceIdType.MESH
F32 = jnp.float32
BF16 = jnp.bfloat16
C_GELU = 0.7978845608028654
K_GELU = 0.044715
NT = (((1,), (1,)), ((), ()))


def peer(model, data):
    return {"model": model, "data": data}


def step_kernel(n_model, win, n_total, x_ref, w1t_ref, w2_ref, ht_ref, lab_ref, drow_ref, a_ref, g1_ref, g2_ref,
                xbuf, usend, ut_s, gp_s, uslab, wslab, xz, zall, lsend, lrecv, esend, et,
                dn_acc, up_acc, dcol, ebr, dat, msend, mrecv, g1t,
                xsem, usend_sem, urecv_sem, wsend_sem, wrecv_sem, psend_sem, precv_sem, zsend_sem, zrecv_sem,
                esend_sem, erecv_sem, lsem, gsend_sem, grecv_sem, msend_sem, mrecv_sem, free_sem):
    me = lax.axis_index("model")
    core = lax.axis_index("data")
    ring = 4
    plane = ring * ring
    n_tok, hidden = x_ref.shape
    blk = n_tok // n_model
    sub_blk = blk // 2
    width = w1t_ref.shape[0]
    half = width // 2
    n_task = lab_ref.shape[0]
    off = hidden - win
    tile = plane * sub_blk
    n_tile = 2 * ring
    n_all = 2 * n_model
    slot_of_me = me * 2 + core
    px, py, pz = lax.rem(me, ring), lax.rem(lax.div(me, ring), ring), lax.div(me, plane)
    group = lax.div(me, ring)
    partner = peer(me, 1 - core)
    wide = 256
    cuts = [(c, min(wide, hidden - c)) for c in range(0, hidden, wide)]

    def at(x, y, z):
        model = lax.rem(z + ring, ring) * plane + lax.rem(y + ring, ring) * ring + lax.rem(x + ring, ring)
        return peer(model, core)

    def remote(src, dst, ssem, rsem, dev):
        return pltpu.make_async_remote_copy(src_ref=src, dst_ref=dst, send_sem=ssem, recv_sem=rsem,
                                            device_id=dev, device_id_type=MESH)

    def other(k):
        dev = lax.rem(slot_of_me + k, n_all)
        return peer(lax.div(dev, 2), lax.rem(dev, 2))

    sem = pltpu.get_barrier_semaphore()

    def tell(k, carry):
        pl.semaphore_signal(sem, inc=1, device_id=other(k), device_id_type=MESH)
        return carry

    lax.fori_loop(1, n_all, tell, 0)

    def block_of(j, k):
        sub = lax.rem(j, ring)
        shift = jnp.where(sub == 0, 2, jnp.where(sub == 1, 1, jnp.where(sub == 2, 3, 0)))
        return lax.rem(group + k, plane) * ring + lax.rem(px + shift, ring)

    def fetch(j, slot):
        def one(k, carry):
            row = block_of(j, k) * blk + lax.div(j, ring) * sub_blk
            pltpu.make_async_copy(x_ref.at[pl.ds(pl.multiple_of(row, sub_blk), sub_blk), :],
                                  xbuf.at[slot, pl.ds(pl.multiple_of(k * sub_blk, sub_blk), sub_blk), :],
                                  xsem.at[slot]).start()
            return carry

        lax.fori_loop(0, plane, one, 0)

    def fetched(slot):
        pltpu.make_async_copy(xbuf.at[slot], xbuf.at[slot], xsem.at[slot]).wait()

    fetch(0, 0)
    w_cols = pl.ds(pl.multiple_of(core * off, LANES), win)
    far_cols = pl.ds(pl.multiple_of((1 - core) * off, LANES), win)
    mine = pl.ds(pl.multiple_of(me * blk, blk), blk)
    own = [pltpu.make_async_copy(x_ref.at[mine, w_cols], xz.at[0], lsem.at[0])]
    coords = ((py, pz), (pz, py))
    for h in range(2):
        c1, c2 = coords[h]
        own.append(pltpu.make_async_copy(w2_ref.at[pl.ds(h * half, half), w_cols],
                                         wslab.at[h, c2 * ring + c1], lsem.at[1 + h]))
    for c in own:
        c.start()

    def near(h, axis, d):
        y_axis = (h == 0) == (axis == 0)
        return at(px, py + d, pz) if y_axis else at(px, py, pz + d)

    def gather_copy(h, stage, way):
        c1, c2 = coords[h]
        d = 1 if way == 0 else -1
        sems = (wsend_sem.at[h, stage, way], wrecv_sem.at[h, stage, way])
        if stage == 0:
            src = w2_ref.at[pl.ds(h * half, half), w_cols]
            return remote(src, wslab.at[h, c2 * ring + c1], *sems, near(h, 0, d))
        if stage == 1:
            piece = c2 * ring + lax.rem(c1 - d + ring, ring)
            ref = wslab.at[h, piece, pl.ds(way * (half // 2), half // 2), :]
            return remote(ref, ref, *sems, near(h, 0, d))
        if stage == 2:
            ref = wslab.at[h, pl.ds(c2 * ring, ring)]
            return remote(ref, ref, *sems, near(h, 1, d))
        ref = wslab.at[h, pl.ds(lax.rem(c2 - d + ring, ring) * ring + way * (ring // 2), ring // 2)]
        return remote(ref, ref, *sems, near(h, 1, d))

    hw = [(h, way) for h in range(2) for way in range(2)]
    dn_acc[...] = jnp.zeros_like(dn_acc)
    up_acc[...] = jnp.zeros_like(up_acc)

    def spread(t, carry):
        dcol[t] = jnp.broadcast_to(drow_ref[t], (LANES, hidden)).T
        return carry

    lax.fori_loop(0, n_task, spread, 0)
    pl.semaphore_wait(sem, n_all - 1)
    far_x = remote(x_ref.at[mine, far_cols], xz.at[1], psend_sem.at[2, 0], precv_sem.at[2, 0], partner)
    for h, way in hw:
        gather_copy(h, 0, way).start()
    far_x.start()

    def forward(j, carry):
        slot = lax.rem(j, 2)

        @pl.when(j + 1 < n_tile)
        def _():
            fetch(j + 1, 1 - slot)

        fetched(slot)
        base = pl.multiple_of(j * tile, tile)
        step = min(512, tile)
        for n in range(0, tile, step):
            a = lax.dot_general(w1t_ref[...], xbuf[slot, n:n + step, :], NT, preferred_element_type=F32)
            a2 = a * a
            th = jnp.tanh(C_GELU * (a + K_GELU * (a * a2)))
            cdf = 0.5 * (1.0 + th)
            slope = cdf + a * (0.5 * (1.0 - th * th) * (C_GELU * (1.0 + (3.0 * K_GELU) * a2)))
            u_f = a * cdf
            ut_s[:, pl.ds(pl.multiple_of(base + n, step), step)] = u_f.astype(BF16)
            gp_s[:, pl.ds(pl.multiple_of(base + n, step), step)] = slope
            usend[pl.ds(pl.multiple_of(base + n, step), step), :] = u_f.T.astype(BF16)
        return carry

    def give(n, carry):
        j = lax.div(n, plane)
        k = lax.rem(n, plane)
        part, sub = lax.div(j, ring), lax.rem(j, ring)
        g = lax.rem(group + k, plane)
        src = usend.at[pl.ds(pl.multiple_of(n * sub_blk, sub_blk), sub_blk), :]
        dst = uslab.at[part, 0, sub, :, pl.ds(pl.multiple_of(group * width, width), width)]

        @pl.when(g != group)
        def _():
            remote(src, dst, usend_sem, urecv_sem.at[part, sub], peer(g * ring + px, core)).start()

        @pl.when(g == group)
        def _():
            pltpu.make_async_copy(src, dst, urecv_sem.at[part, sub]).start()
        return carry

    lax.fori_loop(0, 1, forward, 0)
    lax.fori_loop(0, plane, give, 0)
    for h, way in hw:
        gather_copy(h, 0, way).wait_recv()
        gather_copy(h, 1, way).start()
    lax.fori_loop(1, 2, forward, 0)
    for c in own:
        c.wait()
    for h, way in hw:
        gather_copy(h, 1, way).wait_recv()
    for h, way in hw:
        gather_copy(h, 2, way).start()
    lax.fori_loop(2, n_tile, forward, 0)
    fetch(0, 0)
    for h, way in hw:
        gather_copy(h, 2, way).wait_recv()
        gather_copy(h, 3, way).start()
    lax.fori_loop(plane, ring * plane, give, 0)

    def u_pair(part, s):
        return remote(uslab.at[part, 0, s], uslab.at[part, 1, s], psend_sem.at[part, s], precv_sem.at[part, s], partner)

    def u_arrive(part, s):
        ref = uslab.at[part, 0, s]
        pltpu.make_async_copy(ref, ref, urecv_sem.at[part, s]).wait()
        u_pair(part, s).start()

    def z_out(part, n, q):
        return part * 6 + n * 2 + q

    def z_relay(part, q):
        return 12 + part * 2 + q

    def z_in(part, i, q):
        return 16 + part * 4 + i * 2 + q

    def z_copy(part, n):
        left, right = at(px - 1, py, pz), at(px + 1, py, pz)
        src, dst, dev = ((zall.at[z_out(part, 0, 0)], zall.at[z_relay(part, 0)], right),
                         (zall.at[z_out(part, 0, 1)], zall.at[z_relay(part, 1)], left),
                         (zall.at[pl.ds(z_out(part, 1, 0), 2)], zall.at[pl.ds(z_in(part, 0, 0), 2)], right),
                         (zall.at[pl.ds(z_out(part, 2, 0), 2)], zall.at[pl.ds(z_in(part, 1, 0), 2)], left))[n]
        return remote(src, dst, zsend_sem.at[part, n], zrecv_sem.at[part, n], dev)

    def rows_of(g):
        y, z = g % ring, g // ring
        return [(0, z * ring + y), (1, y * ring + z)]

    def partial_z(part, s, put):
        for c in range(0, win, wide):
            size = min(wide, win - c)
            total = jnp.zeros((2 * sub_blk, size), F32)
            for g in range(0, plane, 2):
                left = jnp.concatenate(
                    [uslab[part, q, s, :, g * width:(g + 2) * width] for q in range(2)], axis=0)
                right = jnp.concatenate([wslab[h, i, :, c:c + size] for h, i in rows_of(g) + rows_of(g + 1)], axis=0)
                total = total + jnp.dot(left, right, preferred_element_type=F32)
            put(c, size, total[:sub_blk], total[sub_blk:])

    def z_far(part):
        u_pair(part, 0).wait_recv()

        def put(c, size, top, low):
            zall[z_out(part, 0, 0), :, c:c + size] = top
            zall[z_out(part, 0, 1), :, c:c + size] = low

        partial_z(part, 0, put)
        z_copy(part, 0).start()
        z_copy(part, 1).start()

    def z_near(part, s):
        u_pair(part, s).wait_recv()
        z_copy(part, s - 1).wait_recv()

        def put(c, size, top, low):
            for q, v in enumerate((top, low)):
                if q == s - 1:
                    v = v + zall[z_relay(part, q), :, c:c + size]
                zall[z_out(part, s, q), :, c:c + size] = v

        partial_z(part, s, put)
        z_copy(part, s + 1).start()

    def z_own(part):
        u_pair(part, 3).wait_recv()
        z_copy(part, 0).wait_send()
        z_copy(part, 1).wait_send()

        def put(c, size, top, low):
            zall[z_out(part, 0, 0), :, c:c + size] = top
            zall[z_out(part, 0, 1), :, c:c + size] = low

        partial_z(part, 3, put)

    pad = jnp.zeros((n_task, LANES - sub_blk), F32)

    def e_out(part):
        z_copy(part, 2).wait_recv()
        z_copy(part, 3).wait_recv()
        z_copy(part, 2).wait_send()
        z_copy(part, 3).wait_send()
        gaps = []
        rows = slice(part * sub_blk, (part + 1) * sub_blk)
        for q in range(2):
            z = (xz[q, rows, :].astype(F32) + ((zall[z_out(part, 0, q)] + zall[z_in(part, 0, q)]) + zall[z_in(part, 1, q)])).astype(BF16)
            gaps.append(lax.dot_general(ht_ref[...], z, NT, preferred_element_type=F32))
        lsend[part] = jnp.concatenate([gaps[1], jnp.concatenate([pad, pad], axis=0)], axis=1)
        swap = remote(lsend.at[part], lrecv.at[part], psend_sem.at[2, 1 + part], precv_sem.at[2, 1 + part], partner)
        swap.start()
        swap.wait()
        logit = gaps[0] + lrecv[part, :, :sub_blk]
        gap = logit[:n_task, :] - logit[n_task:, :]
        first = lab_ref[:, mine][:, rows] == 0
        wrong = 1.0 / (1.0 + jnp.exp(jnp.where(first, gap, -gap)))
        e = jnp.where(first, -wrong, wrong) * (1.0 / n_total)
        esend[part] = jnp.concatenate([e, pad], axis=1)
        dst = et.at[part, me]

        def send(k, carry):
            remote(esend.at[part], dst, esend_sem.at[part], erecv_sem.at[part],
                   peer(lax.rem(me + k, n_model), core)).start()
            return carry

        lax.fori_loop(1, n_model, send, 0)
        pltpu.make_async_copy(esend.at[part], dst, erecv_sem.at[part]).start()

    def e_in(part):
        pltpu.make_async_copy(et.at[part], et.at[part], erecv_sem.at[part]).wait()

    u_arrive(0, 0)
    for h, way in hw:
        gather_copy(h, 3, way).wait_recv()
    z_far(0)
    u_arrive(0, 1)
    z_near(0, 1)
    u_arrive(0, 2)
    z_near(0, 2)
    u_arrive(0, 3)
    lax.fori_loop(ring * plane, n_tile * plane, give, 0)
    far_x.wait_recv()
    z_own(0)
    e_out(0)
    e_in(0)

    def far_down(t):
        rows = pl.ds(pl.multiple_of(lax.rem(t, 2) * half, half), half)
        return gp_s.at[rows, pl.ds(pl.multiple_of(lax.div(t, 2) * hidden, LANES), hidden)]

    def grad_copies(t):
        out = [remote(dn_acc.at[t, pl.ds(pl.multiple_of((1 - core) * half, half), half), :], far_down(t),
                      gsend_sem.at[0, t], grecv_sem.at[0, t], partner)]
        for i in range(2):
            rows = pl.ds(pl.multiple_of(t * width + i * half, half), half)
            out.append(remote(up_acc.at[rows, far_cols], zall.at[2 * t + i],
                              gsend_sem.at[1 + i, t], grecv_sem.at[1 + i, t], partner))
        return out

    def grad_tile(j, carry):
        slot = lax.rem(j, 2)

        @pl.when(j + 1 < n_tile)
        def _():
            fetch(j + 1, 1 - slot)

        @pl.when(j == n_tile - 1)
        def _():
            pl.semaphore_signal(free_sem, inc=1, device_id=partner, device_id_type=MESH)

        part = lax.div(j, ring)
        for k in range(0, plane, 2):
            pieces = [et[part, block_of(j, k + i)][:, :sub_blk] for i in range(2)]
            e_pair = jnp.concatenate(pieces, axis=1)
            for t in range(n_task):
                ebr[t, :, k * sub_blk:(k + 2) * sub_blk] = e_pair[t:t + 1, :]
        fetched(slot)
        base = pl.multiple_of(j * tile, tile)

        def pair_of_tasks(m, carry):
            rows = pl.ds(pl.multiple_of(2 * m * width, 2 * width), 2 * width)
            for q in range(2):
                t = 2 * m + q
                for n in range(0, tile, wide):
                    n_size = min(wide, tile)
                    e_n = ebr[t, :, n:n + n_size]
                    da = jnp.zeros((width, n_size), F32)
                    for c, size in cuts:
                        d_c = jnp.concatenate([dcol[t, c:c + size, :]] * (n_size // LANES), axis=1)
                        dz_t = (d_c * e_n).astype(BF16)
                        da = da + jnp.dot(w2_ref[:, c:c + size], dz_t, preferred_element_type=F32)
                    cols = pl.ds(pl.multiple_of(base + n, n_size), n_size)
                    dat[q * width:(q + 1) * width, n:n + n_size] = (da * gp_s[:, cols]).astype(BF16)
            for q in range(2):
                t = 2 * m + q
                e_col = jnp.broadcast_to(ebr[t], (LANES, tile)).T
                for c, size in cuts:
                    e_b = jnp.concatenate([e_col] * (size // LANES), axis=1)
                    dz = (e_b * drow_ref[t, :, c:c + size]).astype(BF16)
                    dn_acc[t, :, c:c + size] += jnp.dot(ut_s[:, pl.ds(base, tile)], dz, preferred_element_type=F32)
            left = dat[...]
            for c, size in cuts:
                up_acc[rows, c:c + size] += jnp.dot(left, xbuf[slot, :, c:c + size], preferred_element_type=F32)

            @pl.when((j == n_tile - 1) & (m == 0))
            def _():
                pl.semaphore_wait(free_sem, 1)

            @pl.when(j == n_tile - 1)
            def _():
                for q in range(2):
                    for c in grad_copies(2 * m + q):
                        c.start()
            return carry

        lax.fori_loop(0, n_task // 2, pair_of_tasks, 0)

        @pl.when(j == 0)
        def _():
            for s in range(4):
                u_arrive(1, s)
            z_far(1)

        @pl.when(j == 1)
        def _():
            z_near(1, 1)
            z_near(1, 2)
            z_own(1)

        @pl.when(j == 2)
        def _():
            e_out(1)

        @pl.when(j == 3)
        def _():
            e_in(1)
        return carry

    lax.fori_loop(0, n_tile, grad_tile, 0)

    def landed(t, carry):
        for c in grad_copies(t):
            c.wait_recv()
        return carry

    lax.fori_loop(0, n_task, landed, 0)
    pairs = [(t, s) for t in range(n_task) for s in range(t, n_task)]
    lane = lax.broadcasted_iota(jnp.int32, (8, LANES), 1)

    def gram_of(vals, sums):
        return tuple(acc + vals[t] * vals[s] for acc, (t, s) in zip(sums, pairs))

    def down_at(t, r, c):
        return (pl.ds(pl.multiple_of((t % 2) * half + r * 8, 8), 8), slice((t // 2) * hidden + c, (t // 2) * hidden + c + LANES))

    def fold_down(r, sums):
        from_acc = pl.ds(pl.multiple_of(core * half + r * 8, 8), 8)
        for c in range(0, hidden, LANES):
            vals = []
            for t in range(n_task):
                v = dn_acc[t, from_acc, c:c + LANES] + gp_s[down_at(t, r, c)]
                gp_s[down_at(t, r, c)] = v
                vals.append(v)
            sums = gram_of(vals, sums)
        return sums

    first = core * (win - hidden // 2)

    def fold_up(i, r, sums):
        rows = pl.ds(pl.multiple_of(r * 8, 8), 8)
        for c in range(0, win, LANES):
            edge = c < win - hidden // 2 or c + LANES > hidden // 2
            vals = []
            for t in range(n_task):
                v = up_acc[pl.ds(pl.multiple_of(t * width + i * half + r * 8, 8), 8),
                           pl.ds(pl.multiple_of(core * off + c, LANES), LANES)] + zall[2 * t + i, rows, c:c + LANES]
                zall[2 * t + i, rows, c:c + LANES] = v
                vals.append(jnp.where((lane + c >= first) & (lane + c < first + hidden // 2), v, 0.0) if edge else v)
            sums = gram_of(vals, sums)
        return sums

    sums = tuple(jnp.zeros((8, LANES), F32) for _ in pairs)
    sums = lax.fori_loop(0, half // 8, fold_down, sums)
    for i in range(2):
        sums = lax.fori_loop(0, half // 8, functools.partial(fold_up, i), sums)
    lane1 = lax.broadcasted_iota(jnp.int32, (1, LANES), 1)
    row = lax.broadcasted_iota(jnp.int32, (8, LANES), 0)
    out = jnp.zeros((1, LANES), F32)
    for acc, (t, s) in zip(sums, pairs):
        total = jnp.sum(jnp.sum(acc, axis=0, keepdims=True), axis=1, keepdims=True)
        out = out + jnp.where((lane1 == t * n_task + s) | (lane1 == s * n_task + t), total, 0.0)
    msend[...] = out

    def send_gram(k, carry):
        remote(msend, mrecv.at[slot_of_me], msend_sem, mrecv_sem, other(k)).start()
        return carry

    lax.fori_loop(1, n_all, send_gram, 0)
    pltpu.make_async_copy(msend, mrecv.at[slot_of_me], mrecv_sem).start()
    pltpu.make_async_copy(mrecv, mrecv, mrecv_sem).wait()
    flat = jnp.sum(mrecv[...], axis=0)
    gram = jnp.zeros((8, LANES), F32)
    for t in range(n_task):
        line = flat if t == 0 else pltpu.roll(flat, LANES - t * n_task, 1)
        gram = gram + jnp.where((row == t) & (lane < n_task), jnp.broadcast_to(line, (8, LANES)), 0.0)
    scale = jnp.sum(jnp.sum(jnp.where(row == lane, gram, 0.0), axis=1, keepdims=True), axis=0, keepdims=True) / n_task
    gram = gram / scale
    w = jnp.where(lane < n_task, 1.0 / n_task, 0.0).astype(F32)

    def eg_pair(i, w):
        v = jnp.sum(gram * w, axis=1, keepdims=True)
        w_col = jnp.sum(jnp.where(row == lane, w, 0.0), axis=1, keepdims=True)
        w_col = w_col * jnp.exp(-v)
        w_col = w_col / jnp.sum(w_col, axis=0, keepdims=True)
        v = jnp.sum(gram * w_col, axis=0, keepdims=True)
        w_row = jnp.sum(jnp.where(row == lane, w_col, 0.0), axis=0, keepdims=True)
        w_row = w_row * jnp.exp(-v)
        w_row = w_row / jnp.sum(w_row, axis=1, keepdims=True)
        return jnp.broadcast_to(w_row, (8, LANES))

    w = lax.fori_loop(0, STEPS // 2, eg_pair, w)
    a_ref[...] = w
    a = [jnp.broadcast_to(jnp.sum(jnp.where(lane == t, w, 0.0), axis=1, keepdims=True), (8, LANES))
         for t in range(n_task)]

    def mix_down(r, carry):
        rows = pl.ds(pl.multiple_of(r * 8, 8), 8)
        for c in range(0, hidden, LANES):
            total = a[0] * gp_s[down_at(0, r, c)]
            for t in range(1, n_task):
                total = total + a[t] * gp_s[down_at(t, r, c)]
            g2_ref[rows, c:c + LANES] = total
        return carry

    last = z_in(0, 0, 0)

    def mix_up(i, r, carry):
        rows = pl.ds(pl.multiple_of(r * 8, 8), 8)
        for c in range(0, win, LANES):
            total = a[0] * zall[i, rows, c:c + LANES]
            for t in range(1, n_task):
                total = total + a[t] * zall[2 * t + i, rows, c:c + LANES]
            zall[last + i, rows, c:c + LANES] = total
        return carry

    lax.fori_loop(0, half // 8, mix_down, 0)
    for i in range(2):
        lax.fori_loop(0, half // 8, functools.partial(mix_up, i), 0)
    for c in range(0, win, LANES):
        g1t[c:c + LANES, :] = jnp.concatenate([zall[last + i, :, c:c + LANES] for i in range(2)], axis=0).T
    g1_ref[...] = g1t[pl.ds(pl.multiple_of(first, 8), hidden // 2), :]

    for h, way in hw:
        for stage in range(4):
            gather_copy(h, stage, way).wait_send()
    for part in range(2):
        for s in range(4):
            u_pair(part, s).wait_send()
        sent = et.at[part, pl.ds(0, n_model - 1)]
        pltpu.make_async_copy(sent, sent, esend_sem.at[part]).wait()
    far_x.wait_send()
    sent = usend.at[pl.ds(0, n_tok - ring * blk), :]
    pltpu.make_async_copy(sent, sent, usend_sem).wait()

    def gone(t, carry):
        for c in grad_copies(t):
            c.wait_send()
        return carry

    lax.fori_loop(0, n_task, gone, 0)
    sent = mrecv.at[pl.ds(0, n_all - 1)]
    pltpu.make_async_copy(sent, sent, msend_sem).wait()


def solution(mesh):
    n_model, n_data = mesh.shape['model'], mesh.shape['data']

    def local_step(tokens, w_up, w_down, task_heads, labels):
        n_tok, hidden = tokens.shape
        n_total = n_tok * n_data
        width = w_up.shape[1]
        n_task = task_heads.shape[0]
        blk = n_tok // n_model
        sub_blk = blk // 2
        half = width // 2
        win = -(-(hidden // 2) // LANES) * LANES
        off = hidden - win
        tile = 16 * sub_blk
        core = lax.axis_index('data')
        any_spec = pl.BlockSpec(memory_space=pl.ANY)
        vmem_spec = pl.BlockSpec(memory_space=pltpu.VMEM)
        heads = task_heads.astype(F32)
        d_row = heads[:, :, 0] - heads[:, :, 1]
        h_t = jnp.concatenate([task_heads[:, :, 0], task_heads[:, :, 1]], axis=0)
        h_win = lax.dynamic_slice(h_t, (0, core * off), (2 * n_task, win))
        col = lax.broadcasted_iota(jnp.int32, (2 * n_task, win), 1)
        edge = core * (win - hidden // 2)
        h_win = jnp.where((col >= edge) & (col < edge + hidden // 2), h_win, jnp.zeros_like(h_win))
        dma = pltpu.SemaphoreType.DMA
        vmem = pltpu.VMEM
        weights, grad_up, grad_down = pl.pallas_call(
            functools.partial(step_kernel, n_model, win, n_total),
            out_shape=(jax.ShapeDtypeStruct((8, LANES), F32), jax.ShapeDtypeStruct((hidden // 2, width), F32),
                       jax.ShapeDtypeStruct((half, hidden), F32)),
            in_specs=[any_spec, vmem_spec, vmem_spec, vmem_spec, vmem_spec, vmem_spec],
            out_specs=(vmem_spec, vmem_spec, vmem_spec),
            scratch_shapes=[vmem((2, tile, hidden), BF16), vmem((n_tok, width), BF16), vmem((width, n_tok), BF16),
                            vmem((width, n_tok), F32), vmem((2, 2, 4, sub_blk, 16 * width), BF16),
                            vmem((2, 16, half, win), BF16), vmem((2, blk, win), BF16),
                            vmem((24, sub_blk, win), F32), vmem((2, 2 * n_task, LANES), F32),
                            vmem((2, 2 * n_task, LANES), F32), vmem((2, n_task, LANES), F32),
                            vmem((2, n_model, n_task, LANES), F32),
                            vmem((n_task, width, hidden), F32), vmem((n_task * width, hidden), F32),
                            vmem((n_task, hidden, LANES), F32), vmem((n_task, 1, tile), F32), vmem((2 * width, tile), BF16),
                            vmem((1, LANES), F32), vmem((2 * n_model, 1, LANES), F32), vmem((win, width), F32),
                            dma((2,)), dma, dma((2, 4)), dma((2, 4, 2)), dma((2, 4, 2)), dma((3, 4)), dma((3, 4)),
                            dma((2, 4)), dma((2, 4)), dma((2,)), dma((2,)), dma((3,)), dma((3, n_task)),
                            dma((3, n_task)), dma, dma, pltpu.SemaphoreType.REGULAR],
            compiler_params=pltpu.CompilerParams(collective_id=0, has_side_effects=True, vmem_limit_bytes=67043328),
            name='step')(tokens, w_up.T, w_down, h_win, labels, d_row[:, None, :])
        return weights[0, :n_task], grad_up, grad_down

    return jax.shard_map(
        local_step, mesh=mesh,
        in_specs=(P('data', None), P(None, 'model'), P('model', None), P(None, None, None), P(None, 'data')),
        out_specs=(P(None), P('data', 'model'), P(('model', 'data'), None)),
        check_vma=False)
```

```python
import functools

import jax
import jax.numpy as jnp
from jax import lax
from jax.experimental import pallas as pl
from jax.experimental.pallas import tpu as pltpu
from jax.sharding import PartitionSpec as P

STEPS = 20
LANES = 128
MESH = pl.DeviceIdType.MESH
F32 = jnp.float32
BF16 = jnp.bfloat16
C_GELU = 0.7978845608028654
K_GELU = 0.044715
NT = (((1,), (1,)), ((), ()))


def peer(model, data):
    return {"model": model, "data": data}


def step_kernel(n_model, win, n_total, x_ref, w1_ref, w2_ref, h_ref, lab_ref, a_ref, g1_ref, g2_ref,
                w1t_ref, ht_ref, drow_ref, xbuf, usend, ut_s, gp_s, uslab, wslab, xz, zall, lown, lsend, lrecv, esend, et,
                dn_acc, up_acc, dcol, ebr, dat, msend, mrecv, g1t,
                xsem, usend_sem, urecv_sem, wsend_sem, wrecv_sem, psend_sem, precv_sem, zsend_sem, zrecv_sem,
                esend_sem, erecv_sem, ssend_sem, srecv_sem, lsem, gsend_sem, grecv_sem, msend_sem, mrecv_sem, free_sem):
    me = lax.axis_index("model")
    core = lax.axis_index("data")
    ring = 4
    plane = ring * ring
    n_tok, hidden = x_ref.shape
    blk = n_tok // n_model
    n_part = 4
    sub_blk = blk // n_part
    width = w1_ref.shape[1]
    half = width // 2
    n_task = lab_ref.shape[0]
    off = hidden - win
    tile = 2 * plane * sub_blk
    n_tile = 2 * n_part
    n_pair = n_task // 2
    n_slot = n_part * 8
    n_all = 2 * n_model
    slot_of_me = me * 2 + core
    px, py, pz = lax.rem(me, ring), lax.rem(lax.div(me, ring), ring), lax.div(me, plane)
    group = lax.div(me, ring)
    partner = peer(me, 1 - core)
    wide = 256
    cuts = [(c, min(wide, hidden - c)) for c in range(0, hidden, wide)]

    def at(x, y, z):
        model = lax.rem(z + ring, ring) * plane + lax.rem(y + ring, ring) * ring + lax.rem(x + ring, ring)
        return peer(model, core)

    def remote(src, dst, ssem, rsem, dev):
        return pltpu.make_async_remote_copy(src_ref=src, dst_ref=dst, send_sem=ssem, recv_sem=rsem,
                                            device_id=dev, device_id_type=MESH)

    def other(k):
        dev = lax.rem(slot_of_me + k, n_all)
        return peer(lax.div(dev, 2), lax.rem(dev, 2))

    sem = pltpu.get_barrier_semaphore()

    def tell(k, carry):
        pl.semaphore_signal(sem, inc=1, device_id=other(k), device_id_type=MESH)
        return carry

    lax.fori_loop(1, n_all, tell, 0)

    def block_of(j, k):
        sub = lax.rem(2 * j + lax.div(k, plane), ring)
        shift = jnp.where(sub == 0, 2, jnp.where(sub == 1, 1, jnp.where(sub == 2, 3, 0)))
        return lax.rem(group + lax.rem(k, plane), plane) * ring + lax.rem(px + shift, ring)

    def fetch(j, slot):
        def one(k, carry):
            row = block_of(j, k) * blk + lax.div(j, 2) * sub_blk
            pltpu.make_async_copy(x_ref.at[pl.ds(pl.multiple_of(row, sub_blk), sub_blk), :],
                                  xbuf.at[slot, pl.ds(pl.multiple_of(k * sub_blk, sub_blk), sub_blk), :],
                                  xsem.at[slot]).start()
            return carry

        lax.fori_loop(0, 2 * plane, one, 0)

    def fetched(slot):
        pltpu.make_async_copy(xbuf.at[slot], xbuf.at[slot], xsem.at[slot]).wait()

    fetch(0, 0)
    w_cols = pl.ds(pl.multiple_of(core * off, LANES), win)
    far_cols = pl.ds(pl.multiple_of((1 - core) * off, LANES), win)
    mine = pl.ds(pl.multiple_of(me * blk, blk), blk)
    own = [pltpu.make_async_copy(x_ref.at[mine, w_cols], xz.at[0], lsem.at[0])]
    coords = ((py, pz), (pz, py))
    for h in range(2):
        c1, c2 = coords[h]
        own.append(pltpu.make_async_copy(w2_ref.at[pl.ds(h * half, half), w_cols],
                                         wslab.at[h, c2 * ring + c1], lsem.at[1 + h]))
    for c in own:
        c.start()

    def near(h, axis, d):
        y_axis = (h == 0) == (axis == 0)
        return at(px, py + d, pz) if y_axis else at(px, py, pz + d)

    def gather_copy(h, stage, way):
        c1, c2 = coords[h]
        d = 1 if way == 0 else -1
        sems = (wsend_sem.at[h, stage, way], wrecv_sem.at[h, stage, way])
        if stage == 0:
            src = w2_ref.at[pl.ds(h * half, half), w_cols]
            return remote(src, wslab.at[h, c2 * ring + c1], *sems, near(h, 0, d))
        if stage == 1:
            piece = c2 * ring + lax.rem(c1 - d + ring, ring)
            ref = wslab.at[h, piece, pl.ds(way * (half // 2), half // 2), :]
            return remote(ref, ref, *sems, near(h, 0, d))
        if stage == 2:
            ref = wslab.at[h, pl.ds(c2 * ring, ring)]
            return remote(ref, ref, *sems, near(h, 1, d))
        ref = wslab.at[h, pl.ds(lax.rem(c2 - d + ring, ring) * ring + way * (ring // 2), ring // 2)]
        return remote(ref, ref, *sems, near(h, 1, d))

    hw = [(h, way) for h in range(2) for way in range(2)]
    dn_acc[...] = jnp.zeros_like(dn_acc)
    up_acc[...] = jnp.zeros_like(up_acc)
    w1t_ref[...] = w1_ref[...].T
    first = core * (win - hidden // 2)
    col = lax.broadcasted_iota(jnp.int32, (2 * n_task, win), 1)
    h_rows = jnp.concatenate([h_ref[t, c:c + 1, w_cols].astype(F32) for c in range(2) for t in range(n_task)], axis=0)
    ht_ref[...] = jnp.where((col >= first) & (col < first + hidden // 2), h_rows, 0.0).astype(BF16)
    for t in range(n_task):
        drow_ref[t] = h_ref[t, 0:1, :].astype(F32) - h_ref[t, 1:2, :].astype(F32)

    def spread(t, carry):
        dcol[t] = jnp.broadcast_to(drow_ref[t], (LANES, hidden)).T
        return carry

    lax.fori_loop(0, n_task, spread, 0)
    pl.semaphore_wait(sem, n_all - 1)
    far_x = remote(x_ref.at[mine, far_cols], xz.at[1], lsem.at[3], lsem.at[4], partner)
    for h, way in hw:
        gather_copy(h, 0, way).start()
    far_x.start()

    def forward(j, carry):
        slot = lax.rem(j, 2)

        @pl.when(j + 1 < n_tile)
        def _():
            fetch(j + 1, 1 - slot)

        fetched(slot)
        base = pl.multiple_of(j * tile, tile)
        step = min(512, tile)
        for n in range(0, tile, step):
            a = lax.dot_general(w1t_ref[...], xbuf[slot, n:n + step, :], NT, preferred_element_type=F32)
            a2 = a * a
            th = jnp.tanh(C_GELU * (a + K_GELU * (a * a2)))
            cdf = 0.5 * (1.0 + th)
            slope = cdf + a * (0.5 * (1.0 - th * th) * (C_GELU * (1.0 + (3.0 * K_GELU) * a2)))
            u_f = a * cdf
            ut_s[:, pl.ds(pl.multiple_of(base + n, step), step)] = u_f.astype(BF16)
            gp_s[:, pl.ds(pl.multiple_of(base + n, step), step)] = slope
            usend[pl.ds(pl.multiple_of(base + n, step), step), :] = u_f.T.astype(BF16)
        return carry

    def give(n, carry):
        run = lax.div(n, plane)
        part, sub = lax.div(run, ring), lax.rem(run, ring)
        g = lax.rem(group + lax.rem(n, plane), plane)
        src = usend.at[pl.ds(pl.multiple_of(n * sub_blk, sub_blk), sub_blk), :]
        dst = uslab.at[part, 0, sub, :, pl.ds(pl.multiple_of(group * width, width), width)]

        @pl.when(g != group)
        def _():
            remote(src, dst, usend_sem, urecv_sem.at[part, sub], peer(g * ring + px, core)).start()

        @pl.when(g == group)
        def _():
            pltpu.make_async_copy(src, dst, urecv_sem.at[part, sub]).start()
        return carry

    def give_part(part):
        lax.fori_loop(part * (ring * plane), (part + 1) * (ring * plane), give, 0)

    lax.fori_loop(0, 1, forward, 0)
    lax.fori_loop(0, 2 * plane, give, 0)
    for h, way in hw:
        gather_copy(h, 0, way).wait_recv()
        gather_copy(h, 1, way).start()
    lax.fori_loop(1, 2, forward, 0)
    lax.fori_loop(2 * plane, 4 * plane, give, 0)
    for c in own:
        c.wait()
    for h, way in hw:
        gather_copy(h, 1, way).wait_recv()
    for h, way in hw:
        gather_copy(h, 2, way).start()
    lax.fori_loop(2, n_tile, forward, 0)
    fetch(0, 0)
    for h, way in hw:
        gather_copy(h, 2, way).wait_recv()
        gather_copy(h, 3, way).start()
    give_part(1)

    def u_pair(part, s):
        return remote(uslab.at[part, 0, s], uslab.at[part, 1, s], psend_sem.at[part, s], precv_sem.at[part, s], partner)

    def u_arrive(part, s):
        ref = uslab.at[part, 0, s]
        pltpu.make_async_copy(ref, ref, urecv_sem.at[part, s]).wait()
        u_pair(part, s).start()

    def z_out(part, n, q):
        return part * 8 + n * 2 + q

    def z_relay(part, q):
        return n_slot + part * 2 + q

    def z_in(part, i, q):
        return n_slot + 2 * n_part + part * 4 + i * 2 + q

    def z_copy(part, n):
        left, right = at(px - 1, py, pz), at(px + 1, py, pz)
        src, dst, dev = ((zall.at[z_out(part, 0, 0)], zall.at[z_relay(part, 0)], right),
                         (zall.at[z_out(part, 0, 1)], zall.at[z_relay(part, 1)], left),
                         (zall.at[pl.ds(z_out(part, 1, 0), 2)], zall.at[pl.ds(z_in(part, 0, 0), 2)], right),
                         (zall.at[pl.ds(z_out(part, 2, 0), 2)], zall.at[pl.ds(z_in(part, 1, 0), 2)], left))[n]
        return remote(src, dst, zsend_sem.at[part, n], zrecv_sem.at[part, n], dev)

    def rows_of(g):
        y, z = g % ring, g // ring
        return [(0, z * ring + y), (1, y * ring + z)]

    def partial_z(part, subs, relayed):
        for c in range(0, win, wide):
            size = min(wide, win - c)
            total = jnp.zeros((2 * len(subs) * sub_blk, size), F32)
            for g in range(0, plane, 2):
                left = jnp.concatenate(
                    [uslab[part, q, s, :, g * width:(g + 2) * width] for s in subs for q in range(2)], axis=0)
                right = jnp.concatenate([wslab[h, i, :, c:c + size] for h, i in rows_of(g) + rows_of(g + 1)], axis=0)
                total = total + jnp.dot(left, right, preferred_element_type=F32)
            for i, s in enumerate(subs):
                for q in range(2):
                    v = total[(2 * i + q) * sub_blk:(2 * i + q + 1) * sub_blk]
                    if relayed and q == s - 1:
                        v = v + zall[z_relay(part, q), :, c:c + size]
                    zall[z_out(part, s, q), :, c:c + size] = v

    def z_first(s):
        u_pair(0, s).wait_recv()
        if s in (1, 2):
            z_copy(0, s - 1).wait_recv()
        partial_z(0, (s,), True)
        for n in ((0, 1), (2,), (3,), ())[s]:
            z_copy(0, n).start()

    def z_all(part):
        for s in range(4):
            u_pair(part, s).wait_recv()
        partial_z(part, (0, 1, 2, 3), False)
        z_copy(part, 0).start()
        z_copy(part, 1).start()

    def z_relay_on(part):
        for q in range(2):
            z_copy(part, q).wait_recv()
            zall[z_out(part, 1 + q, q)] += zall[z_relay(part, q)]
            z_copy(part, 2 + q).start()

    pad = jnp.zeros((n_task, blk - sub_blk), F32)

    def swap(part):
        return remote(lsend.at[part], lrecv.at[part], ssend_sem.at[part], srecv_sem.at[part], partner)

    def e_logits(part):
        z_copy(part, 2).wait_recv()
        z_copy(part, 3).wait_recv()
        for n in range(4):
            z_copy(part, n).wait_send()
        gaps = []
        rows = pl.ds(pl.multiple_of(part * sub_blk, sub_blk), sub_blk)
        for q in range(2):
            z = (xz[q, rows, :].astype(F32) + ((zall[z_out(part, 3, q)] + zall[z_in(part, 0, q)])
                                               + zall[z_in(part, 1, q)])).astype(BF16)
            gaps.append(lax.dot_general(ht_ref[...], z, NT, preferred_element_type=F32))
        both = jnp.concatenate([pad, pad], axis=0)
        lown[part] = jnp.concatenate([gaps[0], both], axis=1)
        lsend[part] = jnp.concatenate([gaps[1], both], axis=1)
        swap(part).start()

    def e_out(part):
        swap(part).wait()
        logit = lown[part] + lrecv[part]
        gap = logit[:n_task, :] - logit[n_task:, :]
        first_class = pltpu.roll(lab_ref[:, mine], lax.rem(blk - part * sub_blk, blk), 1) == 0
        wrong = 1.0 / (1.0 + jnp.exp(jnp.where(first_class, gap, -gap)))
        esend[part] = jnp.where(first_class, -wrong, wrong) * (1.0 / n_total)
        dst = et.at[part, me]

        def send(k, carry):
            remote(esend.at[part], dst, esend_sem.at[part], erecv_sem.at[part],
                   peer(lax.rem(me + k, n_model), core)).start()
            return carry

        lax.fori_loop(1, n_model, send, 0)
        pltpu.make_async_copy(esend.at[part], dst, erecv_sem.at[part]).start()

    def e_in(part):
        pltpu.make_async_copy(et.at[part], et.at[part], erecv_sem.at[part]).wait()

    def u_in(part):
        for s in range(4):
            u_arrive(part, s)

    u_in(0)
    for h, way in hw:
        gather_copy(h, 3, way).wait_recv()
    for s in range(4):
        z_first(s)
    u_in(1)
    far_x.wait_recv()
    e_logits(0)
    e_out(0)
    z_all(1)

    def far_down(t):
        rows = pl.ds(pl.multiple_of(lax.rem(t, 2) * half, half), half)
        return gp_s.at[rows, pl.ds(pl.multiple_of(lax.div(t, 2) * hidden, LANES), hidden)]

    def grad_copies(t):
        out = [remote(dn_acc.at[t, pl.ds(pl.multiple_of((1 - core) * half, half), half), :], far_down(t),
                      gsend_sem.at[0, t], grecv_sem.at[0, t], partner)]
        for i in range(n_part):
            rows = pl.ds(pl.multiple_of(t * width + i * sub_blk, sub_blk), sub_blk)
            out.append(remote(up_acc.at[rows, far_cols], zall.at[n_part * t + i],
                              gsend_sem.at[1, t], grecv_sem.at[1, t], partner))
        return out

    def grad_tile(j, carry):
        slot = lax.rem(j, 2)

        @pl.when(j + 1 < n_tile)
        def _():
            fetch(j + 1, 1 - slot)

        @pl.when(j == n_tile - 1)
        def _():
            pl.semaphore_signal(free_sem, inc=1, device_id=partner, device_id_type=MESH)

        part = lax.div(j, 2)

        @pl.when(lax.rem(j, 2) == 0)
        def _():
            e_in(part)

        for k in range(0, 2 * plane, n_part):
            pieces = [et[part, block_of(j, k + i)][:, :sub_blk] for i in range(n_part)]
            e_pair = jnp.concatenate(pieces, axis=1)
            for t in range(n_task):
                ebr[t, :, k * sub_blk:(k + n_part) * sub_blk] = e_pair[t:t + 1, :]
        fetched(slot)
        base = pl.multiple_of(j * tile, tile)

        def pair_of_tasks(m, carry):
            rows = pl.ds(pl.multiple_of(2 * m * width, 2 * width), 2 * width)
            for q in range(2):
                t = 2 * m + q
                for n in range(0, tile, wide):
                    n_size = min(wide, tile)
                    e_n = ebr[t, :, n:n + n_size]
                    da = jnp.zeros((width, n_size), F32)
                    for c, size in cuts:
                        d_c = jnp.concatenate([dcol[t, c:c + size, :]] * (n_size // LANES), axis=1)
                        dz_t = (d_c * e_n).astype(BF16)
                        da = da + jnp.dot(w2_ref[:, c:c + size], dz_t, preferred_element_type=F32)
                    cols = pl.ds(pl.multiple_of(base + n, n_size), n_size)
                    dat[q * width:(q + 1) * width, n:n + n_size] = (da * gp_s[:, cols]).astype(BF16)
            for q in range(2):
                t = 2 * m + q
                e_col = jnp.broadcast_to(ebr[t], (LANES, tile)).T
                for c, size in cuts:
                    e_b = jnp.concatenate([e_col] * (size // LANES), axis=1)
                    dz = (e_b * drow_ref[t, :, c:c + size]).astype(BF16)
                    dn_acc[t, :, c:c + size] += jnp.dot(ut_s[:, pl.ds(base, tile)], dz, preferred_element_type=F32)
            left = dat[...]
            for c, size in cuts:
                up_acc[rows, c:c + size] += jnp.dot(left, xbuf[slot, :, c:c + size], preferred_element_type=F32)

            @pl.when((j == n_tile - 1) & (m == 0))
            def _():
                pl.semaphore_wait(free_sem, 1)

            @pl.when(j == n_tile - 1)
            def _():
                for q in range(2):
                    for c in grad_copies(2 * m + q):
                        c.start()
            hook = lax.rem(j, 2) * n_pair + m
            ahead = part + 1

            @pl.when((hook == 0) & (ahead < n_part))
            def _():
                z_relay_on(ahead)

            @pl.when((hook == 0) & (ahead + 1 < n_part))
            def _():
                give_part(ahead + 1)

            @pl.when((hook == 3) & (ahead < n_part))
            def _():
                e_logits(ahead)

            @pl.when((hook == 4) & (ahead < n_part))
            def _():
                e_out(ahead)

            @pl.when((hook == 5) & (ahead + 1 < n_part))
            def _():
                u_in(ahead + 1)

            @pl.when((hook == 6) & (ahead + 1 < n_part))
            def _():
                z_all(ahead + 1)
            return carry

        lax.fori_loop(0, n_pair, pair_of_tasks, 0)
        return carry

    lax.fori_loop(0, n_tile, grad_tile, 0)

    def up_slots(t):
        return zall.at[pl.ds(pl.multiple_of(n_part * t, n_part), n_part)]

    def landed(t, carry):
        grad_copies(t)[0].wait_recv()
        pltpu.make_async_copy(up_slots(t), up_slots(t), grecv_sem.at[1, t]).wait()
        return carry

    lax.fori_loop(0, n_task, landed, 0)
    pairs = [(t, s) for t in range(n_task) for s in range(t, n_task)]
    lane = lax.broadcasted_iota(jnp.int32, (8, LANES), 1)

    def gram_of(vals, sums):
        return tuple(acc + vals[t] * vals[s] for acc, (t, s) in zip(sums, pairs))

    def down_at(t, r, c):
        return (pl.ds(pl.multiple_of((t % 2) * half + r * 8, 8), 8), slice((t // 2) * hidden + c, (t // 2) * hidden + c + LANES))

    def fold_down(r, sums):
        from_acc = pl.ds(pl.multiple_of(core * half + r * 8, 8), 8)
        for c in range(0, hidden, LANES):
            vals = []
            for t in range(n_task):
                v = dn_acc[t, from_acc, c:c + LANES] + gp_s[down_at(t, r, c)]
                gp_s[down_at(t, r, c)] = v
                vals.append(v)
            sums = gram_of(vals, sums)
        return sums

    n_row = sub_blk // 8

    def fold_up(n, sums):
        i, r = lax.div(n, n_row), lax.rem(n, n_row)
        rows = pl.ds(pl.multiple_of(r * 8, 8), 8)
        for c in range(0, win, LANES):
            edge = c < win - hidden // 2 or c + LANES > hidden // 2
            vals = []
            for t in range(n_task):
                v = up_acc[pl.ds(pl.multiple_of(t * width + n * 8, 8), 8),
                           pl.ds(pl.multiple_of(core * off + c, LANES), LANES)] + zall[n_part * t + i, rows, c:c + LANES]
                zall[n_part * t + i, rows, c:c + LANES] = v
                vals.append(jnp.where((lane + c >= first) & (lane + c < first + hidden // 2), v, 0.0) if edge else v)
            sums = gram_of(vals, sums)
        return sums

    sums = tuple(jnp.zeros((8, LANES), F32) for _ in pairs)
    sums = lax.fori_loop(0, half // 8, fold_down, sums)
    sums = lax.fori_loop(0, width // 8, fold_up, sums)
    lane1 = lax.broadcasted_iota(jnp.int32, (1, LANES), 1)
    row = lax.broadcasted_iota(jnp.int32, (8, LANES), 0)
    out = jnp.zeros((1, LANES), F32)
    for acc, (t, s) in zip(sums, pairs):
        total = jnp.sum(jnp.sum(acc, axis=0, keepdims=True), axis=1, keepdims=True)
        out = out + jnp.where((lane1 == t * n_task + s) | (lane1 == s * n_task + t), total, 0.0)
    msend[...] = out

    def send_gram(k, carry):
        remote(msend, mrecv.at[slot_of_me], msend_sem, mrecv_sem, other(k)).start()
        return carry

    lax.fori_loop(1, n_all, send_gram, 0)
    pltpu.make_async_copy(msend, mrecv.at[slot_of_me], mrecv_sem).start()
    pltpu.make_async_copy(mrecv, mrecv, mrecv_sem).wait()
    flat = jnp.sum(mrecv[...], axis=0)
    gram = jnp.zeros((8, LANES), F32)
    for t in range(n_task):
        line = flat if t == 0 else pltpu.roll(flat, LANES - t * n_task, 1)
        gram = gram + jnp.where((row == t) & (lane < n_task), jnp.broadcast_to(line, (8, LANES)), 0.0)
    scale = jnp.sum(jnp.sum(jnp.where(row == lane, gram, 0.0), axis=1, keepdims=True), axis=0, keepdims=True) / n_task
    gram = gram / scale
    w = jnp.where(lane < n_task, 1.0 / n_task, 0.0).astype(F32)

    def eg_pair(i, w):
        v = jnp.sum(gram * w, axis=1, keepdims=True)
        w_col = jnp.sum(jnp.where(row == lane, w, 0.0), axis=1, keepdims=True)
        w_col = w_col * jnp.exp(-v)
        w_col = w_col / jnp.sum(w_col, axis=0, keepdims=True)
        v = jnp.sum(gram * w_col, axis=0, keepdims=True)
        w_row = jnp.sum(jnp.where(row == lane, w_col, 0.0), axis=0, keepdims=True)
        w_row = w_row * jnp.exp(-v)
        w_row = w_row / jnp.sum(w_row, axis=1, keepdims=True)
        return jnp.broadcast_to(w_row, (8, LANES))

    w = lax.fori_loop(0, STEPS // 2, eg_pair, w)
    a_ref[...] = w
    a = [jnp.broadcast_to(jnp.sum(jnp.where(lane == t, w, 0.0), axis=1, keepdims=True), (8, LANES))
         for t in range(n_task)]

    def mix_down(r, carry):
        rows = pl.ds(pl.multiple_of(r * 8, 8), 8)
        for c in range(0, hidden, LANES):
            total = a[0] * gp_s[down_at(0, r, c)]
            for t in range(1, n_task):
                total = total + a[t] * gp_s[down_at(t, r, c)]
            g2_ref[rows, c:c + LANES] = total
        return carry

    last = z_in(0, 0, 0)

    def mix_up(n, carry):
        i, r = lax.div(n, n_row), lax.rem(n, n_row)
        rows = pl.ds(pl.multiple_of(r * 8, 8), 8)
        for c in range(0, win, LANES):
            total = a[0] * zall[i, rows, c:c + LANES]
            for t in range(1, n_task):
                total = total + a[t] * zall[n_part * t + i, rows, c:c + LANES]
            zall[last + i, rows, c:c + LANES] = total
        return carry

    lax.fori_loop(0, half // 8, mix_down, 0)
    lax.fori_loop(0, width // 8, mix_up, 0)
    for c in range(0, win, LANES):
        g1t[c:c + LANES, :] = jnp.concatenate([zall[last + i, :, c:c + LANES] for i in range(n_part)], axis=0).T
    g1_ref[...] = g1t[pl.ds(pl.multiple_of(first, 8), hidden // 2), :]

    for h, way in hw:
        for stage in range(4):
            gather_copy(h, stage, way).wait_send()
    for part in range(n_part):
        for s in range(4):
            u_pair(part, s).wait_send()
        sent = et.at[part, pl.ds(0, n_model - 1)]
        pltpu.make_async_copy(sent, sent, esend_sem.at[part]).wait()
    far_x.wait_send()
    sent = usend.at[pl.ds(0, n_tok - ring * blk), :]
    pltpu.make_async_copy(sent, sent, usend_sem).wait()

    def gone(t, carry):
        grad_copies(t)[0].wait_send()
        pltpu.make_async_copy(up_slots(t), up_slots(t), gsend_sem.at[1, t]).wait()
        return carry

    lax.fori_loop(0, n_task, gone, 0)
    sent = mrecv.at[pl.ds(0, n_all - 1)]
    pltpu.make_async_copy(sent, sent, msend_sem).wait()


def solution(mesh):
    n_model, n_data = mesh.shape['model'], mesh.shape['data']

    def local_step(tokens, w_up, w_down, task_heads, labels):
        n_tok, hidden = tokens.shape
        n_total = n_tok * n_data
        width = w_up.shape[1]
        n_task = task_heads.shape[0]
        blk = n_tok // n_model
        sub_blk = blk // 4
        half = width // 2
        win = -(-(hidden // 2) // LANES) * LANES
        tile = 32 * sub_blk
        any_spec = pl.BlockSpec(memory_space=pl.ANY)
        vmem_spec = pl.BlockSpec(memory_space=pltpu.VMEM)
        dma = pltpu.SemaphoreType.DMA
        vmem = pltpu.VMEM
        weights, grad_up, grad_down = pl.pallas_call(
            functools.partial(step_kernel, n_model, win, n_total),
            out_shape=(jax.ShapeDtypeStruct((8, LANES), F32), jax.ShapeDtypeStruct((hidden // 2, width), F32),
                       jax.ShapeDtypeStruct((half, hidden), F32)),
            in_specs=[any_spec, vmem_spec, vmem_spec, vmem_spec, vmem_spec],
            out_specs=(vmem_spec, vmem_spec, vmem_spec),
            scratch_shapes=[vmem((width, hidden), BF16), vmem((2 * n_task, win), BF16), vmem((n_task, 1, hidden), F32),
                            vmem((2, tile, hidden), BF16), vmem((n_tok, width), BF16), vmem((width, n_tok), BF16),
                            vmem((width, n_tok), F32), vmem((4, 2, 4, sub_blk, 16 * width), BF16),
                            vmem((2, 16, half, win), BF16), vmem((2, blk, win), BF16),
                            vmem((56, sub_blk, win), F32), vmem((4, 2 * n_task, blk), F32),
                            vmem((4, 2 * n_task, blk), F32), vmem((4, 2 * n_task, blk), F32),
                            vmem((4, n_task, blk), F32), vmem((4, n_model, n_task, blk), F32),
                            vmem((n_task, width, hidden), F32), vmem((n_task * width, hidden), F32),
                            vmem((n_task, hidden, LANES), F32), vmem((n_task, 1, tile), F32), vmem((2 * width, tile), BF16),
                            vmem((1, LANES), F32), vmem((2 * n_model, 1, LANES), F32), vmem((win, width), F32),
                            dma((2,)), dma, dma((4, 4)), dma((2, 4, 2)), dma((2, 4, 2)), dma((4, 4)), dma((4, 4)),
                            dma((4, 4)), dma((4, 4)), dma((4,)), dma((4,)), dma((4,)), dma((4,)), dma((5,)),
                            dma((2, n_task)), dma((2, n_task)), dma, dma, pltpu.SemaphoreType.REGULAR],
            compiler_params=pltpu.CompilerParams(collective_id=0, has_side_effects=True, vmem_limit_bytes=67043328),
            name='step')(tokens, w_up, w_down, jnp.transpose(task_heads, (0, 2, 1)), labels)
        return weights[0, :n_task], grad_up, grad_down

    return jax.shard_map(
        local_step, mesh=mesh,
        in_specs=(P('data', None), P(None, 'model'), P('model', None), P(None, None, None), P(None, 'data')),
        out_specs=(P(None), P('data', 'model'), P(('model', 'data'), None)),
        check_vma=False)
```

```python
import functools

import jax
import jax.numpy as jnp
from jax import lax
from jax.experimental import pallas as pl
from jax.experimental.pallas import tpu as pltpu
from jax.sharding import PartitionSpec as P

STEPS = 20
LANES = 128
MESH = pl.DeviceIdType.MESH
F32 = jnp.float32
BF16 = jnp.bfloat16
C_GELU = 0.7978845608028654
K_GELU = 0.044715
NT = (((1,), (1,)), ((), ()))


def peer(model, data):
    return {"model": model, "data": data}


def step_kernel(n_model, win, n_total, x_ref, w1_ref, w2_ref, h_ref, lab_ref, a_ref, g1_ref, g2_ref,
                w1t_ref, ht_ref, drow_ref, xbuf, usend, ut_s, gp_s, uslab, wslab, xz, zall, lown, lsend, lrecv, esend, et,
                dn_acc, up_acc, dcol, ebr, dat, msend, mrecv, g1t,
                xsem, usend_sem, urecv_sem, wsend_sem, wrecv_sem, psend_sem, precv_sem, zsend_sem, zrecv_sem,
                esend_sem, erecv_sem, ssend_sem, srecv_sem, lsem, gsend_sem, grecv_sem, msend_sem, mrecv_sem, free_sem):
    me = lax.axis_index("model")
    core = lax.axis_index("data")
    ring = 4
    plane = ring * ring
    n_tok, hidden = x_ref.shape
    blk = n_tok // n_model
    n_part = 4
    sub_blk = blk // n_part
    width = w1_ref.shape[1]
    half = width // 2
    n_task = lab_ref.shape[0]
    off = hidden - win
    tile = 2 * plane * sub_blk
    n_tile = 2 * n_part
    body_tasks = 4
    n_body = n_task // body_tasks
    n_slot = n_part * 8
    n_all = 2 * n_model
    slot_of_me = me * 2 + core
    px, py, pz = lax.rem(me, ring), lax.rem(lax.div(me, ring), ring), lax.div(me, plane)
    group = lax.div(me, ring)
    partner = peer(me, 1 - core)
    wide = 256
    cuts = [(c, min(wide, hidden - c)) for c in range(0, hidden, wide)]

    def at(x, y, z):
        model = lax.rem(z + ring, ring) * plane + lax.rem(y + ring, ring) * ring + lax.rem(x + ring, ring)
        return peer(model, core)

    def remote(src, dst, ssem, rsem, dev):
        return pltpu.make_async_remote_copy(src_ref=src, dst_ref=dst, send_sem=ssem, recv_sem=rsem,
                                            device_id=dev, device_id_type=MESH)

    def chip(k):
        z, y, x = [lax.rem(lax.div(k, n), ring) for n in (plane, ring, 1)]
        z, y, x = [jnp.where(v == 0, 2, jnp.where(v == 1, 1, jnp.where(v == 2, 3, 0))) for v in (z, y, x)]
        return (lax.rem(pz + z, ring) * plane + lax.rem(py + y, ring) * ring + lax.rem(px + x, ring))

    def other(k):
        return peer(chip(lax.div(k, 2)), lax.rem(core + 1 + lax.rem(k, 2), 2))

    sem = pltpu.get_barrier_semaphore()

    def tell(k, carry):
        pl.semaphore_signal(sem, inc=1, device_id=other(k), device_id_type=MESH)
        return carry

    lax.fori_loop(0, n_all - 1, tell, 0)

    def block_of(j, k):
        sub = lax.rem(2 * j + lax.div(k, plane), ring)
        shift = jnp.where(sub == 0, 2, jnp.where(sub == 1, 1, jnp.where(sub == 2, 3, 0)))
        return lax.rem(group + lax.rem(k, plane), plane) * ring + lax.rem(px + shift, ring)

    def fetch(j, slot):
        def one(k, carry):
            row = block_of(j, k) * blk + lax.div(j, 2) * sub_blk
            pltpu.make_async_copy(x_ref.at[pl.ds(pl.multiple_of(row, sub_blk), sub_blk), :],
                                  xbuf.at[slot, pl.ds(pl.multiple_of(k * sub_blk, sub_blk), sub_blk), :],
                                  xsem.at[slot]).start()
            return carry

        lax.fori_loop(0, 2 * plane, one, 0)

    def fetched(slot):
        pltpu.make_async_copy(xbuf.at[slot], xbuf.at[slot], xsem.at[slot]).wait()

    fetch(0, 0)
    w_cols = pl.ds(pl.multiple_of(core * off, LANES), win)
    far_cols = pl.ds(pl.multiple_of((1 - core) * off, LANES), win)
    mine = pl.ds(pl.multiple_of(me * blk, blk), blk)
    own = [pltpu.make_async_copy(x_ref.at[mine, w_cols], xz.at[0], lsem.at[0])]
    coords = ((py, pz), (pz, py))
    for h in range(2):
        c1, c2 = coords[h]
        own.append(pltpu.make_async_copy(w2_ref.at[pl.ds(h * half, half), w_cols],
                                         wslab.at[h, c2 * ring + c1], lsem.at[1 + h]))
    for c in own:
        c.start()

    def near(h, axis, d):
        y_axis = (h == 0) == (axis == 0)
        return at(px, py + d, pz) if y_axis else at(px, py, pz + d)

    def gather_copy(h, stage, way):
        c1, c2 = coords[h]
        d = 1 if way == 0 else -1
        sems = (wsend_sem.at[h, stage, way], wrecv_sem.at[h, stage, way])
        if stage == 0:
            src = w2_ref.at[pl.ds(h * half, half), w_cols]
            return remote(src, wslab.at[h, c2 * ring + c1], *sems, near(h, 0, d))
        if stage == 1:
            piece = c2 * ring + lax.rem(c1 - d + ring, ring)
            ref = wslab.at[h, piece, pl.ds(way * (half // 2), half // 2), :]
            return remote(ref, ref, *sems, near(h, 0, d))
        if stage == 2:
            ref = wslab.at[h, pl.ds(c2 * ring, ring)]
            return remote(ref, ref, *sems, near(h, 1, d))
        ref = wslab.at[h, pl.ds(lax.rem(c2 - d + ring, ring) * ring + way * (ring // 2), ring // 2)]
        return remote(ref, ref, *sems, near(h, 1, d))

    hw = [(h, way) for h in range(2) for way in range(2)]
    dn_acc[...] = jnp.zeros_like(dn_acc)
    up_acc[...] = jnp.zeros_like(up_acc)
    w1t_ref[...] = w1_ref[...].T
    first = core * (win - hidden // 2)
    col = lax.broadcasted_iota(jnp.int32, (2 * n_task, win), 1)
    h_rows = jnp.concatenate([h_ref[t, c:c + 1, w_cols].astype(F32) for c in range(2) for t in range(n_task)], axis=0)
    ht_ref[...] = jnp.where((col >= first) & (col < first + hidden // 2), h_rows, 0.0).astype(BF16)
    for t in range(n_task):
        drow_ref[t] = h_ref[t, 0:1, :].astype(F32) - h_ref[t, 1:2, :].astype(F32)

    def spread(t, carry):
        dcol[t] = jnp.broadcast_to(drow_ref[t], (LANES, hidden)).T
        return carry

    lax.fori_loop(0, n_task, spread, 0)
    pl.semaphore_wait(sem, n_all - 1)
    far_x = remote(x_ref.at[mine, far_cols], xz.at[1], lsem.at[3], lsem.at[4], partner)
    for h, way in hw:
        gather_copy(h, 0, way).start()
    far_x.start()

    def forward(j, carry):
        slot = lax.rem(j, 2)

        @pl.when(j + 1 < n_tile)
        def _():
            fetch(j + 1, 1 - slot)

        fetched(slot)
        base = pl.multiple_of(j * tile, tile)
        step = min(512, tile)
        for n in range(0, tile, step):
            a = lax.dot_general(w1t_ref[...], xbuf[slot, n:n + step, :], NT, preferred_element_type=F32)
            a2 = a * a
            th = jnp.tanh(C_GELU * (a + K_GELU * (a * a2)))
            cdf = 0.5 * (1.0 + th)
            slope = cdf + a * (0.5 * (1.0 - th * th) * (C_GELU * (1.0 + (3.0 * K_GELU) * a2)))
            u_f = a * cdf
            ut_s[:, pl.ds(pl.multiple_of(base + n, step), step)] = u_f.astype(BF16)
            gp_s[:, pl.ds(pl.multiple_of(base + n, step), step)] = slope
            usend[pl.ds(pl.multiple_of(base + n, step), step), :] = u_f.T.astype(BF16)
        return carry

    def give(n, carry):
        run = lax.div(n, plane)
        part, sub = lax.div(run, ring), lax.rem(run, ring)
        g = lax.rem(group + lax.rem(n, plane), plane)
        src = usend.at[pl.ds(pl.multiple_of(n * sub_blk, sub_blk), sub_blk), :]
        dst = uslab.at[part, 0, sub, :, pl.ds(pl.multiple_of(group * width, width), width)]

        @pl.when(g != group)
        def _():
            remote(src, dst, usend_sem, urecv_sem.at[part, sub], peer(g * ring + px, core)).start()

        @pl.when(g == group)
        def _():
            pltpu.make_async_copy(src, dst, urecv_sem.at[part, sub]).start()
        return carry

    def give_part(part):
        lax.fori_loop(part * (ring * plane), (part + 1) * (ring * plane), give, 0)

    lax.fori_loop(0, 1, forward, 0)
    lax.fori_loop(0, 2 * plane, give, 0)
    for h, way in hw:
        gather_copy(h, 0, way).wait_recv()
        gather_copy(h, 1, way).start()
    lax.fori_loop(1, 2, forward, 0)
    lax.fori_loop(2 * plane, 4 * plane, give, 0)
    for c in own:
        c.wait()
    for h, way in hw:
        gather_copy(h, 1, way).wait_recv()
    for h, way in hw:
        gather_copy(h, 2, way).start()
    lax.fori_loop(2, n_tile, forward, 0)
    fetch(0, 0)
    for h, way in hw:
        gather_copy(h, 2, way).wait_recv()
        gather_copy(h, 3, way).start()
    give_part(1)

    def u_pair(part, s):
        return remote(uslab.at[part, 0, s], uslab.at[part, 1, s], psend_sem.at[part, s], precv_sem.at[part, s], partner)

    def u_arrive(part, s):
        ref = uslab.at[part, 0, s]
        pltpu.make_async_copy(ref, ref, urecv_sem.at[part, s]).wait()
        u_pair(part, s).start()

    def z_out(part, n, q):
        return part * 8 + n * 2 + q

    def z_relay(part, q):
        return n_slot + part * 2 + q

    def z_in(part, i, q):
        return n_slot + 2 * n_part + part * 4 + i * 2 + q

    def z_copy(part, n):
        left, right = at(px - 1, py, pz), at(px + 1, py, pz)
        src, dst, dev = ((zall.at[z_out(part, 0, 0)], zall.at[z_relay(part, 0)], right),
                         (zall.at[z_out(part, 0, 1)], zall.at[z_relay(part, 1)], left),
                         (zall.at[pl.ds(z_out(part, 1, 0), 2)], zall.at[pl.ds(z_in(part, 0, 0), 2)], right),
                         (zall.at[pl.ds(z_out(part, 2, 0), 2)], zall.at[pl.ds(z_in(part, 1, 0), 2)], left))[n]
        return remote(src, dst, zsend_sem.at[part, n], zrecv_sem.at[part, n], dev)

    def rows_of(g):
        y, z = g % ring, g // ring
        return [(0, z * ring + y), (1, y * ring + z)]

    def partial_z(part, subs, relayed):
        for c in range(0, win, wide):
            size = min(wide, win - c)
            total = jnp.zeros((2 * len(subs) * sub_blk, size), F32)
            for g in range(0, plane, 2):
                left = jnp.concatenate(
                    [uslab[part, q, s, :, g * width:(g + 2) * width] for s in subs for q in range(2)], axis=0)
                right = jnp.concatenate([wslab[h, i, :, c:c + size] for h, i in rows_of(g) + rows_of(g + 1)], axis=0)
                total = total + jnp.dot(left, right, preferred_element_type=F32)
            for i, s in enumerate(subs):
                for q in range(2):
                    v = total[(2 * i + q) * sub_blk:(2 * i + q + 1) * sub_blk]
                    if relayed and q == s - 1:
                        v = v + zall[z_relay(part, q), :, c:c + size]
                    zall[z_out(part, s, q), :, c:c + size] = v

    def z_first(s):
        u_pair(0, s).wait_recv()
        if s in (1, 2):
            z_copy(0, s - 1).wait_recv()
        partial_z(0, (s,), True)
        for n in ((0, 1), (2,), (3,), ())[s]:
            z_copy(0, n).start()

    def z_all(part):
        for s in range(4):
            u_pair(part, s).wait_recv()
        partial_z(part, (0, 1, 2, 3), False)
        z_copy(part, 0).start()
        z_copy(part, 1).start()

    def z_relay_on(part):
        for q in range(2):
            z_copy(part, q).wait_recv()
            zall[z_out(part, 1 + q, q)] += zall[z_relay(part, q)]
            z_copy(part, 2 + q).start()

    pad = jnp.zeros((n_task, blk - sub_blk), F32)

    def swap(part):
        return remote(lsend.at[part], lrecv.at[part], ssend_sem.at[part], srecv_sem.at[part], partner)

    def e_logits(part):
        z_copy(part, 2).wait_recv()
        z_copy(part, 3).wait_recv()
        for n in range(4):
            z_copy(part, n).wait_send()
        gaps = []
        rows = pl.ds(pl.multiple_of(part * sub_blk, sub_blk), sub_blk)
        for q in range(2):
            z = (xz[q, rows, :].astype(F32) + ((zall[z_out(part, 3, q)] + zall[z_in(part, 0, q)])
                                               + zall[z_in(part, 1, q)])).astype(BF16)
            gaps.append(lax.dot_general(ht_ref[...], z, NT, preferred_element_type=F32))
        both = jnp.concatenate([pad, pad], axis=0)
        lown[part] = jnp.concatenate([gaps[0], both], axis=1)
        lsend[part] = jnp.concatenate([gaps[1], both], axis=1)
        swap(part).start()

    def e_out(part):
        swap(part).wait()
        logit = lown[part] + lrecv[part]
        gap = logit[:n_task, :] - logit[n_task:, :]
        first_class = pltpu.roll(lab_ref[:, mine], lax.rem(blk - part * sub_blk, blk), 1) == 0
        wrong = 1.0 / (1.0 + jnp.exp(jnp.where(first_class, gap, -gap)))
        esend[part] = jnp.where(first_class, -wrong, wrong) * (1.0 / n_total)
        dst = et.at[part, me]

        def send(k, carry):
            remote(esend.at[part], dst, esend_sem.at[part], erecv_sem.at[part],
                   peer(chip(k), core)).start()
            return carry

        lax.fori_loop(0, n_model - 1, send, 0)
        pltpu.make_async_copy(esend.at[part], dst, erecv_sem.at[part]).start()

    def e_in(part):
        pltpu.make_async_copy(et.at[part], et.at[part], erecv_sem.at[part]).wait()

    def u_in(part):
        for s in range(4):
            u_arrive(part, s)

    u_in(0)
    for h, way in hw:
        gather_copy(h, 3, way).wait_recv()
    for s in range(4):
        z_first(s)
    far_x.wait_recv()
    e_logits(0)
    e_out(0)
    u_in(1)
    z_all(1)
    give_part(2)
    z_relay_on(1)

    def far_down(t):
        rows = pl.ds(pl.multiple_of(lax.rem(t, 2) * half, half), half)
        return gp_s.at[rows, pl.ds(pl.multiple_of(lax.div(t, 2) * hidden, LANES), hidden)]

    def grad_copies(t):
        out = [remote(dn_acc.at[t, pl.ds(pl.multiple_of((1 - core) * half, half), half), :], far_down(t),
                      gsend_sem.at[0, t], grecv_sem.at[0, t], partner)]
        for i in range(n_part):
            rows = pl.ds(pl.multiple_of(t * width + i * sub_blk, sub_blk), sub_blk)
            out.append(remote(up_acc.at[rows, far_cols], zall.at[n_part * t + i],
                              gsend_sem.at[1, t], grecv_sem.at[1, t], partner))
        return out

    def grad_tile(j, carry):
        slot = lax.rem(j, 2)

        @pl.when(j + 1 < n_tile)
        def _():
            fetch(j + 1, 1 - slot)

        @pl.when(j == n_tile - 1)
        def _():
            pl.semaphore_signal(free_sem, inc=1, device_id=partner, device_id_type=MESH)

        part = lax.div(j, 2)

        @pl.when(lax.rem(j, 2) == 0)
        def _():
            e_in(part)

        for k in range(0, 2 * plane, n_part):
            pieces = [et[part, block_of(j, k + i)][:, :sub_blk] for i in range(n_part)]
            e_pair = jnp.concatenate(pieces, axis=1)
            for t in range(n_task):
                ebr[t, :, k * sub_blk:(k + n_part) * sub_blk] = e_pair[t:t + 1, :]
        fetched(slot)
        base = pl.multiple_of(j * tile, tile)

        def some_tasks(m, carry):
            rows = pl.ds(pl.multiple_of(body_tasks * m * width, body_tasks * width), body_tasks * width)
            for q in range(body_tasks):
                t = body_tasks * m + q
                for n in range(0, tile, wide):
                    n_size = min(wide, tile)
                    e_n = ebr[t, :, n:n + n_size]
                    da = jnp.zeros((width, n_size), F32)
                    for c, size in cuts:
                        d_c = jnp.concatenate([dcol[t, c:c + size, :]] * (n_size // LANES), axis=1)
                        dz_t = (d_c * e_n).astype(BF16)
                        da = da + jnp.dot(w2_ref[:, c:c + size], dz_t, preferred_element_type=F32)
                    cols = pl.ds(pl.multiple_of(base + n, n_size), n_size)
                    dat[q * width:(q + 1) * width, n:n + n_size] = (da * gp_s[:, cols]).astype(BF16)
            left = ut_s[:, pl.ds(base, tile)]
            for q in range(0, body_tasks, 2):
                ts = (body_tasks * m + q, body_tasks * m + q + 1)
                e_col = [jnp.broadcast_to(ebr[t], (LANES, tile)).T for t in ts]
                for i, t in enumerate(ts):
                    for c, size in cuts:
                        if size == wide:
                            e_b = jnp.concatenate([e_col[i]] * (size // LANES), axis=1)
                            dz = (e_b * drow_ref[t, :, c:c + size]).astype(BF16)
                            dn_acc[t, :, c:c + size] += jnp.dot(left, dz, preferred_element_type=F32)
                c, size = cuts[-1]
                if size < wide:
                    dz = jnp.concatenate([e_col[i] * drow_ref[t, :, c:c + size] for i, t in enumerate(ts)],
                                         axis=1).astype(BF16)
                    both = jnp.dot(left, dz, preferred_element_type=F32)
                    for i, t in enumerate(ts):
                        dn_acc[t, :, c:c + size] += both[:, i * size:(i + 1) * size]
            left = dat[...]
            for c, size in cuts:
                up_acc[rows, c:c + size] += jnp.dot(left, xbuf[slot, :, c:c + size], preferred_element_type=F32)

            @pl.when((j == n_tile - 1) & (m == 0))
            def _():
                pl.semaphore_wait(free_sem, 1)

            @pl.when(j == n_tile - 1)
            def _():
                for q in range(body_tasks):
                    for c in grad_copies(body_tasks * m + q):
                        c.start()
            hook = lax.rem(j, 2) * n_body + m
            ahead = part + 1

            @pl.when((hook == 0) & (ahead < n_part))
            def _():
                e_logits(ahead)

            @pl.when((hook == 1) & (ahead < n_part))
            def _():
                e_out(ahead)

            @pl.when((hook == 1) & (ahead + 1 < n_part))
            def _():
                u_in(ahead + 1)

            @pl.when((hook == 2) & (ahead + 1 < n_part))
            def _():
                z_all(ahead + 1)

            @pl.when((hook == 2) & (ahead + 2 < n_part))
            def _():
                give_part(ahead + 2)

            @pl.when((hook == 3) & (ahead + 1 < n_part))
            def _():
                z_relay_on(ahead + 1)
            return carry

        lax.fori_loop(0, n_body, some_tasks, 0)
        return carry

    lax.fori_loop(0, n_tile, grad_tile, 0)

    def up_slots(t):
        return zall.at[pl.ds(pl.multiple_of(n_part * t, n_part), n_part)]

    def landed(t, carry):
        grad_copies(t)[0].wait_recv()
        pltpu.make_async_copy(up_slots(t), up_slots(t), grecv_sem.at[1, t]).wait()
        return carry

    lax.fori_loop(0, n_task, landed, 0)
    pairs = [(t, s) for t in range(n_task) for s in range(t, n_task)]
    lane = lax.broadcasted_iota(jnp.int32, (8, LANES), 1)

    def gram_of(vals, sums):
        return tuple(acc + vals[t] * vals[s] for acc, (t, s) in zip(sums, pairs))

    def down_at(t, r, c):
        return (pl.ds(pl.multiple_of((t % 2) * half + r * 8, 8), 8), slice((t // 2) * hidden + c, (t // 2) * hidden + c + LANES))

    def fold_down(r, sums):
        from_acc = pl.ds(pl.multiple_of(core * half + r * 8, 8), 8)
        for c in range(0, hidden, LANES):
            vals = []
            for t in range(n_task):
                v = dn_acc[t, from_acc, c:c + LANES] + gp_s[down_at(t, r, c)]
                gp_s[down_at(t, r, c)] = v
                vals.append(v)
            sums = gram_of(vals, sums)
        return sums

    n_row = sub_blk // 8

    def fold_up(n, sums):
        i, r = lax.div(n, n_row), lax.rem(n, n_row)
        rows = pl.ds(pl.multiple_of(r * 8, 8), 8)
        for c in range(0, win, LANES):
            edge = c < win - hidden // 2 or c + LANES > hidden // 2
            vals = []
            for t in range(n_task):
                v = up_acc[pl.ds(pl.multiple_of(t * width + n * 8, 8), 8),
                           pl.ds(pl.multiple_of(core * off + c, LANES), LANES)] + zall[n_part * t + i, rows, c:c + LANES]
                zall[n_part * t + i, rows, c:c + LANES] = v
                vals.append(jnp.where((lane + c >= first) & (lane + c < first + hidden // 2), v, 0.0) if edge else v)
            sums = gram_of(vals, sums)
        return sums

    sums = tuple(jnp.zeros((8, LANES), F32) for _ in pairs)
    sums = lax.fori_loop(0, half // 8, fold_down, sums)
    sums = lax.fori_loop(0, width // 8, fold_up, sums)
    lane1 = lax.broadcasted_iota(jnp.int32, (1, LANES), 1)
    row = lax.broadcasted_iota(jnp.int32, (8, LANES), 0)
    out = jnp.zeros((1, LANES), F32)
    for acc, (t, s) in zip(sums, pairs):
        total = jnp.sum(jnp.sum(acc, axis=0, keepdims=True), axis=1, keepdims=True)
        out = out + jnp.where((lane1 == t * n_task + s) | (lane1 == s * n_task + t), total, 0.0)
    msend[...] = out

    def send_gram(k, carry):
        remote(msend, mrecv.at[slot_of_me], msend_sem, mrecv_sem, other(k)).start()
        return carry

    lax.fori_loop(0, n_all - 1, send_gram, 0)
    pltpu.make_async_copy(msend, mrecv.at[slot_of_me], mrecv_sem).start()
    pltpu.make_async_copy(mrecv, mrecv, mrecv_sem).wait()
    flat = jnp.sum(mrecv[...], axis=0)
    gram = jnp.zeros((8, LANES), F32)
    for t in range(n_task):
        line = flat if t == 0 else pltpu.roll(flat, LANES - t * n_task, 1)
        gram = gram + jnp.where((row == t) & (lane < n_task), jnp.broadcast_to(line, (8, LANES)), 0.0)
    scale = jnp.sum(jnp.sum(jnp.where(row == lane, gram, 0.0), axis=1, keepdims=True), axis=0, keepdims=True) / n_task
    gram = gram / scale
    w = jnp.where(lane < n_task, 1.0 / n_task, 0.0).astype(F32)

    def eg_pair(i, w):
        v = jnp.sum(gram * w, axis=1, keepdims=True)
        w_col = jnp.sum(jnp.where(row == lane, w, 0.0), axis=1, keepdims=True)
        w_col = w_col * jnp.exp(-v)
        w_col = w_col / jnp.sum(w_col, axis=0, keepdims=True)
        v = jnp.sum(gram * w_col, axis=0, keepdims=True)
        w_row = jnp.sum(jnp.where(row == lane, w_col, 0.0), axis=0, keepdims=True)
        w_row = w_row * jnp.exp(-v)
        w_row = w_row / jnp.sum(w_row, axis=1, keepdims=True)
        return jnp.broadcast_to(w_row, (8, LANES))

    w = lax.fori_loop(0, STEPS // 2, eg_pair, w)
    a_ref[...] = w
    a = [jnp.broadcast_to(jnp.sum(jnp.where(lane == t, w, 0.0), axis=1, keepdims=True), (8, LANES))
         for t in range(n_task)]

    def mix_down(r, carry):
        rows = pl.ds(pl.multiple_of(r * 8, 8), 8)
        for c in range(0, hidden, LANES):
            total = a[0] * gp_s[down_at(0, r, c)]
            for t in range(1, n_task):
                total = total + a[t] * gp_s[down_at(t, r, c)]
            g2_ref[rows, c:c + LANES] = total
        return carry

    last = z_in(0, 0, 0)

    def mix_up(n, carry):
        i, r = lax.div(n, n_row), lax.rem(n, n_row)
        rows = pl.ds(pl.multiple_of(r * 8, 8), 8)
        for c in range(0, win, LANES):
            total = a[0] * zall[i, rows, c:c + LANES]
            for t in range(1, n_task):
                total = total + a[t] * zall[n_part * t + i, rows, c:c + LANES]
            zall[last + i, rows, c:c + LANES] = total
        return carry

    lax.fori_loop(0, half // 8, mix_down, 0)
    lax.fori_loop(0, width // 8, mix_up, 0)
    for c in range(0, win, LANES):
        g1t[c:c + LANES, :] = jnp.concatenate([zall[last + i, :, c:c + LANES] for i in range(n_part)], axis=0).T
    g1_ref[...] = g1t[pl.ds(pl.multiple_of(first, 8), hidden // 2), :]

    for h, way in hw:
        for stage in range(4):
            gather_copy(h, stage, way).wait_send()
    for part in range(n_part):
        for s in range(4):
            u_pair(part, s).wait_send()
        sent = et.at[part, pl.ds(0, n_model - 1)]
        pltpu.make_async_copy(sent, sent, esend_sem.at[part]).wait()
    far_x.wait_send()
    sent = usend.at[pl.ds(0, n_tok - ring * blk), :]
    pltpu.make_async_copy(sent, sent, usend_sem).wait()

    def gone(t, carry):
        grad_copies(t)[0].wait_send()
        pltpu.make_async_copy(up_slots(t), up_slots(t), gsend_sem.at[1, t]).wait()
        return carry

    lax.fori_loop(0, n_task, gone, 0)
    sent = mrecv.at[pl.ds(0, n_all - 1)]
    pltpu.make_async_copy(sent, sent, msend_sem).wait()


def solution(mesh):
    n_model, n_data = mesh.shape['model'], mesh.shape['data']

    def local_step(tokens, w_up, w_down, task_heads, labels):
        n_tok, hidden = tokens.shape
        n_total = n_tok * n_data
        width = w_up.shape[1]
        n_task = task_heads.shape[0]
        blk = n_tok // n_model
        sub_blk = blk // 4
        half = width // 2
        win = -(-(hidden // 2) // LANES) * LANES
        tile = 32 * sub_blk
        any_spec = pl.BlockSpec(memory_space=pl.ANY)
        vmem_spec = pl.BlockSpec(memory_space=pltpu.VMEM)
        dma = pltpu.SemaphoreType.DMA
        vmem = pltpu.VMEM
        weights, grad_up, grad_down = pl.pallas_call(
            functools.partial(step_kernel, n_model, win, n_total),
            out_shape=(jax.ShapeDtypeStruct((8, LANES), F32), jax.ShapeDtypeStruct((hidden // 2, width), F32),
                       jax.ShapeDtypeStruct((half, hidden), F32)),
            in_specs=[any_spec, vmem_spec, vmem_spec, vmem_spec, vmem_spec],
            out_specs=(vmem_spec, vmem_spec, vmem_spec),
            scratch_shapes=[vmem((width, hidden), BF16), vmem((2 * n_task, win), BF16), vmem((n_task, 1, hidden), F32),
                            vmem((2, tile, hidden), BF16), vmem((n_tok, width), BF16), vmem((width, n_tok), BF16),
                            vmem((width, n_tok), F32), vmem((4, 2, 4, sub_blk, 16 * width), BF16),
                            vmem((2, 16, half, win), BF16), vmem((2, blk, win), BF16),
                            vmem((56, sub_blk, win), F32), vmem((4, 2 * n_task, blk), F32),
                            vmem((4, 2 * n_task, blk), F32), vmem((4, 2 * n_task, blk), F32),
                            vmem((4, n_task, blk), F32), vmem((4, n_model, n_task, blk), F32),
                            vmem((n_task, width, hidden), F32), vmem((n_task * width, hidden), F32),
                            vmem((n_task, hidden, LANES), F32), vmem((n_task, 1, tile), F32), vmem((4 * width, tile), BF16),
                            vmem((1, LANES), F32), vmem((2 * n_model, 1, LANES), F32), vmem((win, width), F32),
                            dma((2,)), dma, dma((4, 4)), dma((2, 4, 2)), dma((2, 4, 2)), dma((4, 4)), dma((4, 4)),
                            dma((4, 4)), dma((4, 4)), dma((4,)), dma((4,)), dma((4,)), dma((4,)), dma((5,)),
                            dma((2, n_task)), dma((2, n_task)), dma, dma, pltpu.SemaphoreType.REGULAR],
            compiler_params=pltpu.CompilerParams(collective_id=0, has_side_effects=True, vmem_limit_bytes=67043328),
            name='step')(tokens, w_up, w_down, jnp.transpose(task_heads, (0, 2, 1)), labels)
        return weights[0, :n_task], grad_up, grad_down

    return jax.shard_map(
        local_step, mesh=mesh,
        in_specs=(P('data', None), P(None, 'model'), P('model', None), P(None, None, None), P(None, 'data')),
        out_specs=(P(None), P('data', 'model'), P(('model', 'data'), None)),
        check_vma=False)
```

```python
import functools

import jax
import jax.numpy as jnp
from jax import lax
from jax.experimental import pallas as pl
from jax.experimental.pallas import tpu as pltpu
from jax.sharding import PartitionSpec as P

STEPS = 20
LANES = 128
MESH = pl.DeviceIdType.MESH
F32 = jnp.float32
BF16 = jnp.bfloat16
C_GELU = 0.7978845608028654
K_GELU = 0.044715
NT = (((1,), (1,)), ((), ()))


def peer(model, data):
    return {"model": model, "data": data}


def step_kernel(n_model, win, n_total, x_ref, w1_ref, w2_ref, h_ref, lab_ref, a_ref, g1_ref, g2_ref,
                w1t_ref, ht_ref, drow_ref, xbuf, usend, ut_s, gp_s, uslab, wslab, xz, zall, lown, lsend, lrecv, esend, et,
                dn_acc, up_acc, dcol, ebr, dat, msend, mrecv, g1t,
                xsem, usend_sem, urecv_sem, wsend_sem, wrecv_sem, psend_sem, precv_sem, zsend_sem, zrecv_sem,
                esend_sem, erecv_sem, ssend_sem, srecv_sem, lsem, gsend_sem, grecv_sem, msend_sem, mrecv_sem, free_sem):
    me = lax.axis_index("model")
    core = lax.axis_index("data")
    ring = 4
    plane = ring * ring
    n_tok, hidden = x_ref.shape
    blk = n_tok // n_model
    n_part = 4
    sub_blk = blk // n_part
    width = w1_ref.shape[1]
    half = width // 2
    n_task = lab_ref.shape[0]
    off = hidden - win
    tile = 2 * plane * sub_blk
    n_tile = 2 * n_part
    body_tasks = 4
    n_body = n_task // body_tasks
    n_slot = n_part * 8
    n_all = 2 * n_model
    slot_of_me = me * 2 + core
    px, py, pz = lax.rem(me, ring), lax.rem(lax.div(me, ring), ring), lax.div(me, plane)
    group = lax.div(me, ring)
    partner = peer(me, 1 - core)
    wide = 256
    cuts = [(c, min(wide, hidden - c)) for c in range(0, hidden, wide)]

    def at(x, y, z):
        model = lax.rem(z + ring, ring) * plane + lax.rem(y + ring, ring) * ring + lax.rem(x + ring, ring)
        return peer(model, core)

    def remote(src, dst, ssem, rsem, dev):
        return pltpu.make_async_remote_copy(src_ref=src, dst_ref=dst, send_sem=ssem, recv_sem=rsem,
                                            device_id=dev, device_id_type=MESH)

    def other(k):
        dev = lax.rem(slot_of_me + k, n_all)
        return peer(lax.div(dev, 2), lax.rem(dev, 2))

    sem = pltpu.get_barrier_semaphore()

    def tell(k, carry):
        pl.semaphore_signal(sem, inc=1, device_id=other(k), device_id_type=MESH)
        return carry

    lax.fori_loop(1, n_all, tell, 0)

    def block_of(j, k):
        sub = lax.rem(2 * j + lax.div(k, plane), ring)
        shift = jnp.where(sub == 0, 2, jnp.where(sub == 1, 1, jnp.where(sub == 2, 3, 0)))
        return lax.rem(group + lax.rem(k, plane), plane) * ring + lax.rem(px + shift, ring)

    def fetch(j, slot):
        def one(k, carry):
            row = block_of(j, k) * blk + lax.div(j, 2) * sub_blk
            pltpu.make_async_copy(x_ref.at[pl.ds(pl.multiple_of(row, sub_blk), sub_blk), :],
                                  xbuf.at[slot, pl.ds(pl.multiple_of(k * sub_blk, sub_blk), sub_blk), :],
                                  xsem.at[slot]).start()
            return carry

        lax.fori_loop(0, 2 * plane, one, 0)

    def fetched(slot):
        pltpu.make_async_copy(xbuf.at[slot], xbuf.at[slot], xsem.at[slot]).wait()

    fetch(0, 0)
    w_cols = pl.ds(pl.multiple_of(core * off, LANES), win)
    far_cols = pl.ds(pl.multiple_of((1 - core) * off, LANES), win)
    mine = pl.ds(pl.multiple_of(me * blk, blk), blk)
    own = [pltpu.make_async_copy(x_ref.at[mine, w_cols], xz.at[0], lsem.at[0])]
    coords = ((py, pz), (pz, py))
    for h in range(2):
        c1, c2 = coords[h]
        own.append(pltpu.make_async_copy(w2_ref.at[pl.ds(h * half, half), w_cols],
                                         wslab.at[h, c2 * ring + c1], lsem.at[1 + h]))
    for c in own:
        c.start()

    def near(h, axis, d):
        y_axis = (h == 0) == (axis == 0)
        return at(px, py + d, pz) if y_axis else at(px, py, pz + d)

    def gather_copy(h, stage, way):
        c1, c2 = coords[h]
        d = 1 if way == 0 else -1
        sems = (wsend_sem.at[h, stage, way], wrecv_sem.at[h, stage, way])
        if stage == 0:
            src = w2_ref.at[pl.ds(h * half, half), w_cols]
            return remote(src, wslab.at[h, c2 * ring + c1], *sems, near(h, 0, d))
        if stage == 1:
            piece = c2 * ring + lax.rem(c1 - d + ring, ring)
            ref = wslab.at[h, piece, pl.ds(way * (half // 2), half // 2), :]
            return remote(ref, ref, *sems, near(h, 0, d))
        if stage == 2:
            ref = wslab.at[h, pl.ds(c2 * ring, ring)]
            return remote(ref, ref, *sems, near(h, 1, d))
        ref = wslab.at[h, pl.ds(lax.rem(c2 - d + ring, ring) * ring + way * (ring // 2), ring // 2)]
        return remote(ref, ref, *sems, near(h, 1, d))

    hw = [(h, way) for h in range(2) for way in range(2)]
    dn_acc[...] = jnp.zeros_like(dn_acc)
    up_acc[...] = jnp.zeros_like(up_acc)
    w1t_ref[...] = w1_ref[...].T
    first = core * (win - hidden // 2)
    col = lax.broadcasted_iota(jnp.int32, (2 * n_task, win), 1)
    h_rows = jnp.concatenate([h_ref[t, c:c + 1, w_cols].astype(F32) for c in range(2) for t in range(n_task)], axis=0)
    ht_ref[...] = jnp.where((col >= first) & (col < first + hidden // 2), h_rows, 0.0).astype(BF16)
    for t in range(n_task):
        drow_ref[t] = h_ref[t, 0:1, :].astype(F32) - h_ref[t, 1:2, :].astype(F32)

    def spread(t, carry):
        dcol[t] = jnp.broadcast_to(drow_ref[t], (LANES, hidden)).T
        return carry

    lax.fori_loop(0, n_task, spread, 0)
    pl.semaphore_wait(sem, n_all - 1)
    far_x = remote(x_ref.at[mine, far_cols], xz.at[1], lsem.at[3], lsem.at[4], partner)
    for h, way in hw:
        gather_copy(h, 0, way).start()
    far_x.start()

    def forward(j, carry):
        slot = lax.rem(j, 2)

        @pl.when(j + 1 < n_tile)
        def _():
            fetch(j + 1, 1 - slot)

        fetched(slot)
        base = pl.multiple_of(j * tile, tile)
        step = min(512, tile)
        for n in range(0, tile, step):
            a = lax.dot_general(w1t_ref[...], xbuf[slot, n:n + step, :], NT, preferred_element_type=F32)
            a2 = a * a
            th = jnp.tanh(C_GELU * (a + K_GELU * (a * a2)))
            cdf = 0.5 * (1.0 + th)
            slope = cdf + a * (0.5 * (1.0 - th * th) * (C_GELU * (1.0 + (3.0 * K_GELU) * a2)))
            u_f = a * cdf
            ut_s[:, pl.ds(pl.multiple_of(base + n, step), step)] = u_f.astype(BF16)
            gp_s[:, pl.ds(pl.multiple_of(base + n, step), step)] = slope
            usend[pl.ds(pl.multiple_of(base + n, step), step), :] = u_f.T.astype(BF16)
        return carry

    def give(n, carry):
        run = lax.div(n, plane)
        part, sub = lax.div(run, ring), lax.rem(run, ring)
        g = lax.rem(group + lax.rem(n, plane), plane)
        src = usend.at[pl.ds(pl.multiple_of(n * sub_blk, sub_blk), sub_blk), :]
        dst = uslab.at[part, 0, sub, :, pl.ds(pl.multiple_of(group * width, width), width)]

        @pl.when(g != group)
        def _():
            remote(src, dst, usend_sem, urecv_sem.at[part, sub], peer(g * ring + px, core)).start()

        @pl.when(g == group)
        def _():
            pltpu.make_async_copy(src, dst, urecv_sem.at[part, sub]).start()
        return carry

    def give_part(part):
        lax.fori_loop(part * (ring * plane), (part + 1) * (ring * plane), give, 0)

    lax.fori_loop(0, 1, forward, 0)
    lax.fori_loop(0, plane, give, 0)
    for h, way in hw:
        gather_copy(h, 0, way).wait_recv()
        gather_copy(h, 1, way).start()
    lax.fori_loop(plane, 2 * plane, give, 0)
    lax.fori_loop(1, 2, forward, 0)
    for c in own:
        c.wait()
    for h, way in hw:
        gather_copy(h, 1, way).wait_recv()
    for h, way in hw:
        gather_copy(h, 2, way).start()
    lax.fori_loop(2 * plane, 4 * plane, give, 0)
    lax.fori_loop(2, n_tile, forward, 0)
    fetch(0, 0)
    for h, way in hw:
        gather_copy(h, 2, way).wait_recv()
        gather_copy(h, 3, way).start()
    give_part(1)

    def u_pair(part, s):
        return remote(uslab.at[part, 0, s], uslab.at[part, 1, s], psend_sem.at[part, s], precv_sem.at[part, s], partner)

    def u_arrive(part, s):
        ref = uslab.at[part, 0, s]
        pltpu.make_async_copy(ref, ref, urecv_sem.at[part, s]).wait()
        u_pair(part, s).start()

    def z_out(part, n, q):
        return part * 8 + n * 2 + q

    def z_relay(part, q):
        return n_slot + part * 2 + q

    def z_in(part, i, q):
        return n_slot + 2 * n_part + part * 4 + i * 2 + q

    def z_copy(part, n):
        left, right = at(px - 1, py, pz), at(px + 1, py, pz)
        src, dst, dev = ((zall.at[z_out(part, 0, 0)], zall.at[z_relay(part, 0)], right),
                         (zall.at[z_out(part, 0, 1)], zall.at[z_relay(part, 1)], left),
                         (zall.at[pl.ds(z_out(part, 1, 0), 2)], zall.at[pl.ds(z_in(part, 0, 0), 2)], right),
                         (zall.at[pl.ds(z_out(part, 2, 0), 2)], zall.at[pl.ds(z_in(part, 1, 0), 2)], left))[n]
        return remote(src, dst, zsend_sem.at[part, n], zrecv_sem.at[part, n], dev)

    def rows_of(g):
        y, z = g % ring, g // ring
        return [(0, z * ring + y), (1, y * ring + z)]

    def partial_z(part, subs, relayed):
        for c in range(0, win, wide):
            size = min(wide, win - c)
            total = jnp.zeros((2 * len(subs) * sub_blk, size), F32)
            for g in range(0, plane, 2):
                left = jnp.concatenate(
                    [uslab[part, q, s, :, g * width:(g + 2) * width] for s in subs for q in range(2)], axis=0)
                right = jnp.concatenate([wslab[h, i, :, c:c + size] for h, i in rows_of(g) + rows_of(g + 1)], axis=0)
                total = total + jnp.dot(left, right, preferred_element_type=F32)
            for i, s in enumerate(subs):
                for q in range(2):
                    v = total[(2 * i + q) * sub_blk:(2 * i + q + 1) * sub_blk]
                    if relayed and q == s - 1:
                        v = v + zall[z_relay(part, q), :, c:c + size]
                    zall[z_out(part, s, q), :, c:c + size] = v

    def z_first(s):
        u_pair(0, s).wait_recv()
        if s in (1, 2):
            z_copy(0, s - 1).wait_recv()
        partial_z(0, (s,), True)
        for n in ((0, 1), (2,), (3,), ())[s]:
            z_copy(0, n).start()

    def z_all(part):
        for s in range(4):
            u_pair(part, s).wait_recv()
        partial_z(part, (0, 1, 2, 3), False)
        z_copy(part, 0).start()
        z_copy(part, 1).start()

    def z_relay_on(part):
        for q in range(2):
            z_copy(part, q).wait_recv()
            zall[z_out(part, 1 + q, q)] += zall[z_relay(part, q)]
            z_copy(part, 2 + q).start()

    pad = jnp.zeros((n_task, blk - sub_blk), F32)

    def swap(part):
        return remote(lsend.at[part], lrecv.at[part], ssend_sem.at[part], srecv_sem.at[part], partner)

    def e_logits(part):
        z_copy(part, 2).wait_recv()
        z_copy(part, 3).wait_recv()
        for n in range(4):
            z_copy(part, n).wait_send()
        gaps = []
        rows = pl.ds(pl.multiple_of(part * sub_blk, sub_blk), sub_blk)
        for q in range(2):
            z = (xz[q, rows, :].astype(F32) + ((zall[z_out(part, 3, q)] + zall[z_in(part, 0, q)])
                                               + zall[z_in(part, 1, q)])).astype(BF16)
            gaps.append(lax.dot_general(ht_ref[...], z, NT, preferred_element_type=F32))
        both = jnp.concatenate([pad, pad], axis=0)
        lown[part] = jnp.concatenate([gaps[0], both], axis=1)
        lsend[part] = jnp.concatenate([gaps[1], both], axis=1)
        swap(part).start()

    def e_out(part):
        swap(part).wait()
        logit = lown[part] + lrecv[part]
        gap = logit[:n_task, :] - logit[n_task:, :]
        first_class = pltpu.roll(lab_ref[:, mine], lax.rem(blk - part * sub_blk, blk), 1) == 0
        wrong = 1.0 / (1.0 + jnp.exp(jnp.where(first_class, gap, -gap)))
        esend[part] = jnp.where(first_class, -wrong, wrong) * (1.0 / n_total)
        dst = et.at[part, me]

        def send(k, carry):
            remote(esend.at[part], dst, esend_sem.at[part], erecv_sem.at[part],
                   peer(lax.rem(me + k, n_model), core)).start()
            return carry

        lax.fori_loop(1, n_model, send, 0)
        pltpu.make_async_copy(esend.at[part], dst, erecv_sem.at[part]).start()

    def e_in(part):
        pltpu.make_async_copy(et.at[part], et.at[part], erecv_sem.at[part]).wait()

    def u_in(part):
        for s in range(4):
            u_arrive(part, s)

    u_in(0)
    for h, way in hw:
        gather_copy(h, 3, way).wait_recv()
    for s in range(4):
        z_first(s)
    far_x.wait_recv()
    e_logits(0)
    e_out(0)
    u_in(1)
    z_all(1)
    e_in(0)
    z_relay_on(1)
    give_part(2)

    def far_down(t):
        rows = pl.ds(pl.multiple_of(lax.rem(t, 2) * half, half), half)
        return gp_s.at[rows, pl.ds(pl.multiple_of(lax.div(t, 2) * hidden, LANES), hidden)]

    def grad_copies(t):
        out = [remote(dn_acc.at[t, pl.ds(pl.multiple_of((1 - core) * half, half), half), :], far_down(t),
                      gsend_sem.at[0, t], grecv_sem.at[0, t], partner)]
        for i in range(n_part):
            rows = pl.ds(pl.multiple_of(t * width + i * sub_blk, sub_blk), sub_blk)
            out.append(remote(up_acc.at[rows, far_cols], zall.at[n_part * t + i],
                              gsend_sem.at[1, t], grecv_sem.at[1, t], partner))
        return out

    def grad_tile(j, carry):
        slot = lax.rem(j, 2)

        @pl.when(j + 1 < n_tile)
        def _():
            fetch(j + 1, 1 - slot)

        @pl.when(j == n_tile - 1)
        def _():
            pl.semaphore_signal(free_sem, inc=1, device_id=partner, device_id_type=MESH)

        part = lax.div(j, 2)

        @pl.when((lax.rem(j, 2) == 0) & (j > 0))
        def _():
            e_in(part)

        for k in range(0, 2 * plane, n_part):
            pieces = [et[part, block_of(j, k + i)][:, :sub_blk] for i in range(n_part)]
            e_pair = jnp.concatenate(pieces, axis=1)
            for t in range(n_task):
                ebr[t, :, k * sub_blk:(k + n_part) * sub_blk] = e_pair[t:t + 1, :]
        fetched(slot)
        base = pl.multiple_of(j * tile, tile)

        def some_tasks(m, carry):
            rows = pl.ds(pl.multiple_of(body_tasks * m * width, body_tasks * width), body_tasks * width)
            for q in range(body_tasks):
                t = body_tasks * m + q
                for n in range(0, tile, wide):
                    n_size = min(wide, tile)
                    e_n = ebr[t, :, n:n + n_size]
                    da = jnp.zeros((width, n_size), F32)
                    for c, size in cuts:
                        d_c = jnp.concatenate([dcol[t, c:c + size, :]] * (n_size // LANES), axis=1)
                        dz_t = (d_c * e_n).astype(BF16)
                        da = da + jnp.dot(w2_ref[:, c:c + size], dz_t, preferred_element_type=F32)
                    cols = pl.ds(pl.multiple_of(base + n, n_size), n_size)
                    dat[q * width:(q + 1) * width, n:n + n_size] = (da * gp_s[:, cols]).astype(BF16)
            left = ut_s[:, pl.ds(base, tile)]
            for q in range(0, body_tasks, 2):
                ts = (body_tasks * m + q, body_tasks * m + q + 1)
                e_col = [jnp.broadcast_to(ebr[t], (LANES, tile)).T for t in ts]
                for i, t in enumerate(ts):
                    for c, size in cuts:
                        if size == wide:
                            e_b = jnp.concatenate([e_col[i]] * (size // LANES), axis=1)
                            dz = (e_b * drow_ref[t, :, c:c + size]).astype(BF16)
                            dn_acc[t, :, c:c + size] += jnp.dot(left, dz, preferred_element_type=F32)
                c, size = cuts[-1]
                if size < wide:
                    dz = jnp.concatenate([e_col[i] * drow_ref[t, :, c:c + size] for i, t in enumerate(ts)],
                                         axis=1).astype(BF16)
                    both = jnp.dot(left, dz, preferred_element_type=F32)
                    for i, t in enumerate(ts):
                        dn_acc[t, :, c:c + size] += both[:, i * size:(i + 1) * size]
            left = dat[...]
            for c, size in cuts:
                up_acc[rows, c:c + size] += jnp.dot(left, xbuf[slot, :, c:c + size], preferred_element_type=F32)

            @pl.when((j == n_tile - 1) & (m == 0))
            def _():
                pl.semaphore_wait(free_sem, 1)

            @pl.when(j == n_tile - 1)
            def _():
                for q in range(body_tasks):
                    for c in grad_copies(body_tasks * m + q):
                        c.start()
            hook = lax.rem(j, 2) * n_body + m
            ahead = part + 1

            @pl.when((hook == 0) & (ahead < n_part))
            def _():
                e_logits(ahead)

            @pl.when((hook == 1) & (ahead < n_part))
            def _():
                e_out(ahead)

            @pl.when((hook == 1) & (ahead + 1 < n_part))
            def _():
                u_in(ahead + 1)

            @pl.when((hook == 2) & (ahead + 1 < n_part))
            def _():
                z_all(ahead + 1)

            @pl.when((hook == 2) & (ahead + 2 < n_part))
            def _():
                give_part(ahead + 2)

            @pl.when((hook == 3) & (ahead + 1 < n_part))
            def _():
                z_relay_on(ahead + 1)
            return carry

        lax.fori_loop(0, n_body, some_tasks, 0)
        return carry

    lax.fori_loop(0, n_tile, grad_tile, 0)

    def up_slots(t):
        return zall.at[pl.ds(pl.multiple_of(n_part * t, n_part), n_part)]

    def landed(t, carry):
        grad_copies(t)[0].wait_recv()
        pltpu.make_async_copy(up_slots(t), up_slots(t), grecv_sem.at[1, t]).wait()
        return carry

    lax.fori_loop(0, n_task, landed, 0)
    pairs = [(t, s) for t in range(n_task) for s in range(t, n_task)]
    lane = lax.broadcasted_iota(jnp.int32, (8, LANES), 1)

    def gram_of(vals, sums):
        return tuple(acc + vals[t] * vals[s] for acc, (t, s) in zip(sums, pairs))

    def down_at(t, r, c):
        return (pl.ds(pl.multiple_of((t % 2) * half + r * 8, 8), 8), slice((t // 2) * hidden + c, (t // 2) * hidden + c + LANES))

    def fold_down(r, sums):
        from_acc = pl.ds(pl.multiple_of(core * half + r * 8, 8), 8)
        for c in range(0, hidden, LANES):
            vals = []
            for t in range(n_task):
                v = dn_acc[t, from_acc, c:c + LANES] + gp_s[down_at(t, r, c)]
                gp_s[down_at(t, r, c)] = v
                vals.append(v)
            sums = gram_of(vals, sums)
        return sums

    n_row = sub_blk // 8

    def fold_up(n, sums):
        i, r = lax.div(n, n_row), lax.rem(n, n_row)
        rows = pl.ds(pl.multiple_of(r * 8, 8), 8)
        for c in range(0, win, LANES):
            edge = c < win - hidden // 2 or c + LANES > hidden // 2
            vals = []
            for t in range(n_task):
                v = up_acc[pl.ds(pl.multiple_of(t * width + n * 8, 8), 8),
                           pl.ds(pl.multiple_of(core * off + c, LANES), LANES)] + zall[n_part * t + i, rows, c:c + LANES]
                zall[n_part * t + i, rows, c:c + LANES] = v
                vals.append(jnp.where((lane + c >= first) & (lane + c < first + hidden // 2), v, 0.0) if edge else v)
            sums = gram_of(vals, sums)
        return sums

    sums = tuple(jnp.zeros((8, LANES), F32) for _ in pairs)
    sums = lax.fori_loop(0, half // 8, fold_down, sums)
    sums = lax.fori_loop(0, width // 8, fold_up, sums)
    lane1 = lax.broadcasted_iota(jnp.int32, (1, LANES), 1)
    row = lax.broadcasted_iota(jnp.int32, (8, LANES), 0)
    out = jnp.zeros((1, LANES), F32)
    for acc, (t, s) in zip(sums, pairs):
        total = jnp.sum(jnp.sum(acc, axis=0, keepdims=True), axis=1, keepdims=True)
        out = out + jnp.where((lane1 == t * n_task + s) | (lane1 == s * n_task + t), total, 0.0)
    msend[...] = out

    def send_gram(k, carry):
        remote(msend, mrecv.at[slot_of_me], msend_sem, mrecv_sem, other(k)).start()
        return carry

    lax.fori_loop(1, n_all, send_gram, 0)
    pltpu.make_async_copy(msend, mrecv.at[slot_of_me], mrecv_sem).start()
    pltpu.make_async_copy(mrecv, mrecv, mrecv_sem).wait()
    flat = jnp.sum(mrecv[...], axis=0)
    gram = jnp.zeros((8, LANES), F32)
    for t in range(n_task):
        line = flat if t == 0 else pltpu.roll(flat, LANES - t * n_task, 1)
        gram = gram + jnp.where((row == t) & (lane < n_task), jnp.broadcast_to(line, (8, LANES)), 0.0)
    scale = jnp.sum(jnp.sum(jnp.where(row == lane, gram, 0.0), axis=1, keepdims=True), axis=0, keepdims=True) / n_task
    gram = gram / scale
    w = jnp.where(lane < n_task, 1.0 / n_task, 0.0).astype(F32)

    def eg_pair(i, w):
        v = jnp.sum(gram * w, axis=1, keepdims=True)
        w_col = jnp.sum(jnp.where(row == lane, w, 0.0), axis=1, keepdims=True)
        w_col = w_col * jnp.exp(-v)
        w_col = w_col / jnp.sum(w_col, axis=0, keepdims=True)
        v = jnp.sum(gram * w_col, axis=0, keepdims=True)
        w_row = jnp.sum(jnp.where(row == lane, w_col, 0.0), axis=0, keepdims=True)
        w_row = w_row * jnp.exp(-v)
        w_row = w_row / jnp.sum(w_row, axis=1, keepdims=True)
        return jnp.broadcast_to(w_row, (8, LANES))

    w = lax.fori_loop(0, STEPS // 2, eg_pair, w)
    a_ref[...] = w
    a = [jnp.broadcast_to(jnp.sum(jnp.where(lane == t, w, 0.0), axis=1, keepdims=True), (8, LANES))
         for t in range(n_task)]

    def mix_down(r, carry):
        rows = pl.ds(pl.multiple_of(r * 8, 8), 8)
        for c in range(0, hidden, LANES):
            total = a[0] * gp_s[down_at(0, r, c)]
            for t in range(1, n_task):
                total = total + a[t] * gp_s[down_at(t, r, c)]
            g2_ref[rows, c:c + LANES] = total
        return carry

    last = z_in(0, 0, 0)

    def mix_up(n, carry):
        i, r = lax.div(n, n_row), lax.rem(n, n_row)
        rows = pl.ds(pl.multiple_of(r * 8, 8), 8)
        for c in range(0, win, LANES):
            total = a[0] * zall[i, rows, c:c + LANES]
            for t in range(1, n_task):
                total = total + a[t] * zall[n_part * t + i, rows, c:c + LANES]
            zall[last + i, rows, c:c + LANES] = total
        return carry

    lax.fori_loop(0, half // 8, mix_down, 0)
    lax.fori_loop(0, width // 8, mix_up, 0)
    for c in range(0, win, LANES):
        g1t[c:c + LANES, :] = jnp.concatenate([zall[last + i, :, c:c + LANES] for i in range(n_part)], axis=0).T
    g1_ref[...] = g1t[pl.ds(pl.multiple_of(first, 8), hidden // 2), :]

    for h, way in hw:
        for stage in range(4):
            gather_copy(h, stage, way).wait_send()
    for part in range(n_part):
        for s in range(4):
            u_pair(part, s).wait_send()
        sent = et.at[part, pl.ds(0, n_model - 1)]
        pltpu.make_async_copy(sent, sent, esend_sem.at[part]).wait()
    far_x.wait_send()
    sent = usend.at[pl.ds(0, n_tok - ring * blk), :]
    pltpu.make_async_copy(sent, sent, usend_sem).wait()

    def gone(t, carry):
        grad_copies(t)[0].wait_send()
        pltpu.make_async_copy(up_slots(t), up_slots(t), gsend_sem.at[1, t]).wait()
        return carry

    lax.fori_loop(0, n_task, gone, 0)
    sent = mrecv.at[pl.ds(0, n_all - 1)]
    pltpu.make_async_copy(sent, sent, msend_sem).wait()


def solution(mesh):
    n_model, n_data = mesh.shape['model'], mesh.shape['data']

    def local_step(tokens, w_up, w_down, task_heads, labels):
        n_tok, hidden = tokens.shape
        n_total = n_tok * n_data
        width = w_up.shape[1]
        n_task = task_heads.shape[0]
        blk = n_tok // n_model
        sub_blk = blk // 4
        half = width // 2
        win = -(-(hidden // 2) // LANES) * LANES
        tile = 32 * sub_blk
        any_spec = pl.BlockSpec(memory_space=pl.ANY)
        vmem_spec = pl.BlockSpec(memory_space=pltpu.VMEM)
        dma = pltpu.SemaphoreType.DMA
        vmem = pltpu.VMEM
        weights, grad_up, grad_down = pl.pallas_call(
            functools.partial(step_kernel, n_model, win, n_total),
            out_shape=(jax.ShapeDtypeStruct((8, LANES), F32), jax.ShapeDtypeStruct((hidden // 2, width), F32),
                       jax.ShapeDtypeStruct((half, hidden), F32)),
            in_specs=[any_spec, vmem_spec, vmem_spec, vmem_spec, vmem_spec],
            out_specs=(vmem_spec, vmem_spec, vmem_spec),
            scratch_shapes=[vmem((width, hidden), BF16), vmem((2 * n_task, win), BF16), vmem((n_task, 1, hidden), F32),
                            vmem((2, tile, hidden), BF16), vmem((n_tok, width), BF16), vmem((width, n_tok), BF16),
                            vmem((width, n_tok), F32), vmem((4, 2, 4, sub_blk, 16 * width), BF16),
                            vmem((2, 16, half, win), BF16), vmem((2, blk, win), BF16),
                            vmem((56, sub_blk, win), F32), vmem((4, 2 * n_task, blk), F32),
                            vmem((4, 2 * n_task, blk), F32), vmem((4, 2 * n_task, blk), F32),
                            vmem((4, n_task, blk), F32), vmem((4, n_model, n_task, blk), F32),
                            vmem((n_task, width, hidden), F32), vmem((n_task * width, hidden), F32),
                            vmem((n_task, hidden, LANES), F32), vmem((n_task, 1, tile), F32), vmem((4 * width, tile), BF16),
                            vmem((1, LANES), F32), vmem((2 * n_model, 1, LANES), F32), vmem((win, width), F32),
                            dma((2,)), dma, dma((4, 4)), dma((2, 4, 2)), dma((2, 4, 2)), dma((4, 4)), dma((4, 4)),
                            dma((4, 4)), dma((4, 4)), dma((4,)), dma((4,)), dma((4,)), dma((4,)), dma((5,)),
                            dma((2, n_task)), dma((2, n_task)), dma, dma, pltpu.SemaphoreType.REGULAR],
            compiler_params=pltpu.CompilerParams(collective_id=0, has_side_effects=True, vmem_limit_bytes=67043328),
            name='step')(tokens, w_up, w_down, jnp.transpose(task_heads, (0, 2, 1)), labels)
        return weights[0, :n_task], grad_up, grad_down

    return jax.shard_map(
        local_step, mesh=mesh,
        in_specs=(P('data', None), P(None, 'model'), P('model', None), P(None, None, None), P(None, 'data')),
        out_specs=(P(None), P('data', 'model'), P(('model', 'data'), None)),
        check_vma=False)
```

```python
import functools

import jax
import jax.numpy as jnp
from jax import lax
from jax.experimental import pallas as pl
from jax.experimental.pallas import tpu as pltpu
from jax.sharding import PartitionSpec as P

STEPS = 20
LANES = 128
MESH = pl.DeviceIdType.MESH
F32 = jnp.float32
BF16 = jnp.bfloat16
C_GELU = 0.7978845608028654
K_GELU = 0.044715
NT = (((1,), (1,)), ((), ()))


def peer(model, data):
    return {"model": model, "data": data}


def step_kernel(n_model, win, n_total, x_ref, w1_ref, w2_ref, h_ref, lab_ref, a_ref, g1_ref, g2_ref,
                w1t_ref, ht_ref, drow_ref, xbuf, usend, ut_s, gp_s, uslab, wslab, xz, zall, lown, lsend, lrecv, esend, et,
                dn_acc, up_acc, dcol, ebr, dat, msend, mrecv, g1s, g1t,
                xsem, usend_sem, urecv_sem, wsend_sem, wrecv_sem, psend_sem, precv_sem, zsend_sem, zrecv_sem,
                esend_sem, erecv_sem, ssend_sem, srecv_sem, lsem, gsend_sem, grecv_sem, msend_sem, mrecv_sem, free_sem):
    me = lax.axis_index("model")
    core = lax.axis_index("data")
    ring = 4
    plane = ring * ring
    n_tok, hidden = x_ref.shape
    blk = n_tok // n_model
    n_part = 4
    sub_blk = blk // n_part
    width = w1_ref.shape[1]
    half = width // 2
    n_task = lab_ref.shape[0]
    off = hidden - win
    tile = 2 * plane * sub_blk
    n_tile = 2 * n_part
    body_tasks = 4
    n_body = n_task // body_tasks
    n_slot = n_part * 8
    n_all = 2 * n_model
    slot_of_me = me * 2 + core
    px, py, pz = lax.rem(me, ring), lax.rem(lax.div(me, ring), ring), lax.div(me, plane)
    group = lax.div(me, ring)
    partner = peer(me, 1 - core)
    wide = 256
    cuts = [(c, min(wide, hidden - c)) for c in range(0, hidden, wide)]

    def at(x, y, z):
        model = lax.rem(z + ring, ring) * plane + lax.rem(y + ring, ring) * ring + lax.rem(x + ring, ring)
        return peer(model, core)

    def remote(src, dst, ssem, rsem, dev):
        return pltpu.make_async_remote_copy(src_ref=src, dst_ref=dst, send_sem=ssem, recv_sem=rsem,
                                            device_id=dev, device_id_type=MESH)

    def other(k):
        return peer(lax.rem(me + k // 2, n_model), 1 - core if k % 2 else core)

    sem = pltpu.get_barrier_semaphore()

    for k in range(1, n_all):
        pl.semaphore_signal(sem, inc=1, device_id=other(k), device_id_type=MESH)

    def block_of(j, k):
        sub = lax.rem(2 * j + lax.div(k, plane), ring)
        shift = jnp.where(sub == 0, 2, jnp.where(sub == 1, 1, jnp.where(sub == 2, 3, 0)))
        return lax.rem(group + lax.rem(k, plane), plane) * ring + lax.rem(px + shift, ring)

    def fetch(j, slot):
        for half_run in range(2):
            first_block = block_of(j, half_run * plane) - group * ring
            for k in range(plane):
                row = (lax.rem(group + k, plane) * ring + first_block) * blk + lax.div(j, 2) * sub_blk
                pltpu.make_async_copy(x_ref.at[pl.ds(pl.multiple_of(row, sub_blk), sub_blk), :],
                                      xbuf.at[slot, pl.ds((half_run * plane + k) * sub_blk, sub_blk), :],
                                      xsem.at[slot]).start()

    def fetched(slot):
        pltpu.make_async_copy(xbuf.at[slot], xbuf.at[slot], xsem.at[slot]).wait()

    fetch(0, 0)
    w_cols = pl.ds(pl.multiple_of(core * off, LANES), win)
    far_cols = pl.ds(pl.multiple_of((1 - core) * off, LANES), win)
    mine = pl.ds(pl.multiple_of(me * blk, blk), blk)
    own = [pltpu.make_async_copy(x_ref.at[mine, w_cols], xz.at[0], lsem.at[0])]
    coords = ((py, pz), (pz, py))
    for h in range(2):
        c1, c2 = coords[h]
        own.append(pltpu.make_async_copy(w2_ref.at[pl.ds(h * half, half), w_cols],
                                         wslab.at[h, c2 * ring + c1], lsem.at[1 + h]))
    for c in own:
        c.start()

    def near(h, axis, d):
        y_axis = (h == 0) == (axis == 0)
        return at(px, py + d, pz) if y_axis else at(px, py, pz + d)

    def gather_copy(h, stage, way):
        c1, c2 = coords[h]
        d = 1 if way == 0 else -1
        sems = (wsend_sem.at[h, stage, way], wrecv_sem.at[h, stage, way])
        if stage == 0:
            src = w2_ref.at[pl.ds(h * half, half), w_cols]
            return remote(src, wslab.at[h, c2 * ring + c1], *sems, near(h, 0, d))
        if stage == 1:
            piece = c2 * ring + lax.rem(c1 - d + ring, ring)
            ref = wslab.at[h, piece, pl.ds(way * (half // 2), half // 2), :]
            return remote(ref, ref, *sems, near(h, 0, d))
        if stage == 2:
            ref = wslab.at[h, pl.ds(c2 * ring, ring)]
            return remote(ref, ref, *sems, near(h, 1, d))
        ref = wslab.at[h, pl.ds(lax.rem(c2 - d + ring, ring) * ring + way * (ring // 2), ring // 2)]
        return remote(ref, ref, *sems, near(h, 1, d))

    hw = [(h, way) for h in range(2) for way in range(2)]
    dn_acc[...] = jnp.zeros_like(dn_acc)
    up_acc[...] = jnp.zeros_like(up_acc)
    w1t_ref[...] = w1_ref[...].T
    first = core * (win - hidden // 2)
    col = lax.broadcasted_iota(jnp.int32, (2 * n_task, win), 1)
    h_rows = jnp.concatenate([h_ref[t, c:c + 1, w_cols].astype(F32) for c in range(2) for t in range(n_task)], axis=0)
    ht_ref[...] = jnp.where((col >= first) & (col < first + hidden // 2), h_rows, 0.0).astype(BF16)
    for t in range(n_task):
        drow_ref[t] = h_ref[t, 0:1, :].astype(F32) - h_ref[t, 1:2, :].astype(F32)

    def spread(t, carry):
        dcol[t] = jnp.broadcast_to(drow_ref[t], (LANES, hidden)).T
        return carry

    lax.fori_loop(0, n_task, spread, 0)
    pl.semaphore_wait(sem, n_all - 1)
    far_x = remote(x_ref.at[mine, far_cols], xz.at[1], lsem.at[3], lsem.at[4], partner)
    for h, way in hw:
        gather_copy(h, 0, way).start()
    far_x.start()

    def forward(j, carry):
        slot = lax.rem(j, 2)

        @pl.when(j + 1 < n_tile)
        def _():
            fetch(j + 1, 1 - slot)

        fetched(slot)
        base = pl.multiple_of(j * tile, tile)
        step = min(512, tile)
        for n in range(0, tile, step):
            a = lax.dot_general(w1t_ref[...], xbuf[slot, n:n + step, :], NT, preferred_element_type=F32)
            a2 = a * a
            th = jnp.tanh(C_GELU * (a + K_GELU * (a * a2)))
            cdf = 0.5 * (1.0 + th)
            slope = cdf + a * (0.5 * (1.0 - th * th) * (C_GELU * (1.0 + (3.0 * K_GELU) * a2)))
            u_f = a * cdf
            ut_s[:, pl.ds(pl.multiple_of(base + n, step), step)] = u_f.astype(BF16)
            gp_s[:, pl.ds(pl.multiple_of(base + n, step), step)] = slope
            usend[pl.ds(pl.multiple_of(base + n, step), step), :] = u_f.T.astype(BF16)
        return carry

    def give(run, carry):
        part, sub = lax.div(run, ring), lax.rem(run, ring)
        dst = uslab.at[part, 0, sub, :, pl.ds(pl.multiple_of(group * width, width), width)]
        base = run * (plane * sub_blk)
        for k in range(plane):
            src = usend.at[pl.ds(pl.multiple_of(base + k * sub_blk, sub_blk), sub_blk), :]
            if k == 0:
                pltpu.make_async_copy(src, dst, urecv_sem.at[part, sub]).start()
            else:
                owner = lax.rem(group + k, plane) * ring + px
                remote(src, dst, usend_sem, urecv_sem.at[part, sub], peer(owner, core)).start()
        return carry

    def give_part(part):
        lax.fori_loop(part * ring, (part + 1) * ring, give, 0)

    lax.fori_loop(0, 1, forward, 0)
    lax.fori_loop(0, 1, give, 0)
    for h, way in hw:
        gather_copy(h, 0, way).wait_recv()
        gather_copy(h, 1, way).start()
    lax.fori_loop(1, 2, give, 0)
    lax.fori_loop(1, 2, forward, 0)
    for c in own:
        c.wait()
    for h, way in hw:
        gather_copy(h, 1, way).wait_recv()
    for h, way in hw:
        gather_copy(h, 2, way).start()
    lax.fori_loop(2, 4, give, 0)
    lax.fori_loop(2, n_tile, forward, 0)
    fetch(0, 0)
    for h, way in hw:
        gather_copy(h, 2, way).wait_recv()
        gather_copy(h, 3, way).start()
    give_part(1)

    def u_pair(part, s):
        return remote(uslab.at[part, 0, s], uslab.at[part, 1, s], psend_sem.at[part, s], precv_sem.at[part, s], partner)

    def u_arrive(part, s):
        ref = uslab.at[part, 0, s]
        pltpu.make_async_copy(ref, ref, urecv_sem.at[part, s]).wait()
        u_pair(part, s).start()

    def z_out(part, n, q):
        return part * 8 + n * 2 + q

    def z_relay(part, q):
        return n_slot + part * 2 + q

    def z_in(part, i, q):
        return n_slot + 2 * n_part + part * 4 + i * 2 + q

    def z_copy(part, n):
        left, right = at(px - 1, py, pz), at(px + 1, py, pz)
        src, dst, dev = ((zall.at[z_out(part, 0, 0)], zall.at[z_relay(part, 0)], right),
                         (zall.at[z_out(part, 0, 1)], zall.at[z_relay(part, 1)], left),
                         (zall.at[pl.ds(z_out(part, 1, 0), 2)], zall.at[pl.ds(z_in(part, 0, 0), 2)], right),
                         (zall.at[pl.ds(z_out(part, 2, 0), 2)], zall.at[pl.ds(z_in(part, 1, 0), 2)], left))[n]
        return remote(src, dst, zsend_sem.at[part, n], zrecv_sem.at[part, n], dev)

    def rows_of(g):
        y, z = g % ring, g // ring
        return [(0, z * ring + y), (1, y * ring + z)]

    def partial_z(part, subs, relayed):
        for c in range(0, win, wide):
            size = min(wide, win - c)
            total = jnp.zeros((2 * len(subs) * sub_blk, size), F32)
            for g in range(0, plane, 2):
                left = jnp.concatenate(
                    [uslab[part, q, s, :, g * width:(g + 2) * width] for s in subs for q in range(2)], axis=0)
                right = jnp.concatenate([wslab[h, i, :, c:c + size] for h, i in rows_of(g) + rows_of(g + 1)], axis=0)
                total = total + jnp.dot(left, right, preferred_element_type=F32)
            for i, s in enumerate(subs):
                for q in range(2):
                    v = total[(2 * i + q) * sub_blk:(2 * i + q + 1) * sub_blk]
                    if relayed and q == s - 1:
                        v = v + zall[z_relay(part, q), :, c:c + size]
                    zall[z_out(part, s, q), :, c:c + size] = v

    def z_first(s):
        u_pair(0, s).wait_recv()
        if s in (1, 2):
            z_copy(0, s - 1).wait_recv()
        partial_z(0, (s,), True)
        for n in ((0, 1), (2,), (3,), ())[s]:
            z_copy(0, n).start()

    def z_all(part):
        for s in range(4):
            u_pair(part, s).wait_recv()
        partial_z(part, (0, 1, 2, 3), False)
        z_copy(part, 0).start()
        z_copy(part, 1).start()

    def z_relay_on(part):
        for q in range(2):
            z_copy(part, q).wait_recv()
            zall[z_out(part, 1 + q, q)] += zall[z_relay(part, q)]
            z_copy(part, 2 + q).start()

    pad = jnp.zeros((n_task, blk - sub_blk), F32)

    def swap(part):
        return remote(lsend.at[part], lrecv.at[part], ssend_sem.at[part], srecv_sem.at[part], partner)

    def e_logits(part):
        z_copy(part, 2).wait_recv()
        z_copy(part, 3).wait_recv()
        for n in range(4):
            z_copy(part, n).wait_send()
        gaps = []
        rows = pl.ds(pl.multiple_of(part * sub_blk, sub_blk), sub_blk)
        for q in range(2):
            z = (xz[q, rows, :].astype(F32) + ((zall[z_out(part, 3, q)] + zall[z_in(part, 0, q)])
                                               + zall[z_in(part, 1, q)])).astype(BF16)
            gaps.append(lax.dot_general(ht_ref[...], z, NT, preferred_element_type=F32))
        both = jnp.concatenate([pad, pad], axis=0)
        lown[part] = jnp.concatenate([gaps[0], both], axis=1)
        lsend[part] = jnp.concatenate([gaps[1], both], axis=1)
        swap(part).start()

    def e_out(part):
        swap(part).wait()
        logit = lown[part] + lrecv[part]
        gap = logit[:n_task, :] - logit[n_task:, :]
        first_class = pltpu.roll(lab_ref[:, mine], lax.rem(blk - part * sub_blk, blk), 1) == 0
        wrong = 1.0 / (1.0 + jnp.exp(jnp.where(first_class, gap, -gap)))
        esend[part] = jnp.where(first_class, -wrong, wrong) * (1.0 / n_total)
        dst = et.at[part, me]

        for k in range(1, n_model):
            remote(esend.at[part], dst, esend_sem.at[part], erecv_sem.at[part],
                   peer(lax.rem(me + k, n_model), core)).start()
        pltpu.make_async_copy(esend.at[part], dst, erecv_sem.at[part]).start()

    def e_in(part):
        pltpu.make_async_copy(et.at[part], et.at[part], erecv_sem.at[part]).wait()

    def u_in(part):
        for s in range(4):
            u_arrive(part, s)

    u_in(0)
    for h, way in hw:
        gather_copy(h, 3, way).wait_recv()
    for s in range(4):
        z_first(s)
    far_x.wait_recv()
    e_logits(0)
    e_out(0)
    u_in(1)
    z_all(1)
    e_in(0)
    z_relay_on(1)
    give_part(2)

    def far_down(t):
        rows = pl.ds(pl.multiple_of(lax.rem(t, 2) * half, half), half)
        return gp_s.at[rows, pl.ds(pl.multiple_of(lax.div(t, 2) * hidden, LANES), hidden)]

    def grad_copies(t):
        out = [remote(dn_acc.at[t, pl.ds(pl.multiple_of((1 - core) * half, half), half), :], far_down(t),
                      gsend_sem.at[0, t], grecv_sem.at[0, t], partner)]
        for i in range(n_part):
            rows = pl.ds(pl.multiple_of(t * width + i * sub_blk, sub_blk), sub_blk)
            out.append(remote(up_acc.at[rows, far_cols], zall.at[n_part * t + i],
                              gsend_sem.at[1, t], grecv_sem.at[1, t], partner))
        return out

    def grad_tile(j, carry):
        slot = lax.rem(j, 2)

        @pl.when(j + 1 < n_tile)
        def _():
            fetch(j + 1, 1 - slot)

        @pl.when(j == n_tile - 1)
        def _():
            pl.semaphore_signal(free_sem, inc=1, device_id=partner, device_id_type=MESH)

        part = lax.div(j, 2)

        @pl.when((lax.rem(j, 2) == 0) & (j > 0))
        def _():
            e_in(part)

        for k in range(0, 2 * plane, n_part):
            pieces = [et[part, block_of(j, k + i)][:, :sub_blk] for i in range(n_part)]
            e_pair = jnp.concatenate(pieces, axis=1)
            for t in range(n_task):
                ebr[t, :, k * sub_blk:(k + n_part) * sub_blk] = e_pair[t:t + 1, :]
        fetched(slot)
        base = pl.multiple_of(j * tile, tile)

        def some_tasks(m, carry):
            rows = pl.ds(pl.multiple_of(body_tasks * m * width, body_tasks * width), body_tasks * width)
            for q in range(body_tasks):
                t = body_tasks * m + q
                for n in range(0, tile, wide):
                    n_size = min(wide, tile)
                    e_n = ebr[t, :, n:n + n_size]
                    da = jnp.zeros((width, n_size), F32)
                    for c, size in cuts:
                        d_c = jnp.concatenate([dcol[t, c:c + size, :]] * (n_size // LANES), axis=1)
                        dz_t = (d_c * e_n).astype(BF16)
                        da = da + jnp.dot(w2_ref[:, c:c + size], dz_t, preferred_element_type=F32)
                    cols = pl.ds(pl.multiple_of(base + n, n_size), n_size)
                    dat[q * width:(q + 1) * width, n:n + n_size] = (da * gp_s[:, cols]).astype(BF16)
            left = ut_s[:, pl.ds(base, tile)]
            for q in range(0, body_tasks, 2):
                ts = (body_tasks * m + q, body_tasks * m + q + 1)
                e_col = [jnp.broadcast_to(ebr[t], (LANES, tile)).T for t in ts]
                for i, t in enumerate(ts):
                    for c, size in cuts:
                        if size == wide:
                            e_b = jnp.concatenate([e_col[i]] * (size // LANES), axis=1)
                            dz = (e_b * drow_ref[t, :, c:c + size]).astype(BF16)
                            dn_acc[t, :, c:c + size] += jnp.dot(left, dz, preferred_element_type=F32)
                c, size = cuts[-1]
                if size < wide:
                    dz = jnp.concatenate([e_col[i] * drow_ref[t, :, c:c + size] for i, t in enumerate(ts)],
                                         axis=1).astype(BF16)
                    both = jnp.dot(left, dz, preferred_element_type=F32)
                    for i, t in enumerate(ts):
                        dn_acc[t, :, c:c + size] += both[:, i * size:(i + 1) * size]
            left = dat[...]
            for c, size in cuts:
                up_acc[rows, c:c + size] += jnp.dot(left, xbuf[slot, :, c:c + size], preferred_element_type=F32)

            @pl.when((j == n_tile - 1) & (m == 0))
            def _():
                pl.semaphore_wait(free_sem, 1)

            @pl.when(j == n_tile - 1)
            def _():
                for q in range(body_tasks):
                    for c in grad_copies(body_tasks * m + q):
                        c.start()
            hook = lax.rem(j, 2) * n_body + m
            ahead = part + 1

            @pl.when((hook == 0) & (ahead < n_part))
            def _():
                e_logits(ahead)

            @pl.when((hook == 1) & (ahead < n_part))
            def _():
                e_out(ahead)

            @pl.when((hook == 1) & (ahead + 1 < n_part))
            def _():
                u_in(ahead + 1)

            @pl.when((hook == 2) & (ahead + 1 < n_part))
            def _():
                z_all(ahead + 1)

            @pl.when((hook == 2) & (ahead + 2 < n_part))
            def _():
                give_part(ahead + 2)

            @pl.when((hook == 3) & (ahead + 1 < n_part))
            def _():
                z_relay_on(ahead + 1)
            return carry

        lax.fori_loop(0, n_body, some_tasks, 0)
        return carry

    lax.fori_loop(0, n_tile, grad_tile, 0)

    def up_slots(t):
        return zall.at[pl.ds(pl.multiple_of(n_part * t, n_part), n_part)]

    def landed(t, carry):
        grad_copies(t)[0].wait_recv()
        pltpu.make_async_copy(up_slots(t), up_slots(t), grecv_sem.at[1, t]).wait()
        return carry

    lax.fori_loop(0, n_task, landed, 0)
    pairs = [(t, s) for t in range(n_task) for s in range(t, n_task)]
    lane = lax.broadcasted_iota(jnp.int32, (8, LANES), 1)

    def gram_of(vals, sums):
        return tuple(acc + vals[t] * vals[s] for acc, (t, s) in zip(sums, pairs))

    n_row = sub_blk // 8

    def down_at(t, r, c):
        return (pl.ds(pl.multiple_of((t % 2) * half + r * 8, 8), 8), slice((t // 2) * hidden + c, (t // 2) * hidden + c + LANES))

    def down_sum(t, r, c):
        from_acc = pl.ds(pl.multiple_of(core * half + r * 8, 8), 8)
        return dn_acc[t, from_acc, c:c + LANES] + gp_s[down_at(t, r, c)]

    def up_sum(t, n, c):
        rows = pl.ds(pl.multiple_of(lax.rem(n, n_row) * 8, 8), 8)
        from_acc = pl.ds(pl.multiple_of(t * width + n * 8, 8), 8)
        return (up_acc[from_acc, pl.ds(pl.multiple_of(core * off + c, LANES), LANES)]
                + zall[n_part * t + lax.div(n, n_row), rows, c:c + LANES])

    def fold_down(r, sums):
        for c in range(0, hidden, LANES):
            vals = []
            for t in range(n_task):
                vals.append(down_sum(t, r, c))
            sums = gram_of(vals, sums)
        return sums

    def fold_up(n, sums):
        for c in range(0, win, LANES):
            edge = c < win - hidden // 2 or c + LANES > hidden // 2
            vals = []
            for t in range(n_task):
                v = up_sum(t, n, c)
                vals.append(jnp.where((lane + c >= first) & (lane + c < first + hidden // 2), v, 0.0) if edge else v)
            sums = gram_of(vals, sums)
        return sums

    sums = tuple(jnp.zeros((8, LANES), F32) for _ in pairs)
    sums = lax.fori_loop(0, half // 8, fold_down, sums)
    sums = lax.fori_loop(0, width // 8, fold_up, sums)
    lane1 = lax.broadcasted_iota(jnp.int32, (1, LANES), 1)
    row = lax.broadcasted_iota(jnp.int32, (8, LANES), 0)
    out = jnp.zeros((1, LANES), F32)
    for acc, (t, s) in zip(sums, pairs):
        total = jnp.sum(jnp.sum(acc, axis=0, keepdims=True), axis=1, keepdims=True)
        out = out + jnp.where((lane1 == t * n_task + s) | (lane1 == s * n_task + t), total, 0.0)
    msend[...] = out

    for k in range(1, n_all):
        remote(msend, mrecv.at[slot_of_me], msend_sem, mrecv_sem, other(k)).start()
    pltpu.make_async_copy(msend, mrecv.at[slot_of_me], mrecv_sem).start()
    pltpu.make_async_copy(mrecv, mrecv, mrecv_sem).wait()
    flat = jnp.sum(mrecv[...], axis=0)
    gram = jnp.zeros((8, LANES), F32)
    for t in range(n_task):
        line = flat if t == 0 else pltpu.roll(flat, LANES - t * n_task, 1)
        gram = gram + jnp.where((row == t) & (lane < n_task), jnp.broadcast_to(line, (8, LANES)), 0.0)
    scale = jnp.sum(jnp.sum(jnp.where(row == lane, gram, 0.0), axis=1, keepdims=True), axis=0, keepdims=True) / n_task
    gram = gram / scale
    w = jnp.where(lane < n_task, 1.0 / n_task, 0.0).astype(F32)

    def eg_pair(i, w):
        v = jnp.sum(gram * w, axis=1, keepdims=True)
        w_col = jnp.sum(jnp.where(row == lane, w, 0.0), axis=1, keepdims=True)
        w_col = w_col * jnp.exp(-v)
        w_col = w_col / jnp.sum(w_col, axis=0, keepdims=True)
        v = jnp.sum(gram * w_col, axis=0, keepdims=True)
        w_row = jnp.sum(jnp.where(row == lane, w_col, 0.0), axis=0, keepdims=True)
        w_row = w_row * jnp.exp(-v)
        w_row = w_row / jnp.sum(w_row, axis=1, keepdims=True)
        return jnp.broadcast_to(w_row, (8, LANES))

    w = lax.fori_loop(0, STEPS // 2, eg_pair, w)
    a_ref[...] = w
    a = [jnp.broadcast_to(jnp.sum(jnp.where(lane == t, w, 0.0), axis=1, keepdims=True), (8, LANES))
         for t in range(n_task)]

    def weigh(parts):
        parts = [a[t] * v for t, v in enumerate(parts)]
        while len(parts) > 1:
            parts = [parts[i] + parts[i + 1] for i in range(0, len(parts), 2)]
        return parts[0]

    def mix_down(r, carry):
        rows = pl.ds(pl.multiple_of(r * 8, 8), 8)
        for c in range(0, hidden, LANES):
            g2_ref[rows, c:c + LANES] = weigh([down_sum(t, r, c) for t in range(n_task)])
        return carry

    def mix_up(n, carry):
        rows = pl.ds(pl.multiple_of(n * 8, 8), 8)
        for c in range(0, win, LANES):
            g1s[rows, c:c + LANES] = weigh([up_sum(t, n, c) for t in range(n_task)])
        return carry

    lax.fori_loop(0, half // 8, mix_down, 0)
    lax.fori_loop(0, width // 8, mix_up, 0)
    for c in range(0, win, LANES):
        g1t[c:c + LANES, :] = g1s[:, c:c + LANES].T
    g1_ref[...] = g1t[pl.ds(pl.multiple_of(first, 8), hidden // 2), :]

    for h, way in hw:
        for stage in range(4):
            gather_copy(h, stage, way).wait_send()
    for part in range(n_part):
        for s in range(4):
            u_pair(part, s).wait_send()
        sent = et.at[part, pl.ds(0, n_model - 1)]
        pltpu.make_async_copy(sent, sent, esend_sem.at[part]).wait()
    far_x.wait_send()
    sent = usend.at[pl.ds(0, n_tok - ring * blk), :]
    pltpu.make_async_copy(sent, sent, usend_sem).wait()

    def gone(t, carry):
        grad_copies(t)[0].wait_send()
        pltpu.make_async_copy(up_slots(t), up_slots(t), gsend_sem.at[1, t]).wait()
        return carry

    lax.fori_loop(0, n_task, gone, 0)
    sent = mrecv.at[pl.ds(0, n_all - 1)]
    pltpu.make_async_copy(sent, sent, msend_sem).wait()


def solution(mesh):
    n_model, n_data = mesh.shape['model'], mesh.shape['data']

    def local_step(tokens, w_up, w_down, task_heads, labels):
        n_tok, hidden = tokens.shape
        n_total = n_tok * n_data
        width = w_up.shape[1]
        n_task = task_heads.shape[0]
        blk = n_tok // n_model
        sub_blk = blk // 4
        half = width // 2
        win = -(-(hidden // 2) // LANES) * LANES
        tile = 32 * sub_blk
        any_spec = pl.BlockSpec(memory_space=pl.ANY)
        vmem_spec = pl.BlockSpec(memory_space=pltpu.VMEM)
        dma = pltpu.SemaphoreType.DMA
        vmem = pltpu.VMEM
        weights, grad_up, grad_down = pl.pallas_call(
            functools.partial(step_kernel, n_model, win, n_total),
            out_shape=(jax.ShapeDtypeStruct((8, LANES), F32), jax.ShapeDtypeStruct((hidden // 2, width), F32),
                       jax.ShapeDtypeStruct((half, hidden), F32)),
            in_specs=[any_spec, vmem_spec, vmem_spec, vmem_spec, vmem_spec],
            out_specs=(vmem_spec, vmem_spec, vmem_spec),
            scratch_shapes=[vmem((width, hidden), BF16), vmem((2 * n_task, win), BF16), vmem((n_task, 1, hidden), F32),
                            vmem((2, tile, hidden), BF16), vmem((n_tok, width), BF16), vmem((width, n_tok), BF16),
                            vmem((width, n_tok), F32), vmem((4, 2, 4, sub_blk, 16 * width), BF16),
                            vmem((2, 16, half, win), BF16), vmem((2, blk, win), BF16),
                            vmem((56, sub_blk, win), F32), vmem((4, 2 * n_task, blk), F32),
                            vmem((4, 2 * n_task, blk), F32), vmem((4, 2 * n_task, blk), F32),
                            vmem((4, n_task, blk), F32), vmem((4, n_model, n_task, blk), F32),
                            vmem((n_task, width, hidden), F32), vmem((n_task * width, hidden), F32),
                            vmem((n_task, hidden, LANES), F32), vmem((n_task, 1, tile), F32), vmem((4 * width, tile), BF16),
                            vmem((1, LANES), F32), vmem((2 * n_model, 1, LANES), F32), vmem((width, win), F32), vmem((win, width), F32),
                            dma((2,)), dma, dma((4, 4)), dma((2, 4, 2)), dma((2, 4, 2)), dma((4, 4)), dma((4, 4)),
                            dma((4, 4)), dma((4, 4)), dma((4,)), dma((4,)), dma((4,)), dma((4,)), dma((5,)),
                            dma((2, n_task)), dma((2, n_task)), dma, dma, pltpu.SemaphoreType.REGULAR],
            compiler_params=pltpu.CompilerParams(collective_id=0, has_side_effects=True, vmem_limit_bytes=67043328),
            name='step')(tokens, w_up, w_down, jnp.transpose(task_heads, (0, 2, 1)), labels)
        return weights[0, :n_task], grad_up, grad_down

    return jax.shard_map(
        local_step, mesh=mesh,
        in_specs=(P('data', None), P(None, 'model'), P('model', None), P(None, None, None), P(None, 'data')),
        out_specs=(P(None), P('data', 'model'), P(('model', 'data'), None)),
        check_vma=False)
```

```python
import functools

import jax
import jax.numpy as jnp
from jax import lax
from jax.experimental import pallas as pl
from jax.experimental.pallas import tpu as pltpu
from jax.sharding import PartitionSpec as P

STEPS = 20
LANES = 128
MESH = pl.DeviceIdType.MESH
F32 = jnp.float32
BF16 = jnp.bfloat16
C_GELU = 0.7978845608028654
K_GELU = 0.044715
NT = (((1,), (1,)), ((), ()))


def peer(model, data):
    return {"model": model, "data": data}


def step_kernel(n_model, win, n_total, x_ref, w1_ref, w2_ref, h_ref, lab_ref, a_ref, g1_ref, g2_ref,
                w1t_ref, ht_ref, drow_ref, xbuf, usend, ut_s, gp_s, uslab, wslab, xz, zall, lown, lsend, lrecv, esend, et,
                dn_acc, up_acc, dcol, ebr, dat, msend, mrecv, g1s, g1t,
                xsem, usend_sem, urecv_sem, wsend_sem, wrecv_sem, psend_sem, precv_sem, zsend_sem, zrecv_sem,
                esend_sem, erecv_sem, ssend_sem, srecv_sem, lsem, gsend_sem, grecv_sem, msend_sem, mrecv_sem, free_sem):
    me = lax.axis_index("model")
    core = lax.axis_index("data")
    ring = 4
    plane = ring * ring
    n_tok, hidden = x_ref.shape
    blk = n_tok // n_model
    n_part = 4
    sub_blk = blk // n_part
    width = w1_ref.shape[1]
    half = width // 2
    n_task = lab_ref.shape[0]
    off = hidden - win
    tile = 2 * plane * sub_blk
    n_tile = 2 * n_part
    body_tasks = 4
    n_body = n_task // body_tasks
    n_slot = n_part * 8
    n_all = 2 * n_model
    slot_of_me = me * 2 + core
    px, py, pz = lax.rem(me, ring), lax.rem(lax.div(me, ring), ring), lax.div(me, plane)
    group = lax.div(me, ring)
    partner = peer(me, 1 - core)
    wide = 256
    cuts = [(c, min(wide, hidden - c)) for c in range(0, hidden, wide)]

    def at(x, y, z):
        model = lax.rem(z + ring, ring) * plane + lax.rem(y + ring, ring) * ring + lax.rem(x + ring, ring)
        return peer(model, core)

    def remote(src, dst, ssem, rsem, dev):
        return pltpu.make_async_remote_copy(src_ref=src, dst_ref=dst, send_sem=ssem, recv_sem=rsem,
                                            device_id=dev, device_id_type=MESH)

    def other(k):
        return peer(lax.rem(me + k // 2, n_model), 1 - core if k % 2 else core)

    sem = pltpu.get_barrier_semaphore()

    for k in range(1, n_all):
        pl.semaphore_signal(sem, inc=1, device_id=other(k), device_id_type=MESH)

    def block_of(j, k):
        sub = lax.rem(2 * j + lax.div(k, plane), ring)
        shift = jnp.where(sub == 0, 2, jnp.where(sub == 1, 1, jnp.where(sub == 2, 3, 0)))
        return lax.rem(group + lax.rem(k, plane), plane) * ring + lax.rem(px + shift, ring)

    def fetch(j, slot):
        for half_run in range(2):
            first_block = block_of(j, half_run * plane) - group * ring
            for k in range(plane):
                row = (lax.rem(group + k, plane) * ring + first_block) * blk + lax.div(j, 2) * sub_blk
                pltpu.make_async_copy(x_ref.at[pl.ds(pl.multiple_of(row, sub_blk), sub_blk), :],
                                      xbuf.at[slot, pl.ds((half_run * plane + k) * sub_blk, sub_blk), :],
                                      xsem.at[slot]).start()

    def fetched(slot):
        pltpu.make_async_copy(xbuf.at[slot], xbuf.at[slot], xsem.at[slot]).wait()

    fetch(0, 0)
    w_cols = pl.ds(pl.multiple_of(core * off, LANES), win)
    far_cols = pl.ds(pl.multiple_of((1 - core) * off, LANES), win)
    mine = pl.ds(pl.multiple_of(me * blk, blk), blk)
    own = [pltpu.make_async_copy(x_ref.at[mine, w_cols], xz.at[0], lsem.at[0])]
    coords = ((py, pz), (pz, py))
    for h in range(2):
        c1, c2 = coords[h]
        own.append(pltpu.make_async_copy(w2_ref.at[pl.ds(h * half, half), w_cols],
                                         wslab.at[h, c2 * ring + c1], lsem.at[1 + h]))
    for c in own:
        c.start()

    def near(h, axis, d):
        y_axis = (h == 0) == (axis == 0)
        return at(px, py + d, pz) if y_axis else at(px, py, pz + d)

    def gather_copy(h, stage, way):
        c1, c2 = coords[h]
        d = 1 if way == 0 else -1
        sems = (wsend_sem.at[h, stage, way], wrecv_sem.at[h, stage, way])
        if stage == 0:
            src = w2_ref.at[pl.ds(h * half, half), w_cols]
            return remote(src, wslab.at[h, c2 * ring + c1], *sems, near(h, 0, d))
        if stage == 1:
            piece = c2 * ring + lax.rem(c1 - d + ring, ring)
            ref = wslab.at[h, piece, pl.ds(way * (half // 2), half // 2), :]
            return remote(ref, ref, *sems, near(h, 0, d))
        if stage == 2:
            ref = wslab.at[h, pl.ds(c2 * ring, ring)]
            return remote(ref, ref, *sems, near(h, 1, d))
        ref = wslab.at[h, pl.ds(lax.rem(c2 - d + ring, ring) * ring + way * (ring // 2), ring // 2)]
        return remote(ref, ref, *sems, near(h, 1, d))

    hw = [(h, way) for h in range(2) for way in range(2)]
    dn_acc[...] = jnp.zeros_like(dn_acc)
    up_acc[...] = jnp.zeros_like(up_acc)
    w1t_ref[...] = w1_ref[...].T
    first = core * (win - hidden // 2)
    col = lax.broadcasted_iota(jnp.int32, (2 * n_task, win), 1)
    h_rows = jnp.concatenate([h_ref[t, c:c + 1, w_cols].astype(F32) for c in range(2) for t in range(n_task)], axis=0)
    ht_ref[...] = jnp.where((col >= first) & (col < first + hidden // 2), h_rows, 0.0).astype(BF16)
    for t in range(n_task):
        drow_ref[t] = h_ref[t, 0:1, :].astype(F32) - h_ref[t, 1:2, :].astype(F32)

    def spread(t, carry):
        dcol[t] = jnp.broadcast_to(drow_ref[t], (LANES, hidden)).T
        return carry

    lax.fori_loop(0, n_task, spread, 0)
    pl.semaphore_wait(sem, n_all - 1)
    far_x = remote(x_ref.at[mine, far_cols], xz.at[1], lsem.at[3], lsem.at[4], partner)
    for h, way in hw:
        gather_copy(h, 0, way).start()
    far_x.start()

    def forward(j, carry):
        slot = lax.rem(j, 2)

        @pl.when(j + 1 < n_tile)
        def _():
            fetch(j + 1, 1 - slot)

        fetched(slot)
        base = pl.multiple_of(j * tile, tile)
        step = min(512, tile)
        for n in range(0, tile, step):
            a = lax.dot_general(w1t_ref[...], xbuf[slot, n:n + step, :], NT, preferred_element_type=F32)
            a2 = a * a
            th = jnp.tanh(C_GELU * (a + K_GELU * (a * a2)))
            cdf = 0.5 * (1.0 + th)
            slope = cdf + a * (0.5 * (1.0 - th * th) * (C_GELU * (1.0 + (3.0 * K_GELU) * a2)))
            u_f = a * cdf
            ut_s[:, pl.ds(pl.multiple_of(base + n, step), step)] = u_f.astype(BF16)
            gp_s[:, pl.ds(pl.multiple_of(base + n, step), step)] = slope
            usend[pl.ds(pl.multiple_of(base + n, step), step), :] = u_f.T.astype(BF16)
        return carry

    def give(run, carry):
        part, sub = lax.div(run, ring), lax.rem(run, ring)
        dst = uslab.at[part, 0, sub, :, pl.ds(pl.multiple_of(group * width, width), width)]
        base = run * (plane * sub_blk)
        for k in range(plane):
            src = usend.at[pl.ds(pl.multiple_of(base + k * sub_blk, sub_blk), sub_blk), :]
            if k == 0:
                pltpu.make_async_copy(src, dst, urecv_sem.at[part, sub]).start()
            else:
                owner = lax.rem(group + k, plane) * ring + px
                remote(src, dst, usend_sem, urecv_sem.at[part, sub], peer(owner, core)).start()
        return carry

    def give_part(part):
        lax.fori_loop(part * ring, (part + 1) * ring, give, 0)

    lax.fori_loop(0, 1, forward, 0)
    lax.fori_loop(0, 1, give, 0)
    for h, way in hw:
        gather_copy(h, 0, way).wait_recv()
        gather_copy(h, 1, way).start()
    lax.fori_loop(1, 2, give, 0)
    lax.fori_loop(1, 2, forward, 0)
    for c in own:
        c.wait()
    for h, way in hw:
        gather_copy(h, 1, way).wait_recv()
    for h, way in hw:
        gather_copy(h, 2, way).start()
    lax.fori_loop(2, 4, give, 0)
    lax.fori_loop(2, n_tile, forward, 0)
    fetch(0, 0)
    for h, way in hw:
        gather_copy(h, 2, way).wait_recv()
        gather_copy(h, 3, way).start()
    give_part(1)

    def u_pair(part, s):
        return remote(uslab.at[part, 0, s], uslab.at[part, 1, s], psend_sem.at[part, s], precv_sem.at[part, s], partner)

    def u_arrive(part, s):
        ref = uslab.at[part, 0, s]
        pltpu.make_async_copy(ref, ref, urecv_sem.at[part, s]).wait()
        u_pair(part, s).start()

    def z_out(part, n, q):
        return part * 8 + n * 2 + q

    def z_relay(part, q):
        return n_slot + part * 2 + q

    def z_in(part, i, q):
        return n_slot + 2 * n_part + part * 4 + i * 2 + q

    def z_copy(part, n):
        left, right = at(px - 1, py, pz), at(px + 1, py, pz)
        src, dst, dev = ((zall.at[z_out(part, 0, 0)], zall.at[z_relay(part, 0)], right),
                         (zall.at[z_out(part, 0, 1)], zall.at[z_relay(part, 1)], left),
                         (zall.at[pl.ds(z_out(part, 1, 0), 2)], zall.at[pl.ds(z_in(part, 0, 0), 2)], right),
                         (zall.at[pl.ds(z_out(part, 2, 0), 2)], zall.at[pl.ds(z_in(part, 1, 0), 2)], left))[n]
        return remote(src, dst, zsend_sem.at[part, n], zrecv_sem.at[part, n], dev)

    def rows_of(g):
        y, z = g % ring, g // ring
        return [(0, z * ring + y), (1, y * ring + z)]

    def partial_z(part, subs, relayed):
        for c in range(0, win, wide):
            size = min(wide, win - c)
            total = jnp.zeros((2 * len(subs) * sub_blk, size), F32)
            for g in range(0, plane, 2):
                left = jnp.concatenate(
                    [uslab[part, q, s, :, g * width:(g + 2) * width] for s in subs for q in range(2)], axis=0)
                right = jnp.concatenate([wslab[h, i, :, c:c + size] for h, i in rows_of(g) + rows_of(g + 1)], axis=0)
                total = total + jnp.dot(left, right, preferred_element_type=F32)
            for i, s in enumerate(subs):
                for q in range(2):
                    v = total[(2 * i + q) * sub_blk:(2 * i + q + 1) * sub_blk]
                    if relayed and q == s - 1:
                        v = v + zall[z_relay(part, q), :, c:c + size]
                    zall[z_out(part, s, q), :, c:c + size] = v

    def z_first(s):
        u_pair(0, s).wait_recv()
        if s in (1, 2):
            z_copy(0, s - 1).wait_recv()
        partial_z(0, (s,), True)
        for n in ((0, 1), (2,), (3,), ())[s]:
            z_copy(0, n).start()

    def z_all(part):
        for s in range(4):
            u_pair(part, s).wait_recv()
        partial_z(part, (0, 1, 2, 3), False)
        z_copy(part, 0).start()
        z_copy(part, 1).start()

    def z_relay_on(part):
        for q in range(2):
            z_copy(part, q).wait_recv()
            zall[z_out(part, 1 + q, q)] += zall[z_relay(part, q)]
            z_copy(part, 2 + q).start()

    pad = jnp.zeros((n_task, blk - sub_blk), F32)

    def swap(part):
        return remote(lsend.at[part], lrecv.at[part], ssend_sem.at[part], srecv_sem.at[part], partner)

    def e_logits(part):
        z_copy(part, 2).wait_recv()
        z_copy(part, 3).wait_recv()
        for n in range(4):
            z_copy(part, n).wait_send()
        gaps = []
        rows = pl.ds(pl.multiple_of(part * sub_blk, sub_blk), sub_blk)
        for q in range(2):
            z = (xz[q, rows, :].astype(F32) + ((zall[z_out(part, 3, q)] + zall[z_in(part, 0, q)])
                                               + zall[z_in(part, 1, q)])).astype(BF16)
            gaps.append(lax.dot_general(ht_ref[...], z, NT, preferred_element_type=F32))
        both = jnp.concatenate([pad, pad], axis=0)
        lown[part] = jnp.concatenate([gaps[0], both], axis=1)
        lsend[part] = jnp.concatenate([gaps[1], both], axis=1)
        swap(part).start()

    def e_out(part):
        swap(part).wait()
        logit = lown[part] + lrecv[part]
        gap = logit[:n_task, :] - logit[n_task:, :]
        first_class = pltpu.roll(lab_ref[:, mine], lax.rem(blk - part * sub_blk, blk), 1) == 0
        wrong = 1.0 / (1.0 + jnp.exp(jnp.where(first_class, gap, -gap)))
        esend[part] = jnp.where(first_class, -wrong, wrong) * (1.0 / n_total)
        dst = et.at[part, me]

        for k in range(1, n_model):
            remote(esend.at[part], dst, esend_sem.at[part], erecv_sem.at[part],
                   peer(lax.rem(me + k, n_model), core)).start()
        pltpu.make_async_copy(esend.at[part], dst, erecv_sem.at[part]).start()

    def e_in(part):
        pltpu.make_async_copy(et.at[part], et.at[part], erecv_sem.at[part]).wait()

    def u_in(part):
        for s in range(4):
            u_arrive(part, s)

    u_in(0)
    for h, way in hw:
        gather_copy(h, 3, way).wait_recv()
    for s in range(4):
        z_first(s)
    far_x.wait_recv()
    e_logits(0)
    e_out(0)
    u_in(1)
    z_all(1)
    e_in(0)
    z_relay_on(1)
    give_part(2)

    def far_down(t):
        rows = pl.ds(pl.multiple_of(lax.rem(t, 2) * half, half), half)
        return gp_s.at[rows, pl.ds(pl.multiple_of(lax.div(t, 2) * hidden, LANES), hidden)]

    def grad_copies(t):
        out = [remote(dn_acc.at[t, pl.ds(pl.multiple_of((1 - core) * half, half), half), :], far_down(t),
                      gsend_sem.at[0, t], grecv_sem.at[0, t], partner)]
        for i in range(n_part):
            rows = pl.ds(pl.multiple_of(t * width + i * sub_blk, sub_blk), sub_blk)
            out.append(remote(up_acc.at[rows, far_cols], zall.at[n_part * t + i],
                              gsend_sem.at[1, t], grecv_sem.at[1, t], partner))
        return out

    def grad_tile(j, carry):
        slot = lax.rem(j, 2)

        @pl.when(j + 1 < n_tile)
        def _():
            fetch(j + 1, 1 - slot)

        @pl.when(j == n_tile - 1)
        def _():
            pl.semaphore_signal(free_sem, inc=1, device_id=partner, device_id_type=MESH)

        part = lax.div(j, 2)

        @pl.when((lax.rem(j, 2) == 0) & (j > 0))
        def _():
            e_in(part)

        for k in range(0, 2 * plane, n_part):
            pieces = [et[part, block_of(j, k + i)][:, :sub_blk] for i in range(n_part)]
            e_pair = jnp.concatenate(pieces, axis=1)
            for t in range(n_task):
                ebr[t, :, k * sub_blk:(k + n_part) * sub_blk] = e_pair[t:t + 1, :]
        fetched(slot)
        base = pl.multiple_of(j * tile, tile)

        def some_tasks(m, carry):
            rows = pl.ds(pl.multiple_of(body_tasks * m * width, body_tasks * width), body_tasks * width)
            for q in range(body_tasks):
                t = body_tasks * m + q
                for n in range(0, tile, wide):
                    n_size = min(wide, tile)
                    e_n = ebr[t, :, n:n + n_size]
                    da = jnp.zeros((width, n_size), F32)
                    for c, size in cuts:
                        d_c = jnp.concatenate([dcol[t, c:c + size, :]] * (n_size // LANES), axis=1)
                        dz_t = (d_c * e_n).astype(BF16)
                        da = da + jnp.dot(w2_ref[:, c:c + size], dz_t, preferred_element_type=F32)
                    cols = pl.ds(pl.multiple_of(base + n, n_size), n_size)
                    dat[q * width:(q + 1) * width, n:n + n_size] = (da * gp_s[:, cols]).astype(BF16)
            left = ut_s[:, pl.ds(base, tile)]
            for q in range(0, body_tasks, 2):
                ts = (body_tasks * m + q, body_tasks * m + q + 1)
                e_col = [jnp.broadcast_to(ebr[t], (LANES, tile)).T for t in ts]
                for i, t in enumerate(ts):
                    for c, size in cuts:
                        if size == wide:
                            e_b = jnp.concatenate([e_col[i]] * (size // LANES), axis=1)
                            dz = (e_b * drow_ref[t, :, c:c + size]).astype(BF16)
                            dn_acc[t, :, c:c + size] += jnp.dot(left, dz, preferred_element_type=F32)
                c, size = cuts[-1]
                if size < wide:
                    dz = jnp.concatenate([e_col[i] * drow_ref[t, :, c:c + size] for i, t in enumerate(ts)],
                                         axis=1).astype(BF16)
                    both = jnp.dot(left, dz, preferred_element_type=F32)
                    for i, t in enumerate(ts):
                        dn_acc[t, :, c:c + size] += both[:, i * size:(i + 1) * size]
            left = dat[...]
            for c, size in cuts:
                up_acc[rows, c:c + size] += jnp.dot(left, xbuf[slot, :, c:c + size], preferred_element_type=F32)

            @pl.when((j == n_tile - 1) & (m == 0))
            def _():
                pl.semaphore_wait(free_sem, 1)

            @pl.when(j == n_tile - 1)
            def _():
                copies = [grad_copies(body_tasks * m + q) for q in range(body_tasks)]
                for c in [c[0] for c in copies] + [c for group_of in copies for c in group_of[1:]]:
                    c.start()
            hook = lax.rem(j, 2) * n_body + m
            ahead = part + 1

            @pl.when((hook == 0) & (ahead < n_part))
            def _():
                e_logits(ahead)

            @pl.when((hook == 1) & (ahead < n_part))
            def _():
                e_out(ahead)

            @pl.when((hook == 1) & (ahead + 1 < n_part))
            def _():
                u_in(ahead + 1)

            @pl.when((hook == 2) & (ahead + 1 < n_part))
            def _():
                z_all(ahead + 1)

            @pl.when((hook == 2) & (ahead + 2 < n_part))
            def _():
                give_part(ahead + 2)

            @pl.when((hook == 3) & (ahead + 1 < n_part))
            def _():
                z_relay_on(ahead + 1)
            return carry

        lax.fori_loop(0, n_body, some_tasks, 0)
        return carry

    lax.fori_loop(0, n_tile, grad_tile, 0)

    def up_slots(t):
        return zall.at[pl.ds(pl.multiple_of(n_part * t, n_part), n_part)]

    def down_landed(t, carry):
        grad_copies(t)[0].wait_recv()
        return carry

    def up_landed(t, carry):
        pltpu.make_async_copy(up_slots(t), up_slots(t), grecv_sem.at[1, t]).wait()
        return carry

    pairs = [(t, s) for t in range(n_task) for s in range(t, n_task)]
    lane = lax.broadcasted_iota(jnp.int32, (8, LANES), 1)

    def gram_of(vals, sums):
        return tuple(acc + vals[t] * vals[s] for acc, (t, s) in zip(sums, pairs))

    n_row = sub_blk // 8

    def down_at(t, r, c):
        return (pl.ds(pl.multiple_of((t % 2) * half + r * 8, 8), 8), slice((t // 2) * hidden + c, (t // 2) * hidden + c + LANES))

    def down_sum(t, r, c):
        from_acc = pl.ds(pl.multiple_of(core * half + r * 8, 8), 8)
        return dn_acc[t, from_acc, c:c + LANES] + gp_s[down_at(t, r, c)]

    def up_sum(t, n, c):
        rows = pl.ds(pl.multiple_of(lax.rem(n, n_row) * 8, 8), 8)
        from_acc = pl.ds(pl.multiple_of(t * width + n * 8, 8), 8)
        return (up_acc[from_acc, pl.ds(pl.multiple_of(core * off + c, LANES), LANES)]
                + zall[n_part * t + lax.div(n, n_row), rows, c:c + LANES])

    def fold_down(r, sums):
        for c in range(0, hidden, LANES):
            vals = []
            for t in range(n_task):
                vals.append(down_sum(t, r, c))
            sums = gram_of(vals, sums)
        return sums

    def fold_up(n, sums):
        for c in range(0, win, LANES):
            edge = c < win - hidden // 2 or c + LANES > hidden // 2
            vals = []
            for t in range(n_task):
                v = up_sum(t, n, c)
                vals.append(jnp.where((lane + c >= first) & (lane + c < first + hidden // 2), v, 0.0) if edge else v)
            sums = gram_of(vals, sums)
        return sums

    sums = tuple(jnp.zeros((8, LANES), F32) for _ in pairs)
    lax.fori_loop(0, n_task, down_landed, 0)
    sums = lax.fori_loop(0, half // 8, fold_down, sums)
    lax.fori_loop(0, n_task, up_landed, 0)
    sums = lax.fori_loop(0, width // 8, fold_up, sums)
    lane1 = lax.broadcasted_iota(jnp.int32, (1, LANES), 1)
    row = lax.broadcasted_iota(jnp.int32, (8, LANES), 0)
    out = jnp.zeros((1, LANES), F32)
    for acc, (t, s) in zip(sums, pairs):
        total = jnp.sum(jnp.sum(acc, axis=0, keepdims=True), axis=1, keepdims=True)
        out = out + jnp.where((lane1 == t * n_task + s) | (lane1 == s * n_task + t), total, 0.0)
    msend[...] = out

    for k in range(1, n_all):
        remote(msend, mrecv.at[slot_of_me], msend_sem, mrecv_sem, other(k)).start()
    pltpu.make_async_copy(msend, mrecv.at[slot_of_me], mrecv_sem).start()
    pltpu.make_async_copy(mrecv, mrecv, mrecv_sem).wait()
    flat = jnp.sum(mrecv[...], axis=0)
    gram = jnp.zeros((8, LANES), F32)
    for t in range(n_task):
        line = flat if t == 0 else pltpu.roll(flat, LANES - t * n_task, 1)
        gram = gram + jnp.where((row == t) & (lane < n_task), jnp.broadcast_to(line, (8, LANES)), 0.0)
    scale = jnp.sum(jnp.sum(jnp.where(row == lane, gram, 0.0), axis=1, keepdims=True), axis=0, keepdims=True) / n_task
    gram = gram / scale
    w = jnp.where(lane < n_task, 1.0 / n_task, 0.0).astype(F32)

    def eg_pair(i, w):
        v = jnp.sum(gram * w, axis=1, keepdims=True)
        size = jnp.sum(w, axis=1, keepdims=True)
        w_col = jnp.sum(jnp.where(row == lane, w, 0.0), axis=1, keepdims=True)
        w_col = (w_col / size) * jnp.exp(-(v / size))
        v = jnp.sum(gram * w_col, axis=0, keepdims=True)
        size = jnp.sum(w_col, axis=0, keepdims=True)
        w_row = jnp.sum(jnp.where(row == lane, w_col, 0.0), axis=0, keepdims=True)
        w_row = (w_row / size) * jnp.exp(-(v / size))
        return jnp.broadcast_to(w_row, (8, LANES))

    w = lax.fori_loop(0, STEPS // 2, eg_pair, w)
    w = w / jnp.sum(w, axis=1, keepdims=True)
    a_ref[...] = w
    a = [jnp.broadcast_to(jnp.sum(jnp.where(lane == t, w, 0.0), axis=1, keepdims=True), (8, LANES))
         for t in range(n_task)]

    def weigh(parts):
        parts = [a[t] * v for t, v in enumerate(parts)]
        while len(parts) > 1:
            parts = [parts[i] + parts[i + 1] for i in range(0, len(parts), 2)]
        return parts[0]

    def mix_down(r, carry):
        rows = pl.ds(pl.multiple_of(r * 8, 8), 8)
        for c in range(0, hidden, LANES):
            g2_ref[rows, c:c + LANES] = weigh([down_sum(t, r, c) for t in range(n_task)])
        return carry

    def mix_up(n, carry):
        rows = pl.ds(pl.multiple_of(n * 8, 8), 8)
        for c in range(0, win, LANES):
            g1s[rows, c:c + LANES] = weigh([up_sum(t, n, c) for t in range(n_task)])
        return carry

    lax.fori_loop(0, half // 8, mix_down, 0)
    lax.fori_loop(0, width // 8, mix_up, 0)
    for c in range(0, win, LANES):
        g1t[c:c + LANES, :] = g1s[:, c:c + LANES].T
    g1_ref[...] = g1t[pl.ds(pl.multiple_of(first, 8), hidden // 2), :]

    for h, way in hw:
        for stage in range(4):
            gather_copy(h, stage, way).wait_send()
    for part in range(n_part):
        for s in range(4):
            u_pair(part, s).wait_send()
        sent = et.at[part, pl.ds(0, n_model - 1)]
        pltpu.make_async_copy(sent, sent, esend_sem.at[part]).wait()
    far_x.wait_send()
    sent = usend.at[pl.ds(0, n_tok - ring * blk), :]
    pltpu.make_async_copy(sent, sent, usend_sem).wait()

    def gone(t, carry):
        grad_copies(t)[0].wait_send()
        pltpu.make_async_copy(up_slots(t), up_slots(t), gsend_sem.at[1, t]).wait()
        return carry

    lax.fori_loop(0, n_task, gone, 0)
    sent = mrecv.at[pl.ds(0, n_all - 1)]
    pltpu.make_async_copy(sent, sent, msend_sem).wait()


def solution(mesh):
    n_model, n_data = mesh.shape['model'], mesh.shape['data']

    def local_step(tokens, w_up, w_down, task_heads, labels):
        n_tok, hidden = tokens.shape
        n_total = n_tok * n_data
        width = w_up.shape[1]
        n_task = task_heads.shape[0]
        blk = n_tok // n_model
        sub_blk = blk // 4
        half = width // 2
        win = -(-(hidden // 2) // LANES) * LANES
        tile = 32 * sub_blk
        any_spec = pl.BlockSpec(memory_space=pl.ANY)
        vmem_spec = pl.BlockSpec(memory_space=pltpu.VMEM)
        dma = pltpu.SemaphoreType.DMA
        vmem = pltpu.VMEM
        weights, grad_up, grad_down = pl.pallas_call(
            functools.partial(step_kernel, n_model, win, n_total),
            out_shape=(jax.ShapeDtypeStruct((8, LANES), F32), jax.ShapeDtypeStruct((hidden // 2, width), F32),
                       jax.ShapeDtypeStruct((half, hidden), F32)),
            in_specs=[any_spec, vmem_spec, vmem_spec, vmem_spec, vmem_spec],
            out_specs=(vmem_spec, vmem_spec, vmem_spec),
            scratch_shapes=[vmem((width, hidden), BF16), vmem((2 * n_task, win), BF16), vmem((n_task, 1, hidden), F32),
                            vmem((2, tile, hidden), BF16), vmem((n_tok, width), BF16), vmem((width, n_tok), BF16),
                            vmem((width, n_tok), F32), vmem((4, 2, 4, sub_blk, 16 * width), BF16),
                            vmem((2, 16, half, win), BF16), vmem((2, blk, win), BF16),
                            vmem((56, sub_blk, win), F32), vmem((4, 2 * n_task, blk), F32),
                            vmem((4, 2 * n_task, blk), F32), vmem((4, 2 * n_task, blk), F32),
                            vmem((4, n_task, blk), F32), vmem((4, n_model, n_task, blk), F32),
                            vmem((n_task, width, hidden), F32), vmem((n_task * width, hidden), F32),
                            vmem((n_task, hidden, LANES), F32), vmem((n_task, 1, tile), F32), vmem((4 * width, tile), BF16),
                            vmem((1, LANES), F32), vmem((2 * n_model, 1, LANES), F32), vmem((width, win), F32), vmem((win, width), F32),
                            dma((2,)), dma, dma((4, 4)), dma((2, 4, 2)), dma((2, 4, 2)), dma((4, 4)), dma((4, 4)),
                            dma((4, 4)), dma((4, 4)), dma((4,)), dma((4,)), dma((4,)), dma((4,)), dma((5,)),
                            dma((2, n_task)), dma((2, n_task)), dma, dma, pltpu.SemaphoreType.REGULAR],
            compiler_params=pltpu.CompilerParams(collective_id=0, has_side_effects=True, vmem_limit_bytes=67043328),
            name='step')(tokens, w_up, w_down, jnp.transpose(task_heads, (0, 2, 1)), labels)
        return weights[0, :n_task], grad_up, grad_down

    return jax.shard_map(
        local_step, mesh=mesh,
        in_specs=(P('data', None), P(None, 'model'), P('model', None), P(None, None, None), P(None, 'data')),
        out_specs=(P(None), P('data', 'model'), P(('model', 'data'), None)),
        check_vma=False)
```
